32 devices in a mesh: outer: 4 (over y, x), inner: 8 (over z, core).
Axes of the slice: x: 2, y: 2, z: 4, core: 2. Of those that a mesh axis runs over, the one named last changes fastest.
Arguments:
- queries: bfloat16 [2048, 1024], P(('outer', 'inner')), may hold values from -8 to 8
- key_rows: bfloat16 [2048, 1024], P(('outer', 'inner')), may hold values from -8 to 8
- value_rows: bfloat16 [2048, 1024], P(('outer', 'inner')), may hold values from -6 to 6
Outputs:
- attended: float32 [2048, 1024], P(('outer', 'inner'))
The draws below stay inside these ranges and needn't reach their ends.
All inputs are finite; a program needn't handle non-finite values.
Results may differ from the reference program's by a relative error of at most 0.0021.
Values may be sent and summed in bfloat16 or wider, within the bound.
A program may use at most 64 MiB of HBM per device.

```python
from functools import reduce
import jax
import jax.numpy as jnp
import numpy as np
from jax import lax

HEADS = 16
HEAD_DIM = 64
TOK_DEV = 64
GROUP_LEN = 512
SEQUENCE = 2048


def draw_queries(key, part):
    shape = (SEQUENCE, HEADS * HEAD_DIM)
    base = jax.random.truncated_normal(jax.random.fold_in(key, 1), -6.0, 6.0, shape, jnp.float32)
    return base.astype(jnp.bfloat16)


def draw_key_rows(key, part):
    shape = (SEQUENCE, HEADS * HEAD_DIM)
    base = jax.random.truncated_normal(jax.random.fold_in(key, 2), -6.0, 6.0, shape, jnp.float32)
    return base.astype(jnp.bfloat16)


def block_levels(key, extent, cuts, smallest, top_value):
    def one(axis_at, blocks):
        heights = jax.random.uniform(jax.random.fold_in(jax.random.fold_in(key, 6), axis_at), (blocks,), jnp.float32, smallest / len(cuts), top_value / len(cuts))
        return jnp.repeat(jnp.exp(heights), extent[axis_at] // blocks).reshape((-1,) + (1,) * (len(extent) - axis_at - 1))

    loudness = one(*cuts[0])
    for cut in cuts[1:]:
        loudness = loudness * one(*cut)
    return loudness


def gaussian(key, shape, scale, reach, split=(), kind=jnp.bfloat16):
    gain = block_levels(key, shape, split, -0.22, 0.18) if split else 1.0
    values = jax.random.normal(key, shape, jnp.float32) * scale * gain
    return jnp.minimum(jnp.maximum(values, -reach), reach).astype(kind)


def setup_inputs(seed: int = 0) -> dict:
    key_list = jax.random.split(jax.random.key(seed), 4)
    return {
        "queries": draw_queries(jax.random.fold_in(key_list[3], 71), 0),
        "key_rows": draw_key_rows(jax.random.fold_in(key_list[3], 71), 0),
        "value_rows": gaussian(key_list[2], (SEQUENCE, HEADS * HEAD_DIM), 1.0, 6.0, ((0, 32),)),
    }


FLOOR_SCORE = -1.0e30


def dense_causal(query_rows, key_rows, value_rows, ranks):
    scale = HEAD_DIM ** -0.5
    scores = jnp.dot(query_rows.astype(jnp.float32), key_rows.astype(jnp.float32).T, precision=lax.Precision.HIGHEST) * scale
    scores = jnp.where(ranks[None, :] <= ranks[:, None], scores, FLOOR_SCORE)
    row_max = jnp.max(scores, axis=1)
    weights = jnp.exp(scores - row_max[:, None])
    denominator = jnp.sum(weights, axis=1)
    rounded = lax.optimization_barrier(weights.astype(jnp.bfloat16)).astype(jnp.float32)
    summed = jnp.dot(rounded, value_rows.astype(jnp.float32), precision=lax.Precision.HIGHEST)
    return summed / denominator[:, None], row_max + jnp.log(denominator)


def level_one(queries, key_rows, value_rows):
    blocks = SEQUENCE // TOK_DEV
    ranks = jnp.arange(TOK_DEV, dtype=jnp.int32)

    def one_block(pieces):
        return jax.vmap(dense_causal, in_axes=(1, 1, 1, None), out_axes=(1, 1))(pieces[0], pieces[1], pieces[2], ranks)

    shaped = tuple(a.reshape(blocks, TOK_DEV, HEADS, HEAD_DIM) for a in (queries, key_rows, value_rows))
    outputs, lses = lax.map(one_block, shaped)
    return outputs.reshape(SEQUENCE, HEADS, HEAD_DIM), lses.reshape(SEQUENCE, HEADS)


def level_two(queries, key_rows, value_rows):
    groups = SEQUENCE // GROUP_LEN
    class_len = GROUP_LEN // 4
    ranks = jnp.arange(class_len, dtype=jnp.int32)

    def regroup(array):
        return array.reshape(groups, class_len, 4, HEADS, HEAD_DIM).transpose(0, 3, 2, 1, 4).reshape(groups * HEADS * 4, class_len, HEAD_DIM)

    def one_item(pieces):
        return dense_causal(pieces[0], pieces[1], pieces[2], ranks)

    outputs, lses = lax.map(one_item, (regroup(queries), regroup(key_rows), regroup(value_rows)))
    outputs = outputs.reshape(groups, HEADS, 4, class_len, HEAD_DIM).transpose(0, 3, 2, 1, 4).reshape(SEQUENCE, HEADS, HEAD_DIM)
    lses = lses.reshape(groups, HEADS, 4, class_len).transpose(0, 3, 2, 1).reshape(SEQUENCE, HEADS)
    return outputs, lses


def level_three(queries, key_rows, value_rows):
    sixteenth = SEQUENCE // 16
    pick = np.array([head * 16 + (head // 4) * 4 + residue for head in range(HEADS) for residue in range(4)], np.int32)
    ranks = jnp.arange(sixteenth, dtype=jnp.int32)

    def regroup(array):
        spread = array.reshape(sixteenth, 16, HEADS, HEAD_DIM).transpose(2, 1, 0, 3).reshape(HEADS * 16, sixteenth, HEAD_DIM)
        return jnp.take(spread, pick, axis=0)

    def one_item(pieces):
        return dense_causal(pieces[0], pieces[1], pieces[2], ranks)

    outputs, lses = lax.map(one_item, (regroup(queries), regroup(key_rows), regroup(value_rows)))
    full_out = jnp.zeros((HEADS * 16, sixteenth, HEAD_DIM), jnp.float32).at[pick].set(outputs)
    full_lse = jnp.full((HEADS * 16, sixteenth), FLOOR_SCORE, jnp.float32).at[pick].set(lses)
    full_out = full_out.reshape(HEADS, 16, sixteenth, HEAD_DIM).transpose(2, 1, 0, 3).reshape(SEQUENCE, HEADS, HEAD_DIM)
    full_lse = full_lse.reshape(HEADS, 16, sixteenth).transpose(2, 1, 0).reshape(SEQUENCE, HEADS)
    return full_out, full_lse


def merge_levels(parts):
    row_max = reduce(jnp.maximum, [lse for _, lse in parts])
    weights = [jnp.exp(lse - row_max) for _, lse in parts]
    denominator = reduce(jnp.add, weights)
    summed = reduce(jnp.add, [weight[..., None] * output for weight, (output, _) in zip(weights, parts)])
    return summed / denominator[..., None], row_max + jnp.log(denominator)


def reference(queries, key_rows, value_rows):
    shaped = tuple(a.reshape(SEQUENCE, HEADS, HEAD_DIM) for a in (queries, key_rows, value_rows))
    first = level_one(*shaped)
    second = level_two(*shaped)
    third = level_three(*shaped)
    combined, _ = merge_levels([first, second, third])
    return combined.reshape(SEQUENCE, HEADS * HEAD_DIM)
```

```python
import math
from functools import partial, reduce

import jax
import jax.numpy as jnp
import numpy as np
from jax import lax
from jax.experimental import pallas as pl
from jax.experimental.pallas import tpu as pltpu
from jax.sharding import PartitionSpec as P

HEADS = 16


FLOOR_SCORE = -1e30


def divisor_block(length, limit):
    extent = min(length, limit)
    while length % extent:
        extent -= 1
    return extent


def fresh_state(count, rows, width):
    return (
        jnp.full((count, rows), FLOOR_SCORE, jnp.float32),
        jnp.zeros((count, rows), jnp.float32),
        jnp.zeros((count, rows, width), jnp.float32),
    )


def finish_state(state):
    row_max, denominator, summed = state
    return (summed / denominator[..., None], row_max + jnp.log(denominator))


def online_step(state, query_rows, query_rank, key_rows, value_rows, key_rank):
    row_max, denominator, summed = state
    scale = query_rows.shape[-1] ** (-0.5)
    scores = (
        jnp.einsum("inh,ibh->inb", query_rows, key_rows, preferred_element_type=jnp.float32) * scale
    )
    scores = jnp.where(key_rank[None, None, :] <= query_rank[None, :, None], scores, FLOOR_SCORE)
    new_max = jnp.maximum(row_max, jnp.max(scores, axis=2))
    weights = jnp.exp(scores - new_max[..., None])
    rescale = jnp.exp(row_max - new_max)
    denominator = denominator * rescale + jnp.sum(weights, axis=2)
    summed = summed * rescale[..., None] + jnp.einsum(
        "inb,ibh->inh", weights.astype(jnp.bfloat16), value_rows, preferred_element_type=jnp.float32
    )
    return (new_max, denominator, summed)


def attend_keys(state, query_rows, query_rank, key_rows, value_rows, key_rank, stop=None):
    length = key_rows.shape[1]
    block = divisor_block(length, 512)

    def advance(index, carry):
        start = index * block
        piece_keys = lax.dynamic_slice_in_dim(key_rows, start, block, 1)
        piece_values = lax.dynamic_slice_in_dim(value_rows, start, block, 1)
        piece_rank = lax.dynamic_slice_in_dim(key_rank, start, block, 0)
        return online_step(carry, query_rows, query_rank, piece_keys, piece_values, piece_rank)

    upper = length // block if stop is None else stop
    return lax.fori_loop(0, upper, advance, state)


def attend(query_rows, query_rank, key_rows, value_rows, key_rank):
    count, length, width = query_rows.shape
    block = divisor_block(length, 512)
    steps = length // block
    query_split = query_rows.reshape(count, steps, block, width).swapaxes(0, 1)
    rank_split = query_rank.reshape(steps, block)

    def one_block(pieces):
        state = attend_keys(
            fresh_state(count, block, width),
            pieces[0],
            pieces[1],
            key_rows,
            value_rows,
            key_rank,
            pieces[2] + 1,
        )
        return finish_state(state)

    outputs, lses = lax.map(
        one_block, (query_split, rank_split, jnp.arange(steps, dtype=jnp.int32))
    )
    return (
        outputs.swapaxes(0, 1).reshape(count, length, width),
        lses.swapaxes(0, 1).reshape(count, length),
    )


def merge_levels(parts):
    row_max = reduce(jnp.maximum, [lse for _, lse in parts])
    weights = [jnp.exp(lse - row_max) for _, lse in parts]
    denominator = reduce(jnp.add, weights)
    summed = reduce(
        jnp.add, [weight[..., None] * output for weight, (output, _) in zip(weights, parts)]
    )
    return (summed / denominator[..., None], row_max + jnp.log(denominator))


def on_device(queries, key_rows, value_rows):
    tokens, features = queries.shape
    heads = HEADS
    width = features // heads
    outer_count = lax.axis_size("outer")
    inner_count = lax.axis_size("inner")
    outer_index = lax.axis_index("outer")
    inner_index = lax.axis_index("inner")
    per_device = 4 * heads // inner_count
    quarter = tokens // 4
    sixteenth = tokens // 16
    class_len = quarter * inner_count
    far_len = sixteenth * inner_count

    def to_items(array):
        return (
            array.reshape(quarter, 4, heads, width)
            .transpose(2, 1, 0, 3)
            .reshape(4 * heads, quarter, width)
        )

    local_ranks = jnp.arange(tokens, dtype=jnp.int32)
    head_major = [
        a.reshape(tokens, heads, width).transpose(1, 0, 2) for a in (queries, key_rows, value_rows)
    ]
    near_out, near_lse = attend(
        head_major[0], local_ranks, head_major[1], head_major[2], local_ranks
    )
    near_out = near_out.transpose(1, 0, 2)
    near_lse = near_lse.T
    item_index = inner_index * per_device + jnp.arange(per_device, dtype=jnp.int32)
    band = item_index // 16
    far_query_rank = outer_index * far_len + jnp.arange(far_len, dtype=jnp.int32)
    pick = np.array(
        [head * 16 + head // 4 * 4 + residue for head in range(heads) for residue in range(4)],
        np.int32,
    )

    def to_sixteen(array):
        spread = (
            array.reshape(sixteenth, 16, heads, width)
            .transpose(2, 1, 0, 3)
            .reshape(16 * heads, sixteenth, width)
        )
        return jnp.take(spread, pick, axis=0)

    gathered_k, gathered_v = (
        lax.all_gather(to_sixteen(key_rows), "outer", axis=1, tiled=True),
        lax.all_gather(to_sixteen(value_rows), "outer", axis=1, tiled=True),
    )
    mid_q, mid_k, mid_v, far_k, far_v = (
        lax.all_to_all(to_items(queries), "inner", split_axis=0, concat_axis=1, tiled=True),
        lax.all_to_all(to_items(key_rows), "inner", split_axis=0, concat_axis=1, tiled=True),
        lax.all_to_all(to_items(value_rows), "inner", split_axis=0, concat_axis=1, tiled=True),
        lax.all_to_all(gathered_k, "inner", split_axis=0, concat_axis=1, tiled=True),
        lax.all_to_all(gathered_v, "inner", split_axis=0, concat_axis=1, tiled=True),
    )
    split = mid_q.reshape(per_device, far_len, 4, width)
    picker = jnp.broadcast_to(band[:, None, None, None], (per_device, far_len, 1, width))
    far_q = jnp.take_along_axis(split, picker, axis=2)[:, :, 0, :]
    position = jnp.arange(far_k.shape[1], dtype=jnp.int32)
    far_key_rank = (
        position // sixteenth % outer_count * far_len
        + position // (outer_count * sixteenth) * sixteenth
        + position % sixteenth
    )
    far_state = attend_keys(
        fresh_state(per_device, far_len, width), far_q, far_query_rank, far_k, far_v, far_key_rank
    )
    far_out, far_lse = finish_state(far_state)
    class_ranks = jnp.arange(class_len, dtype=jnp.int32)
    mid_out, mid_lse = attend(mid_q, class_ranks, mid_k, mid_v, class_ranks)
    back_mid, back_mid_lse, back_far, back_far_lse = (
        lax.all_to_all(mid_out, "inner", split_axis=1, concat_axis=0, tiled=True),
        lax.all_to_all(mid_lse, "inner", split_axis=1, concat_axis=0, tiled=True),
        lax.all_to_all(far_out, "inner", split_axis=1, concat_axis=0, tiled=True),
        lax.all_to_all(far_lse, "inner", split_axis=1, concat_axis=0, tiled=True),
    )
    selector = np.array(
        [[band_index == head // 4 for band_index in range(4)] for head in range(heads)]
    )
    spread_out = jnp.where(
        selector[:, :, None, None, None], back_far.reshape(heads, 1, 4, sixteenth, width), 0.0
    )
    spread_lse = jnp.where(
        selector[:, :, None, None], back_far_lse.reshape(heads, 1, 4, sixteenth), FLOOR_SCORE
    )
    far_placed = (
        spread_out.reshape(heads, 16, sixteenth, width)
        .transpose(2, 1, 0, 3)
        .reshape(tokens, heads, width)
    )
    far_placed_lse = (
        spread_lse.reshape(heads, 16, sixteenth).transpose(2, 1, 0).reshape(tokens, heads)
    )
    placed = (
        back_mid.reshape(heads, 4, quarter, width)
        .transpose(2, 1, 0, 3)
        .reshape(tokens, heads, width)
    )
    placed_lse = back_mid_lse.reshape(heads, 4, quarter).transpose(2, 1, 0).reshape(tokens, heads)
    combined, _ = merge_levels(
        [(near_out, near_lse), (placed, placed_lse), (far_placed, far_placed_lse)]
    )
    return combined.reshape(tokens, features)


def fused_kernel(
    dims, q_ref, k_ref, v_ref, out_ref, q_held, k_held, v_held, q_rows, k_rows, v_rows, q_buf, k_buf, v_buf, far_k, far_v,
    top_ref, total_ref, sum_ref, ready, ready_half, landed,
    spare, send_sem, in_sem, far_sem, back_sem, held_sem, stage_sem,
):
    inner, outer, tokens, slab, width = dims
    chips = inner // 2
    half = inner // 2
    pairs = half // 2
    run = tokens // 16
    tile = tokens // 4
    wide = slab * inner // 4
    me = lax.axis_index("inner")
    mine = lax.axis_index("outer")
    chip = me // 2
    core = lax.rem(me, 2)
    side = me // half
    band = me * 4 // inner
    mesh_id = pl.DeviceIdType.MESH
    sources = (k_ref, v_ref, q_ref)
    held = (k_held, v_held, q_held)
    placed = (k_rows, v_rows, q_rows)
    buffers = (k_buf, v_buf, q_buf)
    pick_k, pick_v, rest_k, rest_v, whole_q = range(5)
    pieces = (
        (0, 0, tile),
        (1, 0, tile),
        (0, tile, tokens),
        (1, tile, tokens),
        (2, 0, tokens),
    )

    def columns(index):
        return pl.ds(pl.multiple_of(index * slab, slab), slab)

    def category(which, peer, owner):
        apart = owner // half != peer // half
        late = 4 + owner % half // 2
        if which < 2:
            return jnp.where(apart, 2, 0)
        early = peer // half == (0 if which == whole_q else 1)
        return jnp.where(apart, jnp.where(early, 3, late), 1)

    def drain(semaphore, rows):
        place = spare.at[0 : rows // 2]
        pltpu.make_async_copy(place, place, semaphore).wait()

    def inbound(which, peer, owner):
        array, start, stop = pieces[which]
        return pltpu.make_async_remote_copy(
            src_ref=placed[array].at[start:stop, columns(peer)],
            dst_ref=buffers[array].at[owner, start:stop, :],
            send_sem=send_sem.at[0],
            recv_sem=in_sem.at[category(which, peer, owner)],
            device_id={"inner": peer},
            device_id_type=mesh_id,
        )

    def farbound(which, part, peer, owner):
        blocks = pl.ds(part * half, half)
        return pltpu.make_async_remote_copy(
            src_ref=buffers[which].at[blocks, 0:tile, :],
            dst_ref=(far_k, far_v)[which].at[owner, blocks],
            send_sem=send_sem.at[1],
            recv_sem=far_sem.at[owner],
            device_id={"outer": peer},
            device_id_type=mesh_id,
        )

    def backbound(peer, owner):
        return pltpu.make_async_remote_copy(
            src_ref=ready.at[peer],
            dst_ref=out_ref.at[:, columns(owner)],
            send_sem=send_sem.at[2],
            recv_sem=back_sem.at[0],
            device_id={"inner": peer},
            device_id_type=mesh_id,
        )

    def crossbound(peer, owner):
        return pltpu.make_async_remote_copy(
            src_ref=ready_half.at[peer],
            dst_ref=landed.at[:, columns(owner)],
            send_sem=send_sem.at[2],
            recv_sem=back_sem.at[1 + owner % half // 2],
            device_id={"inner": peer},
            device_id_type=mesh_id,
        )

    own_held = [
        pltpu.make_async_copy(sources[which], held[which], held_sem.at[which]) for which in range(3)
    ]
    for copy in own_held:
        copy.start()

    barrier = pltpu.get_barrier_semaphore()
    partner = chip * 2 + 1 - core

    def greet(place):
        pl.semaphore_signal(barrier, inc=1, device_id=place, device_id_type=mesh_id)

    greet({"inner": partner})
    for step in range(1, outer):
        greet({"inner": chip * 2 + 1, "outer": lax.rem(mine + step, outer)})
    for other in range(chips):
        gap = jnp.abs(chip - other)
        counter = 0 if other >= chips // 2 else jnp.where(gap > 1, 1, 0)

        @pl.when(gap > 0)
        def _():
            greet({"inner": other * 2 + counter})

    def row_place(shape, axis, first):
        row = lax.broadcasted_iota(jnp.int32, shape, axis)
        residue = 4 * lax.rem(first + row // tile, 4) + row % tile // run
        return row % run * 16 + residue

    square = (tokens, tokens)
    at_row = lax.broadcasted_iota(jnp.int32, square, 0)
    at_column = lax.broadcasted_iota(jnp.int32, square, 1)
    for which in range(3):
        own_held[which].wait()
        for first in range(4):
            place = slice(first * wide, (first + 1) * wide)
            order = (row_place(square, 0, first) == at_column).astype(jnp.float32)
            placed[which][:, place] = jnp.dot(
                order.astype(jnp.bfloat16), held[which][:, place], preferred_element_type=jnp.float32
            ).astype(jnp.bfloat16)

    for other in range(outer - 1):

        @pl.when(mine <= other)
        def _():
            far_k[other] = jnp.zeros((inner, tile, slab), jnp.bfloat16)
            far_v[other] = jnp.zeros((inner, tile, slab), jnp.bfloat16)

    for which in range(3):
        buffers[which][me] = placed[which][:, columns(me)]

    adjacent = jnp.where(chip == 0, 1, 2)
    near_count = 1 + 2 * jnp.where(side == 0, adjacent, chips - 1)
    rest_count = 1 + 2 * (outer - 1) + jnp.where(side == 0, 2 * (chips - 1 - adjacent), 0)

    def pass_on(first, stage, count):
        @pl.when(core == first)
        def _():
            pl.semaphore_wait(barrier, count)
            pl.semaphore_signal(
                stage_sem.at[stage], inc=1, device_id={"inner": partner}, device_id_type=mesh_id
            )

        @pl.when(core != first)
        def _():
            pl.semaphore_wait(stage_sem.at[stage], 1)

    def send(which, distance):
        for other in range(2):

            @pl.when(chip + distance < chips)
            def _():
                inbound(which, (chip + distance) * 2 + other, me).start()

            @pl.when(chip - distance >= 0)
            def _():
                inbound(which, (chip - distance) * 2 + other, me).start()

    picks = (pick_k, pick_v)
    rest = (rest_k, rest_v)
    pass_on(0, 0, near_count)
    for which in range(5):
        inbound(which, partner, me).start()

    @pl.when(side == 0)
    def _():
        for which in picks:
            send(which, 1)
        for which in rest:
            send(which, 1)

        @pl.when(chip == 0)
        def _():
            send(whole_q, 1)

        pass_on(1, 1, rest_count)
        for distance in range(chips - 1, 1, -1):
            for which in picks:
                send(which, distance)
        for distance in range(chips - 1, 1, -1):
            for which in rest:
                send(which, distance)
        for distance in range(chips - 1, 1, -1):
            send(whole_q, distance)

        @pl.when(chip > 0)
        def _():
            send(whole_q, 1)

    @pl.when(side == 1)
    def _():
        for distance in range(chips - 1, 0, -1):
            for which in picks:
                send(which, distance)
        for distance in range(chips - 1, 0, -1):
            send(whole_q, distance)
        for which in rest:
            send(which, 1)
        for distance in range(chips - 1, 1, -1):
            for which in rest:
                send(which, distance)

    def forward(part):
        for which in range(2):
            for other in range(1, outer):

                @pl.when(mine < other)
                def _():
                    farbound(which, part, other, mine).start()

    same = at_row % tile // run == at_column % tile // run
    both = (at_row < tile) & (at_column < tile)
    below = jnp.where(same, jnp.where(both, 1.0, 0.0), FLOOR_SCORE)
    before = row_place(square, 1, band) <= row_place(square, 0, band)
    diagonal = jnp.where(
        before, jnp.where(same, jnp.where(both, math.log2(3.0), 1.0), 0.0), FLOOR_SCORE
    )
    never = jnp.full(square, FLOOR_SCORE, jnp.float32)

    def twice(table):
        return jnp.concatenate([table, table], axis=0)

    below_pair = twice(jnp.concatenate([below, below], axis=1))
    below_pair = jnp.concatenate([below_pair, below_pair], axis=0)
    edge_pair = jnp.concatenate(
        [jnp.concatenate([diagonal, never], axis=1), jnp.concatenate([below, diagonal], axis=1)], axis=0
    )
    edge_pair = twice(edge_pair)
    far_rows = inner * tile
    far_shape = (pairs * 4 * tile, (outer - 1) * far_rows)
    far_query = lax.broadcasted_iota(jnp.int32, far_shape, 0)
    far_key = lax.broadcasted_iota(jnp.int32, far_shape, 1)
    far_table = jnp.where(
        (far_query % tile // run == far_key % tile // run) & (far_key // far_rows < mine), 0.0, FLOOR_SCORE
    )
    factor = width ** (-0.5) * math.log2(math.e)
    contract = (((1,), (1,)), ((), ()))

    def by_head(rows):
        lane_head = lax.broadcasted_iota(jnp.int32, rows.shape, 1) // width
        return jnp.concatenate(
            [jnp.where(lane_head == head, rows, jnp.zeros_like(rows)) for head in range(2)], axis=0
        )

    def attend_block(old, rows, keys, values, table):
        scores = lax.dot_general(rows, keys, contract, preferred_element_type=jnp.float32)
        scores = scores * factor + table
        top = jnp.max(scores, axis=1, keepdims=True)
        if old is not None:
            top = jnp.maximum(top, old[0])
        weights = jnp.exp2(scores - top)
        total = jnp.sum(weights, axis=1, keepdims=True)
        summed = jnp.dot(weights.astype(jnp.bfloat16), values, preferred_element_type=jnp.float32)
        if old is not None:
            rescale = jnp.exp2(old[0] - top)
            total = total + old[1] * rescale
            summed = summed + old[2] * rescale
        return top, total, summed

    def load_state(index, pair):
        return (
            top_ref[index, pair].reshape(4 * tokens, 1),
            total_ref[index, pair].reshape(4 * tokens, 1),
            sum_ref[index, pair].reshape(4 * tokens, slab),
        )

    def keep_state(index, pair, state):
        top_ref[index, pair] = state[0].reshape(4, tokens, 1)
        total_ref[index, pair] = state[1].reshape(4, tokens, 1)
        sum_ref[index, pair] = state[2].reshape(4, tokens, slab)

    def pair_queries(index, pair):
        rows = q_buf[pl.ds(index * half + 2 * pair, 2)].reshape(2 * tokens, slab)
        return by_head(rows)

    def edge(index, pair, old):
        blocks = pl.ds(index * half, 2 * pair + 2)
        count = (2 * pair + 2) * tokens
        keys = k_buf[blocks].reshape(count, slab)
        values = v_buf[blocks].reshape(count, slab)
        table = jnp.concatenate([below_pair] * pair + [edge_pair], axis=1)
        return attend_block(old, pair_queries(index, pair), keys, values, table)

    def far_block(index):
        rows = [
            by_head(q_buf[pl.ds(index * half + 2 * pair, 2), 0:tile].reshape(2 * tile, slab))
            for pair in range(pairs)
        ]
        count = pairs * 4 * tile
        old = (
            top_ref[index, :, :, 0:tile].reshape(count, 1),
            total_ref[index, :, :, 0:tile].reshape(count, 1),
            sum_ref[index, :, :, 0:tile].reshape(count, slab),
        )
        keys = far_k[...].reshape((outer - 1) * far_rows, slab)
        values = far_v[...].reshape((outer - 1) * far_rows, slab)
        top, total, summed = attend_block(old, jnp.concatenate(rows, axis=0), keys, values, far_table)
        top_ref[index, :, :, 0:tile] = top.reshape(pairs, 4, tile, 1)
        total_ref[index, :, :, 0:tile] = total.reshape(pairs, 4, tile, 1)
        sum_ref[index, :, :, 0:tile] = summed.reshape(pairs, 4, tile, slab)

    pair_rows = (2 * tokens, 2 * tokens)
    natural = lax.broadcasted_iota(jnp.int32, pair_rows, 0)
    stored = lax.broadcasted_iota(jnp.int32, pair_rows, 1)
    stored_place = stored // tokens * tokens + row_place(pair_rows, 1, band) % tokens
    restore = (natural == stored_place).astype(jnp.float32).astype(jnp.bfloat16)
    lane_head = lax.broadcasted_iota(jnp.int32, (2 * tokens, slab), 1) // width

    def finish(index, pair):
        summed = sum_ref[index, pair] / total_ref[index, pair]
        summed = summed.reshape(2, 2 * tokens, slab)
        return jnp.where(lane_head == 0, summed[0], summed[1])

    def restored(result, exact):
        coarse = result.astype(jnp.bfloat16)
        moved = jnp.dot(restore, coarse, preferred_element_type=jnp.float32)
        if exact:
            rest = (result - coarse.astype(jnp.float32)).astype(jnp.bfloat16)
            moved = moved + jnp.dot(restore, rest, preferred_element_type=jnp.float32)
        return moved.reshape(2, tokens, slab)

    here = side * half
    there = (1 - side) * half
    drain(in_sem.at[0], (half - 1) * 2 * tile)

    @pl.when(side == 1)
    def _():
        pass_on(1, 1, rest_count)

    forward(side)
    drain(in_sem.at[1], (half - 1) * (3 * tokens - 2 * tile))
    for pair in range(pairs):
        keep_state(side, pair, edge(side, pair, None))
        other_count = 4 * tokens
        keep_state(
            1 - side,
            pair,
            (
                jnp.full((other_count, 1), FLOOR_SCORE, jnp.float32),
                jnp.zeros((other_count, 1), jnp.float32),
                jnp.zeros((other_count, slab), jnp.float32),
            ),
        )
    drain(in_sem.at[2], half * 2 * tile)
    forward(1 - side)

    @pl.when(side == 0)
    def _():
        drain(in_sem.at[3], half * tokens)

    @pl.when(side == 1)
    def _():
        drain(in_sem.at[3], half * 2 * (tokens - tile))

    low_keys = k_buf[0:half].reshape(half * tokens, slab)
    low_values = v_buf[0:half].reshape(half * tokens, slab)
    for pair in range(pairs):
        table = jnp.concatenate([below_pair] * pairs, axis=1)
        keep_state(
            1,
            pair,
            attend_block(load_state(1, pair), pair_queries(1, pair), low_keys, low_values, table),
        )

    for other in range(outer - 1):

        @pl.when(mine > other)
        def _():
            drain(far_sem.at[other], 2 * far_rows)

    far_block(side)
    for pair in range(pairs):
        moved = restored(finish(side, pair), True)
        for step in range(2):
            peer = here + 2 * pair + step
            ready[peer] = moved[step]

            @pl.when(peer == me)
            def _():
                out_ref[:, columns(me)] = moved[step]

            @pl.when(peer != me)
            def _():
                backbound(peer, me).start()

    for pair in range(pairs):

        @pl.when(side == 0)
        def _():
            drain(in_sem.at[4 + pair], 4 * (tokens - tile))

        @pl.when(side == 1)
        def _():
            drain(in_sem.at[4 + pair], 2 * tokens)

        keep_state(1 - side, pair, edge(1 - side, pair, load_state(1 - side, pair)))
        if pair == pairs - 1:
            far_block(1 - side)
    for pair in range(pairs):
        moved = restored(finish(1 - side, pair), False).astype(jnp.bfloat16)
        for step in range(2):
            peer = there + 2 * pair + step
            ready_half[peer] = moved[step]
            crossbound(peer, me).start()

    drain(back_sem.at[0], (half - 1) * 2 * tokens)
    for pair in range(pairs):
        drain(back_sem.at[1 + pair], 2 * tokens)
        for step in (2 * pair, 2 * pair + 1):
            owner = there + step
            out_ref[:, columns(owner)] = landed[:, columns(owner)].astype(jnp.float32)

    drain(send_sem.at[0], (inner - 1) * 3 * tokens)
    drain(send_sem.at[2], (half - 1) * 2 * tokens + half * tokens)
    for count in range(1, outer):

        @pl.when(outer - 1 - mine == count)
        def _():
            drain(send_sem.at[1], count * 2 * far_rows)


def fused(queries, key_rows, value_rows):
    tokens, features = queries.shape
    inner = lax.axis_size("inner")
    outer = lax.axis_size("outer")
    slab = features // inner
    tile = tokens // 4
    pairs = inner // 4
    any_space = pl.BlockSpec(memory_space=pl.ANY)
    dims = (inner, outer, tokens, slab, features // HEADS)
    return pl.pallas_call(
        partial(fused_kernel, dims),
        out_shape=pltpu.VMEM((tokens, features), jnp.float32),
        in_specs=[any_space] * 3,
        out_specs=pl.BlockSpec(memory_space=pltpu.VMEM),
        scratch_shapes=[
            *[pltpu.VMEM((tokens, features), jnp.bfloat16)] * 6,
            *[pltpu.VMEM((inner, tokens, slab), jnp.bfloat16)] * 3,
            *[pltpu.VMEM((outer - 1, inner, tile, slab), jnp.bfloat16)] * 2,
            *[pltpu.VMEM((2, pairs, 4, tokens, 1), jnp.float32)] * 2,
            pltpu.VMEM((2, pairs, 4, tokens, slab), jnp.float32),
            pltpu.VMEM((inner, tokens, slab), jnp.float32),
            pltpu.VMEM((inner, tokens, slab), jnp.bfloat16),
            pltpu.VMEM((tokens, features), jnp.bfloat16),
            pltpu.VMEM((inner * 2 * tokens, slab), jnp.float32),
            pltpu.SemaphoreType.DMA((3,)),
            pltpu.SemaphoreType.DMA((4 + pairs,)),
            pltpu.SemaphoreType.DMA((outer - 1,)),
            pltpu.SemaphoreType.DMA((1 + pairs,)),
            pltpu.SemaphoreType.DMA((3,)),
            pltpu.SemaphoreType.REGULAR((2,)),
        ],
        compiler_params=pltpu.CompilerParams(collective_id=0, has_side_effects=True),
    )(queries, key_rows, value_rows)


def device_program(queries, key_rows, value_rows):
    tokens, features = queries.shape
    inner = lax.axis_size("inner")
    outer = lax.axis_size("outer")
    width = features // HEADS
    fits = (
        inner * 2 == HEADS
        and outer > 1
        and inner % 4 == 0
        and width * 2 == 128
        and tokens % 64 == 0
        and inner * tokens <= 1024
        and (outer - 1) * inner * tokens // 4 <= 1024
    )
    if fits:
        return fused(queries, key_rows, value_rows)
    return on_device(queries, key_rows, value_rows)


def solution(mesh):
    placed = (P(("outer", "inner"), None), P(("outer", "inner"), None), P(("outer", "inner"), None))
    return jax.shard_map(
        device_program,
        mesh=mesh,
        in_specs=placed,
        out_specs=P(("outer", "inner"), None),
        check_vma=False,
    )
```

```python
import math
from functools import partial, reduce

import jax
import jax.numpy as jnp
import numpy as np
from jax import lax
from jax.experimental import pallas as pl
from jax.experimental.pallas import tpu as pltpu
from jax.sharding import PartitionSpec as P

HEADS = 16


FLOOR_SCORE = -1e30


def divisor_block(length, limit):
    extent = min(length, limit)
    while length % extent:
        extent -= 1
    return extent


def fresh_state(count, rows, width):
    return (
        jnp.full((count, rows), FLOOR_SCORE, jnp.float32),
        jnp.zeros((count, rows), jnp.float32),
        jnp.zeros((count, rows, width), jnp.float32),
    )


def finish_state(state):
    row_max, denominator, summed = state
    return (summed / denominator[..., None], row_max + jnp.log(denominator))


def online_step(state, query_rows, query_rank, key_rows, value_rows, key_rank):
    row_max, denominator, summed = state
    scale = query_rows.shape[-1] ** (-0.5)
    scores = (
        jnp.einsum("inh,ibh->inb", query_rows, key_rows, preferred_element_type=jnp.float32) * scale
    )
    scores = jnp.where(key_rank[None, None, :] <= query_rank[None, :, None], scores, FLOOR_SCORE)
    new_max = jnp.maximum(row_max, jnp.max(scores, axis=2))
    weights = jnp.exp(scores - new_max[..., None])
    rescale = jnp.exp(row_max - new_max)
    denominator = denominator * rescale + jnp.sum(weights, axis=2)
    summed = summed * rescale[..., None] + jnp.einsum(
        "inb,ibh->inh", weights.astype(jnp.bfloat16), value_rows, preferred_element_type=jnp.float32
    )
    return (new_max, denominator, summed)


def attend_keys(state, query_rows, query_rank, key_rows, value_rows, key_rank, stop=None):
    length = key_rows.shape[1]
    block = divisor_block(length, 512)

    def advance(index, carry):
        start = index * block
        piece_keys = lax.dynamic_slice_in_dim(key_rows, start, block, 1)
        piece_values = lax.dynamic_slice_in_dim(value_rows, start, block, 1)
        piece_rank = lax.dynamic_slice_in_dim(key_rank, start, block, 0)
        return online_step(carry, query_rows, query_rank, piece_keys, piece_values, piece_rank)

    upper = length // block if stop is None else stop
    return lax.fori_loop(0, upper, advance, state)


def attend(query_rows, query_rank, key_rows, value_rows, key_rank):
    count, length, width = query_rows.shape
    block = divisor_block(length, 512)
    steps = length // block
    query_split = query_rows.reshape(count, steps, block, width).swapaxes(0, 1)
    rank_split = query_rank.reshape(steps, block)

    def one_block(pieces):
        state = attend_keys(
            fresh_state(count, block, width),
            pieces[0],
            pieces[1],
            key_rows,
            value_rows,
            key_rank,
            pieces[2] + 1,
        )
        return finish_state(state)

    outputs, lses = lax.map(
        one_block, (query_split, rank_split, jnp.arange(steps, dtype=jnp.int32))
    )
    return (
        outputs.swapaxes(0, 1).reshape(count, length, width),
        lses.swapaxes(0, 1).reshape(count, length),
    )


def merge_levels(parts):
    row_max = reduce(jnp.maximum, [lse for _, lse in parts])
    weights = [jnp.exp(lse - row_max) for _, lse in parts]
    denominator = reduce(jnp.add, weights)
    summed = reduce(
        jnp.add, [weight[..., None] * output for weight, (output, _) in zip(weights, parts)]
    )
    return (summed / denominator[..., None], row_max + jnp.log(denominator))


def on_device(queries, key_rows, value_rows):
    tokens, features = queries.shape
    heads = HEADS
    width = features // heads
    outer_count = lax.axis_size("outer")
    inner_count = lax.axis_size("inner")
    outer_index = lax.axis_index("outer")
    inner_index = lax.axis_index("inner")
    per_device = 4 * heads // inner_count
    quarter = tokens // 4
    sixteenth = tokens // 16
    class_len = quarter * inner_count
    far_len = sixteenth * inner_count

    def to_items(array):
        return (
            array.reshape(quarter, 4, heads, width)
            .transpose(2, 1, 0, 3)
            .reshape(4 * heads, quarter, width)
        )

    local_ranks = jnp.arange(tokens, dtype=jnp.int32)
    head_major = [
        a.reshape(tokens, heads, width).transpose(1, 0, 2) for a in (queries, key_rows, value_rows)
    ]
    near_out, near_lse = attend(
        head_major[0], local_ranks, head_major[1], head_major[2], local_ranks
    )
    near_out = near_out.transpose(1, 0, 2)
    near_lse = near_lse.T
    item_index = inner_index * per_device + jnp.arange(per_device, dtype=jnp.int32)
    band = item_index // 16
    far_query_rank = outer_index * far_len + jnp.arange(far_len, dtype=jnp.int32)
    pick = np.array(
        [head * 16 + head // 4 * 4 + residue for head in range(heads) for residue in range(4)],
        np.int32,
    )

    def to_sixteen(array):
        spread = (
            array.reshape(sixteenth, 16, heads, width)
            .transpose(2, 1, 0, 3)
            .reshape(16 * heads, sixteenth, width)
        )
        return jnp.take(spread, pick, axis=0)

    gathered_k, gathered_v = (
        lax.all_gather(to_sixteen(key_rows), "outer", axis=1, tiled=True),
        lax.all_gather(to_sixteen(value_rows), "outer", axis=1, tiled=True),
    )
    mid_q, mid_k, mid_v, far_k, far_v = (
        lax.all_to_all(to_items(queries), "inner", split_axis=0, concat_axis=1, tiled=True),
        lax.all_to_all(to_items(key_rows), "inner", split_axis=0, concat_axis=1, tiled=True),
        lax.all_to_all(to_items(value_rows), "inner", split_axis=0, concat_axis=1, tiled=True),
        lax.all_to_all(gathered_k, "inner", split_axis=0, concat_axis=1, tiled=True),
        lax.all_to_all(gathered_v, "inner", split_axis=0, concat_axis=1, tiled=True),
    )
    split = mid_q.reshape(per_device, far_len, 4, width)
    picker = jnp.broadcast_to(band[:, None, None, None], (per_device, far_len, 1, width))
    far_q = jnp.take_along_axis(split, picker, axis=2)[:, :, 0, :]
    position = jnp.arange(far_k.shape[1], dtype=jnp.int32)
    far_key_rank = (
        position // sixteenth % outer_count * far_len
        + position // (outer_count * sixteenth) * sixteenth
        + position % sixteenth
    )
    far_state = attend_keys(
        fresh_state(per_device, far_len, width), far_q, far_query_rank, far_k, far_v, far_key_rank
    )
    far_out, far_lse = finish_state(far_state)
    class_ranks = jnp.arange(class_len, dtype=jnp.int32)
    mid_out, mid_lse = attend(mid_q, class_ranks, mid_k, mid_v, class_ranks)
    back_mid, back_mid_lse, back_far, back_far_lse = (
        lax.all_to_all(mid_out, "inner", split_axis=1, concat_axis=0, tiled=True),
        lax.all_to_all(mid_lse, "inner", split_axis=1, concat_axis=0, tiled=True),
        lax.all_to_all(far_out, "inner", split_axis=1, concat_axis=0, tiled=True),
        lax.all_to_all(far_lse, "inner", split_axis=1, concat_axis=0, tiled=True),
    )
    selector = np.array(
        [[band_index == head // 4 for band_index in range(4)] for head in range(heads)]
    )
    spread_out = jnp.where(
        selector[:, :, None, None, None], back_far.reshape(heads, 1, 4, sixteenth, width), 0.0
    )
    spread_lse = jnp.where(
        selector[:, :, None, None], back_far_lse.reshape(heads, 1, 4, sixteenth), FLOOR_SCORE
    )
    far_placed = (
        spread_out.reshape(heads, 16, sixteenth, width)
        .transpose(2, 1, 0, 3)
        .reshape(tokens, heads, width)
    )
    far_placed_lse = (
        spread_lse.reshape(heads, 16, sixteenth).transpose(2, 1, 0).reshape(tokens, heads)
    )
    placed = (
        back_mid.reshape(heads, 4, quarter, width)
        .transpose(2, 1, 0, 3)
        .reshape(tokens, heads, width)
    )
    placed_lse = back_mid_lse.reshape(heads, 4, quarter).transpose(2, 1, 0).reshape(tokens, heads)
    combined, _ = merge_levels(
        [(near_out, near_lse), (placed, placed_lse), (far_placed, far_placed_lse)]
    )
    return combined.reshape(tokens, features)


def fused_kernel(
    dims, q_ref, k_ref, v_ref, out_ref, q_held, k_held, v_held, q_rows, k_rows, v_rows, q_buf, k_buf, v_buf, far_k, far_v,
    state_ref, ready, ready_half, landed,
    spare, send_sem, in_sem, far_sem, back_sem, held_sem, stage_sem,
):
    inner, outer, tokens, slab, width = dims
    chips = inner // 2
    half = inner // 2
    pairs = half // 2
    run = tokens // 16
    tile = tokens // 4
    wide = slab * inner // 4
    me = lax.axis_index("inner")
    mine = lax.axis_index("outer")
    chip = me // 2
    core = lax.rem(me, 2)
    side = me // half
    band = me * 4 // inner
    mesh_id = pl.DeviceIdType.MESH
    sources = (k_ref, v_ref, q_ref)
    held = (k_held, v_held, q_held)
    placed = (k_rows, v_rows, q_rows)
    buffers = (k_buf, v_buf, q_buf)
    pick_k, pick_v, rest_k, rest_v, whole_q = range(5)
    pieces = (
        (0, 0, tile),
        (1, 0, tile),
        (0, tile, tokens),
        (1, tile, tokens),
        (2, 0, tokens),
    )

    def columns(index):
        return pl.ds(pl.multiple_of(index * slab, slab), slab)

    def drain(semaphore, rows):
        place = spare.at[0 : rows // 2]
        pltpu.make_async_copy(place, place, semaphore).wait()

    def inbound(which, peer, owner, arrival):
        array, start, stop = pieces[which]
        return pltpu.make_async_remote_copy(
            src_ref=placed[array].at[start:stop, columns(peer)],
            dst_ref=buffers[array].at[owner, start:stop, :],
            send_sem=send_sem.at[0],
            recv_sem=in_sem.at[arrival],
            device_id={"inner": peer},
            device_id_type=mesh_id,
        )

    def farbound(which, part, peer, owner):
        blocks = pl.ds(part * half, half)
        return pltpu.make_async_remote_copy(
            src_ref=buffers[which].at[blocks, 0:tile, :],
            dst_ref=(far_k, far_v)[which].at[owner, blocks],
            send_sem=send_sem.at[1],
            recv_sem=far_sem.at[owner],
            device_id={"outer": peer},
            device_id_type=mesh_id,
        )

    def backbound(peer, owner):
        return pltpu.make_async_remote_copy(
            src_ref=ready.at[peer],
            dst_ref=out_ref.at[:, columns(owner)],
            send_sem=send_sem.at[2],
            recv_sem=back_sem.at[0],
            device_id={"inner": peer},
            device_id_type=mesh_id,
        )

    def crossbound(peer, owner):
        return pltpu.make_async_remote_copy(
            src_ref=ready_half.at[peer],
            dst_ref=landed.at[:, columns(owner)],
            send_sem=send_sem.at[2],
            recv_sem=back_sem.at[1 + owner % half // 2],
            device_id={"inner": peer},
            device_id_type=mesh_id,
        )

    own_held = [
        pltpu.make_async_copy(sources[which], held[which], held_sem.at[which]) for which in range(3)
    ]
    for copy in own_held:
        copy.start()

    barrier = pltpu.get_barrier_semaphore()
    partner = chip * 2 + 1 - core

    def greet(place):
        pl.semaphore_signal(barrier, inc=1, device_id=place, device_id_type=mesh_id)

    greet({"inner": partner})
    for step in range(1, outer):
        greet({"inner": chip * 2 + 1, "outer": lax.rem(mine + step, outer)})
    for other in range(chips):
        if other < chips // 2:
            counter = jnp.where(jnp.abs(chip - other) > 1, 1, 0)
        else:
            counter = jnp.where(chip > other, 1, 0)

        @pl.when(chip != other)
        def _():
            greet({"inner": other * 2 + counter})

    def row_place(shape, axis, first):
        row = lax.broadcasted_iota(jnp.int32, shape, axis)
        residue = 4 * lax.rem(first + row // tile, 4) + row % tile // run
        return row % run * 16 + residue

    square = (tokens, tokens)
    at_row = lax.broadcasted_iota(jnp.int32, square, 0)
    at_column = lax.broadcasted_iota(jnp.int32, square, 1)
    orders = [
        (row_place(square, 0, first) == at_column).astype(jnp.float32).astype(jnp.bfloat16)
        for first in range(4)
    ]

    def place_rows(which):
        own_held[which].wait()
        for first in range(4):
            place = slice(first * wide, (first + 1) * wide)
            placed[which][:, place] = jnp.dot(
                orders[first], held[which][:, place], preferred_element_type=jnp.float32
            ).astype(jnp.bfloat16)
        buffers[which][me] = placed[which][:, columns(me)]

    adjacent = jnp.where(chip == 0, 1, 2)
    near_count = 1 + 2 * jnp.where(side == 0, adjacent, chip)
    rest_count = 1 + 2 * (outer - 1) + 2 * (chips - 1 - jnp.where(side == 0, adjacent, chip))

    def pass_on(first, stage, count):
        @pl.when(core == first)
        def _():
            pl.semaphore_wait(barrier, count)
            pl.semaphore_signal(
                stage_sem.at[stage], inc=1, device_id={"inner": partner}, device_id_type=mesh_id
            )

        @pl.when(core != first)
        def _():
            pl.semaphore_wait(stage_sem.at[stage], 1)

    picks = (pick_k, pick_v)
    rest = (rest_k, rest_v)
    query = (whole_q,)

    def arrival_of(which, source, target):
        low = chips // 2
        apart = (source < low) != (target < low)
        if which in picks:
            return 2 if apart else 0
        if not apart:
            return 1
        early = (which == whole_q) == (target < low)
        return 3 if early else 4 + source % low

    def send(source, batches):
        for group, targets in batches:
            for target in targets:
                for which in group:
                    for other in range(2):
                        arrival = arrival_of(which, source, target)
                        inbound(which, target * 2 + other, me, arrival).start()

    def send_partner(group):
        for which in group:
            inbound(which, partner, me, 0 if which in picks else 1).start()

    place_rows(0)
    place_rows(1)
    pass_on(0, 0, near_count)
    send_partner(picks + rest)

    @pl.when(chip == 0)
    def _():
        send(0, ((picks, (1,)), (rest, (1,))))

    @pl.when(chip == 1)
    def _():
        send(1, ((picks, (2, 0)), (rest, (2, 0))))

    @pl.when(chip == 2)
    def _():
        send(2, ((picks, (0, 1)),))

    @pl.when(chip == 3)
    def _():
        send(3, ((picks, (0, 1, 2)),))

    place_rows(2)
    send_partner(query)

    @pl.when(chip == 0)
    def _():
        send(0, ((query, (1,)),))
        pass_on(1, 1, rest_count)
        send(0, ((picks, (3, 2)), (rest, (3, 2)), (query, (3, 2))))

    @pl.when(chip == 1)
    def _():
        send(1, ((query, (0,)),))
        pass_on(1, 1, rest_count)
        send(1, ((picks, (3,)), (rest, (3,)), (query, (3, 2))))

    @pl.when(chip == 2)
    def _():
        send(2, ((query, (0, 1)),))
        pass_on(1, 1, rest_count)
        send(2, ((picks, (3,)), (rest, (0, 1)), (query, (3,)), (rest, (3,))))

    @pl.when(chip == 3)
    def _():
        send(3, ((query, (0, 1, 2)), (rest, (2,)), (rest, (0, 1))))

    for other in range(outer - 1):

        @pl.when(mine <= other)
        def _():
            far_k[other] = jnp.zeros((inner, tile, slab), jnp.bfloat16)
            far_v[other] = jnp.zeros((inner, tile, slab), jnp.bfloat16)

    def forward(part):
        for which in range(2):
            for other in range(1, outer):

                @pl.when(mine < other)
                def _():
                    farbound(which, part, other, mine).start()

    same = at_row % tile // run == at_column % tile // run
    both = (at_row < tile) & (at_column < tile)
    below = jnp.where(same, jnp.where(both, 1.0, 0.0), FLOOR_SCORE)
    before = row_place(square, 1, band) <= row_place(square, 0, band)
    diagonal = jnp.where(
        before, jnp.where(same, jnp.where(both, math.log2(3.0), 1.0), 0.0), FLOOR_SCORE
    )
    never = jnp.full(square, FLOOR_SCORE, jnp.float32)

    def twice(table):
        return jnp.concatenate([table, table], axis=0)

    below_pair = twice(jnp.concatenate([below, below], axis=1))
    below_pair = jnp.concatenate([below_pair, below_pair], axis=0)
    edge_pair = jnp.concatenate(
        [jnp.concatenate([diagonal, never], axis=1), jnp.concatenate([below, diagonal], axis=1)], axis=0
    )
    edge_pair = twice(edge_pair)
    far_rows = inner * tile
    far_shape = (pairs * 4 * tile, (outer - 1) * far_rows)
    far_query = lax.broadcasted_iota(jnp.int32, far_shape, 0)
    far_key = lax.broadcasted_iota(jnp.int32, far_shape, 1)
    far_table = jnp.where(
        (far_query % tile // run == far_key % tile // run) & (far_key // far_rows < mine), 0.0, FLOOR_SCORE
    )
    factor = width ** (-0.5) * math.log2(math.e)
    contract = (((1,), (1,)), ((), ()))

    def by_head(rows):
        lane_head = lax.broadcasted_iota(jnp.int32, rows.shape, 1) // width
        return jnp.concatenate(
            [jnp.where(lane_head == head, rows, jnp.zeros_like(rows)) for head in range(2)], axis=0
        )

    def across(column):
        return jnp.broadcast_to(column, (column.shape[0], slab))

    def attend_part(rows, keys, values, table):
        scores = lax.dot_general(rows, keys, contract, preferred_element_type=jnp.float32)
        scores = scores * factor + table
        top = jnp.max(scores, axis=1, keepdims=True)
        weights = jnp.exp2(scores - top)
        total = jnp.sum(weights, axis=1, keepdims=True)
        summed = jnp.dot(weights.astype(jnp.bfloat16), values, preferred_element_type=jnp.float32)
        return across(top), across(total), summed

    def join(one, two):
        top = jnp.maximum(one[0], two[0])
        first = jnp.exp2(one[0] - top)
        second = jnp.exp2(two[0] - top)
        return top, one[1] * first + two[1] * second, one[2] * first + two[2] * second

    def join_tile(state, far):
        cut = [part.reshape(4, tokens, slab) for part in state]
        met = join([part[:, 0:tile] for part in cut], far)
        return [
            jnp.concatenate([new, old[:, tile:]], axis=1).reshape(4 * tokens, slab)
            for new, old in zip(met, cut)
        ]

    def load_state(index, pair):
        return [state_ref[which, index, pair] for which in range(3)]

    def keep_state(index, pair, state):
        for which in range(3):
            state_ref[which, index, pair] = state[which]

    def pair_queries(index, pair):
        rows = q_buf[index * half + 2 * pair : index * half + 2 * pair + 2]
        return by_head(rows.reshape(2 * tokens, slab))

    def span_of(buffer, start, stop):
        return buffer[start:stop].reshape((stop - start) * tokens, slab)

    def edge(index, pair):
        start = index * half
        stop = start + 2 * pair + 2
        table = jnp.concatenate([below_pair] * pair + [edge_pair], axis=1)
        return attend_part(
            pair_queries(index, pair), span_of(k_buf, start, stop), span_of(v_buf, start, stop), table
        )

    def below_block(pair):
        table = jnp.concatenate([below_pair] * pairs, axis=1)
        return attend_part(
            pair_queries(1, pair), span_of(k_buf, 0, half), span_of(v_buf, 0, half), table
        )

    def far_block(index, first, stop):
        span = stop - first
        rows = [
            by_head(
                q_buf[index * half + 2 * pair : index * half + 2 * pair + 2, 0:tile].reshape(2 * tile, slab)
            )
            for pair in range(first, stop)
        ]
        count = span * 4 * tile
        keys = far_k[...].reshape((outer - 1) * far_rows, slab)
        values = far_v[...].reshape((outer - 1) * far_rows, slab)
        state = attend_part(jnp.concatenate(rows, axis=0), keys, values, far_table[0:count])
        return [
            [part.reshape(span, 4, tile, slab)[place] for part in state] for place in range(span)
        ]

    pair_rows = (2 * tokens, 2 * tokens)
    natural = lax.broadcasted_iota(jnp.int32, pair_rows, 0)
    stored = lax.broadcasted_iota(jnp.int32, pair_rows, 1)
    stored_place = stored // tokens * tokens + row_place(pair_rows, 1, band) % tokens
    restore = (natural == stored_place).astype(jnp.float32).astype(jnp.bfloat16)
    lane_head = lax.broadcasted_iota(jnp.int32, (2 * tokens, slab), 1) // width

    def finish(state):
        summed = (state[2] / state[1]).reshape(2, 2 * tokens, slab)
        return jnp.where(lane_head == 0, summed[0], summed[1])

    def restored(result, exact):
        coarse = result.astype(jnp.bfloat16)
        moved = jnp.dot(restore, coarse, preferred_element_type=jnp.float32)
        if exact:
            rest = (result - coarse.astype(jnp.float32)).astype(jnp.bfloat16)
            moved = moved + jnp.dot(restore, rest, preferred_element_type=jnp.float32)
        return moved.reshape(2, tokens, slab)

    def return_near(index, pair, state):
        moved = restored(finish(state), True)
        for step in range(2):
            peer = index * half + 2 * pair + step
            ready[peer] = moved[step]

            @pl.when(me == peer)
            def _():
                out_ref[:, columns(me)] = moved[step]

            @pl.when(me != peer)
            def _():
                backbound(peer, me).start()

    def return_apart(index, pair, state):
        moved = restored(finish(state), False).astype(jnp.bfloat16)
        for step in range(2):
            peer = index * half + 2 * pair + step
            ready_half[peer] = moved[step]
            crossbound(peer, me).start()

    drain(in_sem.at[0], (half - 1) * 2 * tile)

    @pl.when(chip == chips - 1)
    def _():
        pass_on(1, 1, rest_count)

    forward(side)
    drain(in_sem.at[2], half * 2 * tile)
    forward(1 - side)
    drain(in_sem.at[1], (half - 1) * (3 * tokens - 2 * tile))

    def wait_far():
        for other in range(outer - 1):

            @pl.when(mine > other)
            def _():
                drain(far_sem.at[other], 2 * far_rows)

    @pl.when(side == 0)
    def _():
        for pair in range(pairs):
            keep_state(0, pair, edge(0, pair))
        drain(in_sem.at[3], half * tokens)
        for pair in range(pairs):
            keep_state(1, pair, below_block(pair))
        wait_far()
        near_far = far_block(0, 0, pairs)
        apart_far = far_block(1, 0, pairs)
        for pair in range(pairs):
            keep_state(1, pair, join_tile(load_state(1, pair), apart_far[pair]))
            return_near(0, pair, join_tile(load_state(0, pair), near_far[pair]))
        for pair in range(pairs):
            drain(in_sem.at[4 + pair], 4 * (tokens - tile))
            return_apart(1, pair, join(load_state(1, pair), edge(1, pair)))

    @pl.when(side == 1)
    def _():
        for pair in range(pairs):
            keep_state(1, pair, edge(1, pair))
        drain(in_sem.at[3], half * 2 * (tokens - tile))
        for pair in range(pairs):
            keep_state(1, pair, join(load_state(1, pair), below_block(pair)))
        wait_far()
        for pair in range(pairs):
            drain(in_sem.at[4 + pair], 2 * tokens)
            apart_far = far_block(0, pair, pair + 1)
            return_apart(0, pair, join_tile(edge(0, pair), apart_far[0]))
        near_far = far_block(1, 0, pairs)
        for pair in range(pairs):
            return_near(1, pair, join_tile(load_state(1, pair), near_far[pair]))

    there = (1 - side) * half
    drain(back_sem.at[0], (half - 1) * 2 * tokens)
    for pair in range(pairs):
        drain(back_sem.at[1 + pair], 2 * tokens)
        for step in (2 * pair, 2 * pair + 1):
            owner = there + step
            out_ref[:, columns(owner)] = landed[:, columns(owner)].astype(jnp.float32)

    drain(send_sem.at[0], (inner - 1) * 3 * tokens)
    drain(send_sem.at[2], (half - 1) * 2 * tokens + half * tokens)
    for count in range(1, outer):

        @pl.when(outer - 1 - mine == count)
        def _():
            drain(send_sem.at[1], count * 2 * far_rows)


def fused(queries, key_rows, value_rows):
    tokens, features = queries.shape
    inner = lax.axis_size("inner")
    outer = lax.axis_size("outer")
    slab = features // inner
    tile = tokens // 4
    pairs = inner // 4
    any_space = pl.BlockSpec(memory_space=pl.ANY)
    dims = (inner, outer, tokens, slab, features // HEADS)
    return pl.pallas_call(
        partial(fused_kernel, dims),
        out_shape=pltpu.VMEM((tokens, features), jnp.float32),
        in_specs=[any_space] * 3,
        out_specs=pl.BlockSpec(memory_space=pltpu.VMEM),
        scratch_shapes=[
            *[pltpu.VMEM((tokens, features), jnp.bfloat16)] * 6,
            *[pltpu.VMEM((inner, tokens, slab), jnp.bfloat16)] * 3,
            *[pltpu.VMEM((outer - 1, inner, tile, slab), jnp.bfloat16)] * 2,
            pltpu.VMEM((3, 2, pairs, 4 * tokens, slab), jnp.float32),
            pltpu.VMEM((inner, tokens, slab), jnp.float32),
            pltpu.VMEM((inner, tokens, slab), jnp.bfloat16),
            pltpu.VMEM((tokens, features), jnp.bfloat16),
            pltpu.VMEM((inner * 2 * tokens, slab), jnp.float32),
            pltpu.SemaphoreType.DMA((3,)),
            pltpu.SemaphoreType.DMA((4 + pairs,)),
            pltpu.SemaphoreType.DMA((outer - 1,)),
            pltpu.SemaphoreType.DMA((1 + pairs,)),
            pltpu.SemaphoreType.DMA((3,)),
            pltpu.SemaphoreType.REGULAR((2,)),
        ],
        compiler_params=pltpu.CompilerParams(collective_id=0, has_side_effects=True),
    )(queries, key_rows, value_rows)


def device_program(queries, key_rows, value_rows):
    tokens, features = queries.shape
    inner = lax.axis_size("inner")
    outer = lax.axis_size("outer")
    width = features // HEADS
    fits = (
        inner * 2 == HEADS
        and outer > 1
        and inner % 4 == 0
        and width * 2 == 128
        and tokens % 64 == 0
        and inner * tokens <= 1024
        and (outer - 1) * inner * tokens // 4 <= 1024
    )
    if fits:
        return fused(queries, key_rows, value_rows)
    return on_device(queries, key_rows, value_rows)


def solution(mesh):
    placed = (P(("outer", "inner"), None), P(("outer", "inner"), None), P(("outer", "inner"), None))
    return jax.shard_map(
        device_program,
        mesh=mesh,
        in_specs=placed,
        out_specs=P(("outer", "inner"), None),
        check_vma=False,
    )
```

```python
import math
from functools import partial, reduce

import jax
import jax.numpy as jnp
import numpy as np
from jax import lax
from jax.experimental import pallas as pl
from jax.experimental.pallas import tpu as pltpu
from jax.sharding import PartitionSpec as P

HEADS = 16


FLOOR_SCORE = -1e30


def divisor_block(length, limit):
    extent = min(length, limit)
    while length % extent:
        extent -= 1
    return extent


def fresh_state(count, rows, width):
    return (
        jnp.full((count, rows), FLOOR_SCORE, jnp.float32),
        jnp.zeros((count, rows), jnp.float32),
        jnp.zeros((count, rows, width), jnp.float32),
    )


def finish_state(state):
    row_max, denominator, summed = state
    return (summed / denominator[..., None], row_max + jnp.log(denominator))


def online_step(state, query_rows, query_rank, key_rows, value_rows, key_rank):
    row_max, denominator, summed = state
    scale = query_rows.shape[-1] ** (-0.5)
    scores = (
        jnp.einsum("inh,ibh->inb", query_rows, key_rows, preferred_element_type=jnp.float32) * scale
    )
    scores = jnp.where(key_rank[None, None, :] <= query_rank[None, :, None], scores, FLOOR_SCORE)
    new_max = jnp.maximum(row_max, jnp.max(scores, axis=2))
    weights = jnp.exp(scores - new_max[..., None])
    rescale = jnp.exp(row_max - new_max)
    denominator = denominator * rescale + jnp.sum(weights, axis=2)
    summed = summed * rescale[..., None] + jnp.einsum(
        "inb,ibh->inh", weights.astype(jnp.bfloat16), value_rows, preferred_element_type=jnp.float32
    )
    return (new_max, denominator, summed)


def attend_keys(state, query_rows, query_rank, key_rows, value_rows, key_rank, stop=None):
    length = key_rows.shape[1]
    block = divisor_block(length, 512)

    def advance(index, carry):
        start = index * block
        piece_keys = lax.dynamic_slice_in_dim(key_rows, start, block, 1)
        piece_values = lax.dynamic_slice_in_dim(value_rows, start, block, 1)
        piece_rank = lax.dynamic_slice_in_dim(key_rank, start, block, 0)
        return online_step(carry, query_rows, query_rank, piece_keys, piece_values, piece_rank)

    upper = length // block if stop is None else stop
    return lax.fori_loop(0, upper, advance, state)


def attend(query_rows, query_rank, key_rows, value_rows, key_rank):
    count, length, width = query_rows.shape
    block = divisor_block(length, 512)
    steps = length // block
    query_split = query_rows.reshape(count, steps, block, width).swapaxes(0, 1)
    rank_split = query_rank.reshape(steps, block)

    def one_block(pieces):
        state = attend_keys(
            fresh_state(count, block, width),
            pieces[0],
            pieces[1],
            key_rows,
            value_rows,
            key_rank,
            pieces[2] + 1,
        )
        return finish_state(state)

    outputs, lses = lax.map(
        one_block, (query_split, rank_split, jnp.arange(steps, dtype=jnp.int32))
    )
    return (
        outputs.swapaxes(0, 1).reshape(count, length, width),
        lses.swapaxes(0, 1).reshape(count, length),
    )


def merge_levels(parts):
    row_max = reduce(jnp.maximum, [lse for _, lse in parts])
    weights = [jnp.exp(lse - row_max) for _, lse in parts]
    denominator = reduce(jnp.add, weights)
    summed = reduce(
        jnp.add, [weight[..., None] * output for weight, (output, _) in zip(weights, parts)]
    )
    return (summed / denominator[..., None], row_max + jnp.log(denominator))


def on_device(queries, key_rows, value_rows):
    tokens, features = queries.shape
    heads = HEADS
    width = features // heads
    outer_count = lax.axis_size("outer")
    inner_count = lax.axis_size("inner")
    outer_index = lax.axis_index("outer")
    inner_index = lax.axis_index("inner")
    per_device = 4 * heads // inner_count
    quarter = tokens // 4
    sixteenth = tokens // 16
    class_len = quarter * inner_count
    far_len = sixteenth * inner_count

    def to_items(array):
        return (
            array.reshape(quarter, 4, heads, width)
            .transpose(2, 1, 0, 3)
            .reshape(4 * heads, quarter, width)
        )

    local_ranks = jnp.arange(tokens, dtype=jnp.int32)
    head_major = [
        a.reshape(tokens, heads, width).transpose(1, 0, 2) for a in (queries, key_rows, value_rows)
    ]
    near_out, near_lse = attend(
        head_major[0], local_ranks, head_major[1], head_major[2], local_ranks
    )
    near_out = near_out.transpose(1, 0, 2)
    near_lse = near_lse.T
    item_index = inner_index * per_device + jnp.arange(per_device, dtype=jnp.int32)
    band = item_index // 16
    far_query_rank = outer_index * far_len + jnp.arange(far_len, dtype=jnp.int32)
    pick = np.array(
        [head * 16 + head // 4 * 4 + residue for head in range(heads) for residue in range(4)],
        np.int32,
    )

    def to_sixteen(array):
        spread = (
            array.reshape(sixteenth, 16, heads, width)
            .transpose(2, 1, 0, 3)
            .reshape(16 * heads, sixteenth, width)
        )
        return jnp.take(spread, pick, axis=0)

    gathered_k, gathered_v = (
        lax.all_gather(to_sixteen(key_rows), "outer", axis=1, tiled=True),
        lax.all_gather(to_sixteen(value_rows), "outer", axis=1, tiled=True),
    )
    mid_q, mid_k, mid_v, far_k, far_v = (
        lax.all_to_all(to_items(queries), "inner", split_axis=0, concat_axis=1, tiled=True),
        lax.all_to_all(to_items(key_rows), "inner", split_axis=0, concat_axis=1, tiled=True),
        lax.all_to_all(to_items(value_rows), "inner", split_axis=0, concat_axis=1, tiled=True),
        lax.all_to_all(gathered_k, "inner", split_axis=0, concat_axis=1, tiled=True),
        lax.all_to_all(gathered_v, "inner", split_axis=0, concat_axis=1, tiled=True),
    )
    split = mid_q.reshape(per_device, far_len, 4, width)
    picker = jnp.broadcast_to(band[:, None, None, None], (per_device, far_len, 1, width))
    far_q = jnp.take_along_axis(split, picker, axis=2)[:, :, 0, :]
    position = jnp.arange(far_k.shape[1], dtype=jnp.int32)
    far_key_rank = (
        position // sixteenth % outer_count * far_len
        + position // (outer_count * sixteenth) * sixteenth
        + position % sixteenth
    )
    far_state = attend_keys(
        fresh_state(per_device, far_len, width), far_q, far_query_rank, far_k, far_v, far_key_rank
    )
    far_out, far_lse = finish_state(far_state)
    class_ranks = jnp.arange(class_len, dtype=jnp.int32)
    mid_out, mid_lse = attend(mid_q, class_ranks, mid_k, mid_v, class_ranks)
    back_mid, back_mid_lse, back_far, back_far_lse = (
        lax.all_to_all(mid_out, "inner", split_axis=1, concat_axis=0, tiled=True),
        lax.all_to_all(mid_lse, "inner", split_axis=1, concat_axis=0, tiled=True),
        lax.all_to_all(far_out, "inner", split_axis=1, concat_axis=0, tiled=True),
        lax.all_to_all(far_lse, "inner", split_axis=1, concat_axis=0, tiled=True),
    )
    selector = np.array(
        [[band_index == head // 4 for band_index in range(4)] for head in range(heads)]
    )
    spread_out = jnp.where(
        selector[:, :, None, None, None], back_far.reshape(heads, 1, 4, sixteenth, width), 0.0
    )
    spread_lse = jnp.where(
        selector[:, :, None, None], back_far_lse.reshape(heads, 1, 4, sixteenth), FLOOR_SCORE
    )
    far_placed = (
        spread_out.reshape(heads, 16, sixteenth, width)
        .transpose(2, 1, 0, 3)
        .reshape(tokens, heads, width)
    )
    far_placed_lse = (
        spread_lse.reshape(heads, 16, sixteenth).transpose(2, 1, 0).reshape(tokens, heads)
    )
    placed = (
        back_mid.reshape(heads, 4, quarter, width)
        .transpose(2, 1, 0, 3)
        .reshape(tokens, heads, width)
    )
    placed_lse = back_mid_lse.reshape(heads, 4, quarter).transpose(2, 1, 0).reshape(tokens, heads)
    combined, _ = merge_levels(
        [(near_out, near_lse), (placed, placed_lse), (far_placed, far_placed_lse)]
    )
    return combined.reshape(tokens, features)


def fused_kernel(
    dims, q_ref, k_ref, v_ref, out_ref, q_held, k_held, v_held, q_rows, k_rows, v_rows, q_buf, k_buf, v_buf, far_k, far_v,
    state_ref, ready, ready_half, landed,
    spare, send_sem, in_sem, far_sem, back_sem, held_sem, stage_sem,
):
    inner, outer, tokens, slab, width = dims
    chips = inner // 2
    half = inner // 2
    pairs = half // 2
    run = tokens // 16
    tile = tokens // 4
    wide = slab * inner // 4
    me = lax.axis_index("inner")
    mine = lax.axis_index("outer")
    chip = me // 2
    core = lax.rem(me, 2)
    side = me // half
    band = me * 4 // inner
    mesh_id = pl.DeviceIdType.MESH
    sources = (k_ref, v_ref, q_ref)
    held = (k_held, v_held, q_held)
    placed = (k_rows, v_rows, q_rows)
    buffers = (k_buf, v_buf, q_buf)
    pick_k, pick_v, rest_k, rest_v, whole_q = range(5)
    pieces = (
        (0, 0, tile),
        (1, 0, tile),
        (0, tile, tokens),
        (1, tile, tokens),
        (2, 0, tokens),
    )

    def columns(index):
        return pl.ds(pl.multiple_of(index * slab, slab), slab)

    def drain(semaphore, rows):
        place = spare.at[0 : rows // 2]
        pltpu.make_async_copy(place, place, semaphore).wait()

    def inbound(which, peer, owner, arrival):
        array, start, stop = pieces[which]
        return pltpu.make_async_remote_copy(
            src_ref=placed[array].at[start:stop, columns(peer)],
            dst_ref=buffers[array].at[owner, start:stop, :],
            send_sem=send_sem.at[0],
            recv_sem=in_sem.at[arrival],
            device_id={"inner": peer},
            device_id_type=mesh_id,
        )

    def farbound(which, part, peer, owner):
        blocks = pl.ds(part * half, half)
        return pltpu.make_async_remote_copy(
            src_ref=buffers[which].at[blocks, 0:tile, :],
            dst_ref=(far_k, far_v)[which].at[owner, blocks],
            send_sem=send_sem.at[1],
            recv_sem=far_sem.at[owner],
            device_id={"outer": peer},
            device_id_type=mesh_id,
        )

    def backbound(peer, owner):
        return pltpu.make_async_remote_copy(
            src_ref=ready.at[peer],
            dst_ref=out_ref.at[:, columns(owner)],
            send_sem=send_sem.at[2],
            recv_sem=back_sem.at[0],
            device_id={"inner": peer},
            device_id_type=mesh_id,
        )

    def crossbound(peer, owner):
        return pltpu.make_async_remote_copy(
            src_ref=ready_half.at[peer],
            dst_ref=landed.at[:, columns(owner)],
            send_sem=send_sem.at[2],
            recv_sem=back_sem.at[1 + owner % half // 2],
            device_id={"inner": peer},
            device_id_type=mesh_id,
        )

    own_held = [
        pltpu.make_async_copy(sources[which], held[which], held_sem.at[which]) for which in range(3)
    ]
    for copy in own_held:
        copy.start()

    barrier = pltpu.get_barrier_semaphore()
    partner = chip * 2 + 1 - core

    def greet(place):
        pl.semaphore_signal(barrier, inc=1, device_id=place, device_id_type=mesh_id)

    greet({"inner": partner})
    for step in range(1, outer):
        greet({"inner": chip * 2 + 1, "outer": lax.rem(mine + step, outer)})
    for other in range(chips):
        if other < chips // 2:
            counter = jnp.where(jnp.abs(chip - other) > 1, 1, 0)
        else:
            counter = jnp.where(chip > other, 1, 0)

        @pl.when(chip != other)
        def _():
            greet({"inner": other * 2 + counter})

    def row_place(shape, axis, first):
        row = lax.broadcasted_iota(jnp.int32, shape, axis)
        residue = 4 * lax.rem(first + row // tile, 4) + row % tile // run
        return row % run * 16 + residue

    square = (tokens, tokens)
    at_row = lax.broadcasted_iota(jnp.int32, square, 0)
    at_column = lax.broadcasted_iota(jnp.int32, square, 1)
    orders = [
        (row_place(square, 0, first) == at_column).astype(jnp.float32).astype(jnp.bfloat16)
        for first in range(4)
    ]

    def place_rows(which):
        own_held[which].wait()
        for first in range(4):
            place = slice(first * wide, (first + 1) * wide)
            placed[which][:, place] = jnp.dot(
                orders[first], held[which][:, place], preferred_element_type=jnp.float32
            ).astype(jnp.bfloat16)
        buffers[which][me] = placed[which][:, columns(me)]

    adjacent = jnp.where(chip == 0, 1, 2)
    near_count = 1 + 2 * jnp.where(side == 0, adjacent, chip)
    rest_count = 1 + 2 * (outer - 1) + 2 * (chips - 1 - jnp.where(side == 0, adjacent, chip))

    def pass_on(first, stage, count):
        @pl.when(core == first)
        def _():
            pl.semaphore_wait(barrier, count)
            pl.semaphore_signal(
                stage_sem.at[stage], inc=1, device_id={"inner": partner}, device_id_type=mesh_id
            )

        @pl.when(core != first)
        def _():
            pl.semaphore_wait(stage_sem.at[stage], 1)

    picks = (pick_k, pick_v)
    rest = (rest_k, rest_v)
    query = (whole_q,)

    def arrival_of(which, source, target):
        low = chips // 2
        apart = (source < low) != (target < low)
        if which in picks:
            return 2 if apart else 0
        if not apart:
            return 1
        if target < low:
            return 3 if which == whole_q else 4 + source % low
        if source == 0:
            return 4
        return 5 if which == whole_q else 3

    def send(source, batches):
        for group, targets in batches:
            for target in targets:
                for which in group:
                    for other in range(2):
                        arrival = arrival_of(which, source, target)
                        inbound(which, target * 2 + other, me, arrival).start()

    def send_partner(group):
        for which in group:
            inbound(which, partner, me, 0 if which in picks else 1).start()

    place_rows(0)
    place_rows(1)
    pass_on(0, 0, near_count)
    send_partner(picks + rest)

    @pl.when(chip == 0)
    def _():
        send(0, ((picks, (1,)), (rest, (1,))))

    @pl.when(chip == 1)
    def _():
        send(1, ((picks, (2, 0)), ((rest_k,), (2,)), (rest, (0,))))

    @pl.when(chip == 2)
    def _():
        send(2, ((picks, (0, 1)),))

    @pl.when(chip == 3)
    def _():
        send(3, ((picks, (0, 1, 2)),))

    place_rows(2)
    send_partner(query)

    @pl.when(chip == 0)
    def _():
        send(0, ((query, (1,)),))
        pass_on(1, 1, rest_count)
        send(0, ((picks, (3, 2)), (rest, (3,)), (query, (3,)), (rest, (2,)), (query, (2,))))

    @pl.when(chip == 1)
    def _():
        send(1, ((query, (0,)),))
        pass_on(1, 1, rest_count)
        send(1, ((picks, (3,)), (rest, (3,)), ((rest_v,), (2,)), (query, (3, 2))))

    @pl.when(chip == 2)
    def _():
        send(2, ((query, (0, 1)),))
        pass_on(1, 1, rest_count)
        send(2, ((picks, (3,)), (rest, (0, 1)), (query, (3,)), (rest, (3,))))

    @pl.when(chip == 3)
    def _():
        send(3, ((query, (0, 1, 2)), (rest, (2,)), (rest, (0, 1))))

    for other in range(outer - 1):

        @pl.when(mine <= other)
        def _():
            far_k[other] = jnp.zeros((inner, tile, slab), jnp.bfloat16)
            far_v[other] = jnp.zeros((inner, tile, slab), jnp.bfloat16)

    def forward(part):
        for other in range(outer - 1, 0, -1):

            @pl.when(mine < other)
            def _():
                for which in range(2):
                    farbound(which, part, other, mine).start()

    same = at_row % tile // run == at_column % tile // run
    both = (at_row < tile) & (at_column < tile)
    below = jnp.where(same, jnp.where(both, 1.0, 0.0), FLOOR_SCORE)
    before = row_place(square, 1, band) <= row_place(square, 0, band)
    diagonal = jnp.where(
        before, jnp.where(same, jnp.where(both, math.log2(3.0), 1.0), 0.0), FLOOR_SCORE
    )
    never = jnp.full(square, FLOOR_SCORE, jnp.float32)

    def twice(table):
        return jnp.concatenate([table, table], axis=0)

    below_pair = twice(jnp.concatenate([below, below], axis=1))
    below_pair = jnp.concatenate([below_pair, below_pair], axis=0)
    edge_pair = jnp.concatenate(
        [jnp.concatenate([diagonal, never], axis=1), jnp.concatenate([below, diagonal], axis=1)], axis=0
    )
    edge_pair = twice(edge_pair)
    far_rows = inner * tile
    far_shape = (pairs * 4 * tile, (outer - 1) * far_rows)
    far_query = lax.broadcasted_iota(jnp.int32, far_shape, 0)
    far_key = lax.broadcasted_iota(jnp.int32, far_shape, 1)
    far_table = jnp.where(
        (far_query % tile // run == far_key % tile // run) & (far_key // far_rows < mine), 0.0, FLOOR_SCORE
    )
    factor = width ** (-0.5) * math.log2(math.e)
    contract = (((1,), (1,)), ((), ()))

    def by_head(rows):
        lane_head = lax.broadcasted_iota(jnp.int32, rows.shape, 1) // width
        return jnp.concatenate(
            [jnp.where(lane_head == head, rows, jnp.zeros_like(rows)) for head in range(2)], axis=0
        )

    def across(column):
        return jnp.broadcast_to(column, (column.shape[0], slab))

    def attend_part(rows, keys, values, table):
        scores = lax.dot_general(rows, keys, contract, preferred_element_type=jnp.float32)
        scores = scores * factor + table
        top = jnp.max(scores, axis=1, keepdims=True)
        weights = jnp.exp2(scores - top)
        total = jnp.sum(weights, axis=1, keepdims=True)
        summed = jnp.dot(weights.astype(jnp.bfloat16), values, preferred_element_type=jnp.float32)
        return across(top), across(total), summed

    def join(one, two):
        top = jnp.maximum(one[0], two[0])
        first = jnp.exp2(one[0] - top)
        second = jnp.exp2(two[0] - top)
        return top, one[1] * first + two[1] * second, one[2] * first + two[2] * second

    def join_tile(state, far):
        cut = [part.reshape(4, tokens, slab) for part in state]
        met = join([part[:, 0:tile] for part in cut], far)
        return [
            jnp.concatenate([new, old[:, tile:]], axis=1).reshape(4 * tokens, slab)
            for new, old in zip(met, cut)
        ]

    def load_state(index, pair):
        return [state_ref[which, index, pair] for which in range(3)]

    def keep_state(index, pair, state):
        for which in range(3):
            state_ref[which, index, pair] = state[which]

    def pair_queries(index, pair):
        rows = q_buf[index * half + 2 * pair : index * half + 2 * pair + 2]
        return by_head(rows.reshape(2 * tokens, slab))

    def span_of(buffer, start, stop):
        return buffer[start:stop].reshape((stop - start) * tokens, slab)

    def edge(index, pair):
        start = index * half
        stop = start + 2 * pair + 2
        table = jnp.concatenate([below_pair] * pair + [edge_pair], axis=1)
        return attend_part(
            pair_queries(index, pair), span_of(k_buf, start, stop), span_of(v_buf, start, stop), table
        )

    def below_block(pair):
        table = jnp.concatenate([below_pair] * pairs, axis=1)
        return attend_part(
            pair_queries(1, pair), span_of(k_buf, 0, half), span_of(v_buf, 0, half), table
        )

    def far_block(index, first, stop):
        span = stop - first
        rows = [
            by_head(
                q_buf[index * half + 2 * pair : index * half + 2 * pair + 2, 0:tile].reshape(2 * tile, slab)
            )
            for pair in range(first, stop)
        ]
        count = span * 4 * tile
        keys = far_k[...].reshape((outer - 1) * far_rows, slab)
        values = far_v[...].reshape((outer - 1) * far_rows, slab)
        state = attend_part(jnp.concatenate(rows, axis=0), keys, values, far_table[0:count])
        return [
            [part.reshape(span, 4, tile, slab)[place] for part in state] for place in range(span)
        ]

    pair_rows = (2 * tokens, 2 * tokens)
    natural = lax.broadcasted_iota(jnp.int32, pair_rows, 0)
    stored = lax.broadcasted_iota(jnp.int32, pair_rows, 1)
    stored_place = stored // tokens * tokens + row_place(pair_rows, 1, band) % tokens
    restore = (natural == stored_place).astype(jnp.float32).astype(jnp.bfloat16)
    lane_head = lax.broadcasted_iota(jnp.int32, (2 * tokens, slab), 1) // width

    def finish(state):
        total, summed = (part.reshape(2, 2 * tokens, slab) for part in state[1:])
        return jnp.where(lane_head == 0, summed[0], summed[1]) / jnp.where(
            lane_head == 0, total[0], total[1]
        )

    def restored(result, exact):
        coarse = result.astype(jnp.bfloat16)
        moved = jnp.dot(restore, coarse, preferred_element_type=jnp.float32)
        if exact:
            rest = (result - coarse.astype(jnp.float32)).astype(jnp.bfloat16)
            moved = moved + jnp.dot(restore, rest, preferred_element_type=jnp.float32)
        return moved.reshape(2, tokens, slab)

    def return_near(index, states):
        for pair, state in enumerate(states):
            moved = restored(finish(state), True)
            for step in range(2):
                ready[index * half + 2 * pair + step] = moved[step]
        for step in range(1, half):
            backbound(index * half + lax.rem(me + step, half), me).start()
        out_ref[:, columns(me)] = ready[me]

    def return_apart(index, pair, state):
        moved = restored(finish(state), False).astype(jnp.bfloat16)
        for step in range(2):
            peer = index * half + 2 * pair + step
            ready_half[peer] = moved[step]
            crossbound(peer, me).start()

    drain(in_sem.at[0], (half - 1) * 2 * tile)

    @pl.when(chip == chips - 1)
    def _():
        pass_on(1, 1, rest_count)

    forward(side)
    drain(in_sem.at[2], half * 2 * tile)
    forward(1 - side)
    drain(in_sem.at[1], (half - 1) * (3 * tokens - 2 * tile))

    def wait_far():
        for other in range(outer - 1):

            @pl.when(mine > other)
            def _():
                drain(far_sem.at[other], 2 * far_rows)

    @pl.when(side == 0)
    def _():
        for pair in range(pairs):
            keep_state(0, pair, edge(0, pair))
        drain(in_sem.at[3], half * tokens)
        for pair in range(pairs):
            keep_state(1, pair, below_block(pair))
        wait_far()
        near_far = far_block(0, 0, pairs)
        apart_far = far_block(1, 0, pairs)
        for pair in range(pairs):
            keep_state(1, pair, join_tile(load_state(1, pair), apart_far[pair]))
        return_near(
            0, [join_tile(load_state(0, pair), near_far[pair]) for pair in range(pairs)]
        )
        for pair in range(pairs):
            drain(in_sem.at[4 + pair], 4 * (tokens - tile))
            return_apart(1, pair, join(load_state(1, pair), edge(1, pair)))

    @pl.when(side == 1)
    def _():
        for pair in range(pairs):
            keep_state(1, pair, edge(1, pair))
        def join_below():
            drain(in_sem.at[3], 4 * (tokens - tile))
            for pair in range(pairs):
                keep_state(1, pair, join(load_state(1, pair), below_block(pair)))

        drain(in_sem.at[4], 4 * (tokens - tile) + 2 * tokens)

        first = (mine == 0) | (chip == chips - 1)

        @pl.when(jnp.logical_not(first))
        def _():
            join_below()

        wait_far()
        return_apart(0, 0, join_tile(edge(0, 0), far_block(0, 0, 1)[0]))

        def near_block():
            near_far = far_block(1, 0, pairs)
            return_near(
                1, [join_tile(load_state(1, pair), near_far[pair]) for pair in range(pairs)]
            )

        @pl.when(first)
        def _():
            join_below()

        @pl.when(chip < chips - 1)
        def _():
            near_block()

        drain(in_sem.at[5], 2 * tokens)
        return_apart(0, 1, join_tile(edge(0, 1), far_block(0, 1, 2)[0]))

        @pl.when(chip == chips - 1)
        def _():
            near_block()

    there = (1 - side) * half
    drain(back_sem.at[0], (half - 1) * 2 * tokens)
    for pair in range(pairs):
        drain(back_sem.at[1 + pair], 2 * tokens)
        for step in (2 * pair, 2 * pair + 1):
            owner = there + step
            out_ref[:, columns(owner)] = landed[:, columns(owner)].astype(jnp.float32)

    drain(send_sem.at[0], (inner - 1) * 3 * tokens)
    drain(send_sem.at[2], (half - 1) * 2 * tokens + half * tokens)
    for count in range(1, outer):

        @pl.when(outer - 1 - mine == count)
        def _():
            drain(send_sem.at[1], count * 2 * far_rows)


def fused(queries, key_rows, value_rows):
    tokens, features = queries.shape
    inner = lax.axis_size("inner")
    outer = lax.axis_size("outer")
    slab = features // inner
    tile = tokens // 4
    pairs = inner // 4
    any_space = pl.BlockSpec(memory_space=pl.ANY)
    dims = (inner, outer, tokens, slab, features // HEADS)
    return pl.pallas_call(
        partial(fused_kernel, dims),
        out_shape=pltpu.VMEM((tokens, features), jnp.float32),
        in_specs=[any_space] * 3,
        out_specs=pl.BlockSpec(memory_space=pltpu.VMEM),
        scratch_shapes=[
            *[pltpu.VMEM((tokens, features), jnp.bfloat16)] * 6,
            *[pltpu.VMEM((inner, tokens, slab), jnp.bfloat16)] * 3,
            *[pltpu.VMEM((outer - 1, inner, tile, slab), jnp.bfloat16)] * 2,
            pltpu.VMEM((3, 2, pairs, 4 * tokens, slab), jnp.float32),
            pltpu.VMEM((inner, tokens, slab), jnp.float32),
            pltpu.VMEM((inner, tokens, slab), jnp.bfloat16),
            pltpu.VMEM((tokens, features), jnp.bfloat16),
            pltpu.VMEM((inner * 2 * tokens, slab), jnp.float32),
            pltpu.SemaphoreType.DMA((3,)),
            pltpu.SemaphoreType.DMA((4 + pairs,)),
            pltpu.SemaphoreType.DMA((outer - 1,)),
            pltpu.SemaphoreType.DMA((1 + pairs,)),
            pltpu.SemaphoreType.DMA((3,)),
            pltpu.SemaphoreType.REGULAR((2,)),
        ],
        compiler_params=pltpu.CompilerParams(collective_id=0, has_side_effects=True),
    )(queries, key_rows, value_rows)


def device_program(queries, key_rows, value_rows):
    tokens, features = queries.shape
    inner = lax.axis_size("inner")
    outer = lax.axis_size("outer")
    width = features // HEADS
    fits = (
        inner * 2 == HEADS
        and outer > 1
        and inner % 4 == 0
        and width * 2 == 128
        and tokens % 64 == 0
        and inner * tokens <= 1024
        and (outer - 1) * inner * tokens // 4 <= 1024
    )
    if fits:
        return fused(queries, key_rows, value_rows)
    return on_device(queries, key_rows, value_rows)


def solution(mesh):
    placed = (P(("outer", "inner"), None), P(("outer", "inner"), None), P(("outer", "inner"), None))
    return jax.shard_map(
        device_program,
        mesh=mesh,
        in_specs=placed,
        out_specs=P(("outer", "inner"), None),
        check_vma=False,
    )
```

```python
import math
from functools import partial, reduce

import jax
import jax.numpy as jnp
import numpy as np
from jax import lax
from jax.experimental import pallas as pl
from jax.experimental.pallas import tpu as pltpu
from jax.sharding import PartitionSpec as P

HEADS = 16


FLOOR_SCORE = -1e30


def divisor_block(length, limit):
    extent = min(length, limit)
    while length % extent:
        extent -= 1
    return extent


def fresh_state(count, rows, width):
    return (
        jnp.full((count, rows), FLOOR_SCORE, jnp.float32),
        jnp.zeros((count, rows), jnp.float32),
        jnp.zeros((count, rows, width), jnp.float32),
    )


def finish_state(state):
    row_max, denominator, summed = state
    return (summed / denominator[..., None], row_max + jnp.log(denominator))


def online_step(state, query_rows, query_rank, key_rows, value_rows, key_rank):
    row_max, denominator, summed = state
    scale = query_rows.shape[-1] ** (-0.5)
    scores = (
        jnp.einsum("inh,ibh->inb", query_rows, key_rows, preferred_element_type=jnp.float32) * scale
    )
    scores = jnp.where(key_rank[None, None, :] <= query_rank[None, :, None], scores, FLOOR_SCORE)
    new_max = jnp.maximum(row_max, jnp.max(scores, axis=2))
    weights = jnp.exp(scores - new_max[..., None])
    rescale = jnp.exp(row_max - new_max)
    denominator = denominator * rescale + jnp.sum(weights, axis=2)
    summed = summed * rescale[..., None] + jnp.einsum(
        "inb,ibh->inh", weights.astype(jnp.bfloat16), value_rows, preferred_element_type=jnp.float32
    )
    return (new_max, denominator, summed)


def attend_keys(state, query_rows, query_rank, key_rows, value_rows, key_rank, stop=None):
    length = key_rows.shape[1]
    block = divisor_block(length, 512)

    def advance(index, carry):
        start = index * block
        piece_keys = lax.dynamic_slice_in_dim(key_rows, start, block, 1)
        piece_values = lax.dynamic_slice_in_dim(value_rows, start, block, 1)
        piece_rank = lax.dynamic_slice_in_dim(key_rank, start, block, 0)
        return online_step(carry, query_rows, query_rank, piece_keys, piece_values, piece_rank)

    upper = length // block if stop is None else stop
    return lax.fori_loop(0, upper, advance, state)


def attend(query_rows, query_rank, key_rows, value_rows, key_rank):
    count, length, width = query_rows.shape
    block = divisor_block(length, 512)
    steps = length // block
    query_split = query_rows.reshape(count, steps, block, width).swapaxes(0, 1)
    rank_split = query_rank.reshape(steps, block)

    def one_block(pieces):
        state = attend_keys(
            fresh_state(count, block, width),
            pieces[0],
            pieces[1],
            key_rows,
            value_rows,
            key_rank,
            pieces[2] + 1,
        )
        return finish_state(state)

    outputs, lses = lax.map(
        one_block, (query_split, rank_split, jnp.arange(steps, dtype=jnp.int32))
    )
    return (
        outputs.swapaxes(0, 1).reshape(count, length, width),
        lses.swapaxes(0, 1).reshape(count, length),
    )


def merge_levels(parts):
    row_max = reduce(jnp.maximum, [lse for _, lse in parts])
    weights = [jnp.exp(lse - row_max) for _, lse in parts]
    denominator = reduce(jnp.add, weights)
    summed = reduce(
        jnp.add, [weight[..., None] * output for weight, (output, _) in zip(weights, parts)]
    )
    return (summed / denominator[..., None], row_max + jnp.log(denominator))


def on_device(queries, key_rows, value_rows):
    tokens, features = queries.shape
    heads = HEADS
    width = features // heads
    outer_count = lax.axis_size("outer")
    inner_count = lax.axis_size("inner")
    outer_index = lax.axis_index("outer")
    inner_index = lax.axis_index("inner")
    per_device = 4 * heads // inner_count
    quarter = tokens // 4
    sixteenth = tokens // 16
    class_len = quarter * inner_count
    far_len = sixteenth * inner_count

    def to_items(array):
        return (
            array.reshape(quarter, 4, heads, width)
            .transpose(2, 1, 0, 3)
            .reshape(4 * heads, quarter, width)
        )

    local_ranks = jnp.arange(tokens, dtype=jnp.int32)
    head_major = [
        a.reshape(tokens, heads, width).transpose(1, 0, 2) for a in (queries, key_rows, value_rows)
    ]
    near_out, near_lse = attend(
        head_major[0], local_ranks, head_major[1], head_major[2], local_ranks
    )
    near_out = near_out.transpose(1, 0, 2)
    near_lse = near_lse.T
    item_index = inner_index * per_device + jnp.arange(per_device, dtype=jnp.int32)
    band = item_index // 16
    far_query_rank = outer_index * far_len + jnp.arange(far_len, dtype=jnp.int32)
    pick = np.array(
        [head * 16 + head // 4 * 4 + residue for head in range(heads) for residue in range(4)],
        np.int32,
    )

    def to_sixteen(array):
        spread = (
            array.reshape(sixteenth, 16, heads, width)
            .transpose(2, 1, 0, 3)
            .reshape(16 * heads, sixteenth, width)
        )
        return jnp.take(spread, pick, axis=0)

    gathered_k, gathered_v = (
        lax.all_gather(to_sixteen(key_rows), "outer", axis=1, tiled=True),
        lax.all_gather(to_sixteen(value_rows), "outer", axis=1, tiled=True),
    )
    mid_q, mid_k, mid_v, far_k, far_v = (
        lax.all_to_all(to_items(queries), "inner", split_axis=0, concat_axis=1, tiled=True),
        lax.all_to_all(to_items(key_rows), "inner", split_axis=0, concat_axis=1, tiled=True),
        lax.all_to_all(to_items(value_rows), "inner", split_axis=0, concat_axis=1, tiled=True),
        lax.all_to_all(gathered_k, "inner", split_axis=0, concat_axis=1, tiled=True),
        lax.all_to_all(gathered_v, "inner", split_axis=0, concat_axis=1, tiled=True),
    )
    split = mid_q.reshape(per_device, far_len, 4, width)
    picker = jnp.broadcast_to(band[:, None, None, None], (per_device, far_len, 1, width))
    far_q = jnp.take_along_axis(split, picker, axis=2)[:, :, 0, :]
    position = jnp.arange(far_k.shape[1], dtype=jnp.int32)
    far_key_rank = (
        position // sixteenth % outer_count * far_len
        + position // (outer_count * sixteenth) * sixteenth
        + position % sixteenth
    )
    far_state = attend_keys(
        fresh_state(per_device, far_len, width), far_q, far_query_rank, far_k, far_v, far_key_rank
    )
    far_out, far_lse = finish_state(far_state)
    class_ranks = jnp.arange(class_len, dtype=jnp.int32)
    mid_out, mid_lse = attend(mid_q, class_ranks, mid_k, mid_v, class_ranks)
    back_mid, back_mid_lse, back_far, back_far_lse = (
        lax.all_to_all(mid_out, "inner", split_axis=1, concat_axis=0, tiled=True),
        lax.all_to_all(mid_lse, "inner", split_axis=1, concat_axis=0, tiled=True),
        lax.all_to_all(far_out, "inner", split_axis=1, concat_axis=0, tiled=True),
        lax.all_to_all(far_lse, "inner", split_axis=1, concat_axis=0, tiled=True),
    )
    selector = np.array(
        [[band_index == head // 4 for band_index in range(4)] for head in range(heads)]
    )
    spread_out = jnp.where(
        selector[:, :, None, None, None], back_far.reshape(heads, 1, 4, sixteenth, width), 0.0
    )
    spread_lse = jnp.where(
        selector[:, :, None, None], back_far_lse.reshape(heads, 1, 4, sixteenth), FLOOR_SCORE
    )
    far_placed = (
        spread_out.reshape(heads, 16, sixteenth, width)
        .transpose(2, 1, 0, 3)
        .reshape(tokens, heads, width)
    )
    far_placed_lse = (
        spread_lse.reshape(heads, 16, sixteenth).transpose(2, 1, 0).reshape(tokens, heads)
    )
    placed = (
        back_mid.reshape(heads, 4, quarter, width)
        .transpose(2, 1, 0, 3)
        .reshape(tokens, heads, width)
    )
    placed_lse = back_mid_lse.reshape(heads, 4, quarter).transpose(2, 1, 0).reshape(tokens, heads)
    combined, _ = merge_levels(
        [(near_out, near_lse), (placed, placed_lse), (far_placed, far_placed_lse)]
    )
    return combined.reshape(tokens, features)


def fused_kernel(
    dims, q_ref, k_ref, v_ref, out_ref, q_held, k_held, v_held, q_rows, k_rows, v_rows, q_buf, k_buf, v_buf, far_k, far_v,
    state_ref, ready, ready_half, landed, side_k, side_v, local_ref, far_out, far_landed,
    spare, send_sem, in_sem, far_sem, back_sem, held_sem, stage_sem,
):
    inner, outer, tokens, slab, width = dims
    chips = inner // 2
    half = inner // 2
    pairs = half // 2
    run = tokens // 16
    tile = tokens // 4
    wide = slab * inner // 4
    me = lax.axis_index("inner")
    mine = lax.axis_index("outer")
    chip = me // 2
    core = lax.rem(me, 2)
    side = me // half
    band = me * 4 // inner
    mesh_id = pl.DeviceIdType.MESH
    sources = (k_ref, v_ref, q_ref)
    held = (k_held, v_held, q_held)
    placed = (k_rows, v_rows, q_rows)
    buffers = (k_buf, v_buf, q_buf)
    pick_k, pick_v, rest_k, rest_v, whole_q, pick_q = range(6)
    pieces = (
        (0, 0, tile),
        (1, 0, tile),
        (0, tile, tokens),
        (1, tile, tokens),
        (2, 0, tokens),
        (2, 0, tile),
    )

    def columns(index):
        return pl.ds(pl.multiple_of(index * slab, slab), slab)

    def drain(semaphore, rows):
        place = spare.at[0 : rows // 2]
        pltpu.make_async_copy(place, place, semaphore).wait()

    def inbound(which, peer, owner, arrival):
        array, start, stop = pieces[which]
        return pltpu.make_async_remote_copy(
            src_ref=placed[array].at[start:stop, columns(peer)],
            dst_ref=buffers[array].at[owner, start:stop, :],
            send_sem=send_sem.at[0],
            recv_sem=in_sem.at[arrival],
            device_id={"inner": peer},
            device_id_type=mesh_id,
        )

    def farbound(which, part, peer, owner):
        blocks = pl.ds(part * half, half)
        return pltpu.make_async_remote_copy(
            src_ref=buffers[which].at[blocks, 0:tile, :],
            dst_ref=(far_k, far_v)[which].at[owner, blocks],
            send_sem=send_sem.at[1],
            recv_sem=far_sem.at[owner],
            device_id={"outer": peer},
            device_id_type=mesh_id,
        )

    def backbound(peer, owner):
        return pltpu.make_async_remote_copy(
            src_ref=ready.at[peer],
            dst_ref=out_ref.at[:, columns(owner)],
            send_sem=send_sem.at[2],
            recv_sem=back_sem.at[0],
            device_id={"inner": peer},
            device_id_type=mesh_id,
        )

    def sidebound(which):
        return pltpu.make_async_remote_copy(
            src_ref=placed[which].at[:, half * slab : inner * slab],
            dst_ref=(side_k, side_v)[which],
            send_sem=send_sem.at[0],
            recv_sem=in_sem.at[6],
            device_id={"inner": 1},
            device_id_type=mesh_id,
        )

    def partbound(peer):
        return pltpu.make_async_remote_copy(
            src_ref=far_out.at[peer],
            dst_ref=far_landed.at[:, :, columns(me - half)],
            send_sem=send_sem.at[2],
            recv_sem=back_sem.at[1],
            device_id={"inner": peer},
            device_id_type=mesh_id,
        )

    def crossbound(peer, owner, arrival):
        return pltpu.make_async_remote_copy(
            src_ref=ready_half.at[peer],
            dst_ref=landed.at[:, columns(owner)],
            send_sem=send_sem.at[2],
            recv_sem=back_sem.at[arrival],
            device_id={"inner": peer},
            device_id_type=mesh_id,
        )

    own_held = [
        pltpu.make_async_copy(sources[which], held[which], held_sem.at[which]) for which in range(3)
    ]
    for copy in own_held:
        copy.start()

    barrier = pltpu.get_barrier_semaphore()
    partner = chip * 2 + 1 - core

    def greet(place):
        pl.semaphore_signal(barrier, inc=1, device_id=place, device_id_type=mesh_id)

    greet({"inner": partner})
    for step in range(1, outer):
        greet({"inner": chip * 2 + 1, "outer": lax.rem(mine + step, outer)})
    for other in range(chips):
        if other < chips // 2:
            counter = jnp.where(jnp.abs(chip - other) > 1, 1, 0)
        else:
            counter = jnp.where(chip > other, 1, 0)

        @pl.when(chip != other)
        def _():
            greet({"inner": other * 2 + counter})

    def row_place(shape, axis, first):
        row = lax.broadcasted_iota(jnp.int32, shape, axis)
        residue = 4 * lax.rem(first + row // tile, 4) + row % tile // run
        return row % run * 16 + residue

    square = (tokens, tokens)
    at_row = lax.broadcasted_iota(jnp.int32, square, 0)
    at_column = lax.broadcasted_iota(jnp.int32, square, 1)
    orders = [
        (row_place(square, 0, first) == at_column).astype(jnp.float32).astype(jnp.bfloat16)
        for first in range(4)
    ]

    def place_rows(which):
        own_held[which].wait()
        for first in range(4):
            place = slice(first * wide, (first + 1) * wide)
            placed[which][:, place] = jnp.dot(
                orders[first], held[which][:, place], preferred_element_type=jnp.float32
            ).astype(jnp.bfloat16)
        buffers[which][me] = placed[which][:, columns(me)]

    adjacent = jnp.where(chip == 0, 1, 2)
    near_count = 1 + 2 * jnp.where(side == 0, adjacent, chip)
    rest_count = 1 + 2 * (outer - 1) + 2 * (chips - 1 - jnp.where(side == 0, adjacent, chip))

    def pass_on(first, stage, count):
        @pl.when(core == first)
        def _():
            pl.semaphore_wait(barrier, count)
            pl.semaphore_signal(
                stage_sem.at[stage], inc=1, device_id={"inner": partner}, device_id_type=mesh_id
            )

        @pl.when(core != first)
        def _():
            pl.semaphore_wait(stage_sem.at[stage], 1)

    picks = (pick_k, pick_v)
    rest = (rest_k, rest_v)
    query = (whole_q,)

    def arrival_of(which, source, target):
        low = chips // 2
        apart = (source < low) != (target < low)
        if which in picks:
            return 2 if apart else 0
        if not apart:
            return 1
        if target < low:
            return 3 if which == whole_q else 4 + source % low
        if source == 0:
            return 4
        return 5 if which == whole_q else 3

    def send(source, batches):
        for group, targets in batches:
            for target in targets:
                for which in group:
                    for other in range(2):
                        arrival = arrival_of(which, source, target)
                        inbound(which, target * 2 + other, me, arrival).start()

    def send_partner(group):
        for which in group:
            inbound(which, partner, me, 0 if which in picks else 1).start()

    place_rows(0)
    place_rows(1)
    pass_on(0, 0, near_count)
    send_partner(picks + rest)

    @pl.when(chip == 0)
    def _():
        send(0, ((picks, (1,)), (rest, (1,))))

        @pl.when(core == 0)
        def _():
            for which in range(2):
                sidebound(which).start()


    @pl.when(chip == 1)
    def _():
        send(1, ((picks, (2, 0)), ((rest_k,), (2,)), (rest, (0,))))

    @pl.when(chip == 2)
    def _():
        send(2, ((picks, (0, 1)),))

    @pl.when(chip == 3)
    def _():
        send(3, ((picks, (0, 1, 2)),))

    place_rows(2)
    send_partner(query)

    @pl.when(chip == 0)
    def _():
        send(0, ((query, (1,)),))
        pass_on(1, 1, rest_count)
        send(0, ((picks, (3, 2)), ((pick_q,) + rest, (3, 2))))

    @pl.when(chip == 1)
    def _():
        send(1, ((query, (0,)),))
        pass_on(1, 1, rest_count)
        send(1, ((picks, (3,)), (rest, (3,)), ((rest_v,), (2,)), (query, (3, 2))))

    @pl.when(chip == 2)
    def _():
        send(2, ((query, (0, 1)),))
        pass_on(1, 1, rest_count)
        send(2, ((picks, (3,)), (rest, (0, 1)), (query, (3,)), (rest, (3,))))

    @pl.when(chip == 3)
    def _():
        send(3, ((query, (0, 1, 2)), (rest, (2,)), (rest, (0, 1))))

    @pl.when(me == 0)
    def _():
        side_k[...] = k_rows[:, half * slab : inner * slab]
        side_v[...] = v_rows[:, half * slab : inner * slab]

    for other in range(outer - 1):

        @pl.when(mine <= other)
        def _():
            far_k[other] = jnp.zeros((inner, tile, slab), jnp.bfloat16)
            far_v[other] = jnp.zeros((inner, tile, slab), jnp.bfloat16)

    def forward(part):
        for other in range(outer - 1, 0, -1):

            @pl.when(mine < other)
            def _():
                for which in range(2):
                    farbound(which, part, other, mine).start()

    same = at_row % tile // run == at_column % tile // run
    both = (at_row < tile) & (at_column < tile)
    below = jnp.where(same, jnp.where(both, 1.0, 0.0), FLOOR_SCORE)
    before = row_place(square, 1, band) <= row_place(square, 0, band)
    diagonal = jnp.where(
        before, jnp.where(same, jnp.where(both, math.log2(3.0), 1.0), 0.0), FLOOR_SCORE
    )
    never = jnp.full(square, FLOOR_SCORE, jnp.float32)

    def twice(table):
        return jnp.concatenate([table, table], axis=0)

    below_pair = twice(jnp.concatenate([below, below], axis=1))
    below_pair = jnp.concatenate([below_pair, below_pair], axis=0)
    edge_pair = jnp.concatenate(
        [jnp.concatenate([diagonal, never], axis=1), jnp.concatenate([below, diagonal], axis=1)], axis=0
    )
    edge_pair = twice(edge_pair)
    far_rows = inner * tile
    far_shape = (pairs * 4 * tile, (outer - 1) * far_rows)
    far_query = lax.broadcasted_iota(jnp.int32, far_shape, 0)
    far_key = lax.broadcasted_iota(jnp.int32, far_shape, 1)
    far_table = jnp.where(
        (far_query % tile // run == far_key % tile // run) & (far_key // far_rows < mine), 0.0, FLOOR_SCORE
    )
    factor = width ** (-0.5) * math.log2(math.e)
    contract = (((1,), (1,)), ((), ()))

    def by_head(rows):
        lane_head = lax.broadcasted_iota(jnp.int32, rows.shape, 1) // width
        return jnp.concatenate(
            [jnp.where(lane_head == head, rows, jnp.zeros_like(rows)) for head in range(2)], axis=0
        )

    def across(column):
        return jnp.broadcast_to(column, (column.shape[0], slab))

    def attend_part(rows, keys, values, table):
        scores = lax.dot_general(rows, keys, contract, preferred_element_type=jnp.float32)
        scores = scores * factor + table
        top = jnp.max(scores, axis=1, keepdims=True)
        weights = jnp.exp2(scores - top)
        total = jnp.sum(weights, axis=1, keepdims=True)
        summed = jnp.dot(weights.astype(jnp.bfloat16), values, preferred_element_type=jnp.float32)
        return across(top), across(total), summed

    def join(one, two):
        top = jnp.maximum(one[0], two[0])
        first = jnp.exp2(one[0] - top)
        second = jnp.exp2(two[0] - top)
        return top, one[1] * first + two[1] * second, one[2] * first + two[2] * second

    def join_tile(state, far):
        cut = [part.reshape(4, tokens, slab) for part in state]
        met = join([part[:, 0:tile] for part in cut], far)
        return [
            jnp.concatenate([new, old[:, tile:]], axis=1).reshape(4 * tokens, slab)
            for new, old in zip(met, cut)
        ]

    def load_state(index, pair):
        return [state_ref[which, index, pair] for which in range(3)]

    def keep_state(index, pair, state):
        for which in range(3):
            state_ref[which, index, pair] = state[which]

    def pair_queries(index, pair):
        rows = q_buf[index * half + 2 * pair : index * half + 2 * pair + 2]
        return by_head(rows.reshape(2 * tokens, slab))

    def span_of(buffer, start, stop):
        return buffer[start:stop].reshape((stop - start) * tokens, slab)

    def edge(index, pair):
        start = index * half
        stop = start + 2 * pair + 2
        table = jnp.concatenate([below_pair] * pair + [edge_pair], axis=1)
        return attend_part(
            pair_queries(index, pair), span_of(k_buf, start, stop), span_of(v_buf, start, stop), table
        )

    def below_block(pair):
        table = jnp.concatenate([below_pair] * pairs, axis=1)
        return attend_part(
            pair_queries(1, pair), span_of(k_buf, 0, half), span_of(v_buf, 0, half), table
        )

    def far_block(index, first, stop):
        span = stop - first
        rows = [
            by_head(
                q_buf[index * half + 2 * pair : index * half + 2 * pair + 2, 0:tile].reshape(2 * tile, slab)
            )
            for pair in range(first, stop)
        ]
        count = span * 4 * tile
        keys = far_k[...].reshape((outer - 1) * far_rows, slab)
        values = far_v[...].reshape((outer - 1) * far_rows, slab)
        state = attend_part(jnp.concatenate(rows, axis=0), keys, values, far_table[0:count])
        return [
            [part.reshape(span, 4, tile, slab)[place] for part in state] for place in range(span)
        ]

    pair_rows = (2 * tokens, 2 * tokens)
    natural = lax.broadcasted_iota(jnp.int32, pair_rows, 0)
    stored = lax.broadcasted_iota(jnp.int32, pair_rows, 1)
    stored_place = stored // tokens * tokens + row_place(pair_rows, 1, band) % tokens
    restore = (natural == stored_place).astype(jnp.float32).astype(jnp.bfloat16)
    lane_head = lax.broadcasted_iota(jnp.int32, (2 * tokens, slab), 1) // width

    def finish(state):
        total, summed = (part.reshape(2, 2 * tokens, slab) for part in state[1:])
        return jnp.where(lane_head == 0, summed[0], summed[1]) / jnp.where(
            lane_head == 0, total[0], total[1]
        )

    def restored(result, exact):
        coarse = result.astype(jnp.bfloat16)
        moved = jnp.dot(restore, coarse, preferred_element_type=jnp.float32)
        if exact:
            rest = (result - coarse.astype(jnp.float32)).astype(jnp.bfloat16)
            moved = moved + jnp.dot(restore, rest, preferred_element_type=jnp.float32)
        return moved.reshape(2, tokens, slab)

    def keep_exact(index, pair, state):
        moved = restored(finish(state), True)
        for step in range(2):
            ready[index * half + 2 * pair + step] = moved[step]

    def send_half(index, pair, state, arrival):
        moved = restored(finish(state), False).astype(jnp.bfloat16)
        for step in range(2):
            peer = index * half + 2 * pair + step
            ready_half[peer] = moved[step]
            crossbound(peer, me, arrival).start()

    head_lane = lax.broadcasted_iota(jnp.int32, (tokens, slab), 1) // width

    def local_part(place):
        first = (half + place) * 4 // inner
        at = slice((half + place) * slab, (half + place + 1) * slab)
        side_at = slice(place * slab, (place + 1) * slab)
        before = row_place(square, 1, first) <= row_place(square, 0, first)
        own = jnp.where(
            before, jnp.where(same, jnp.where(both, math.log2(3.0), 1.0), 0.0), FLOOR_SCORE
        )
        table = jnp.concatenate([jnp.where(core == 1, below, FLOOR_SCORE), own], axis=1)
        keys = jnp.concatenate([side_k[:, side_at], k_rows[:, at]], axis=0)
        values = jnp.concatenate([side_v[:, side_at], v_rows[:, at]], axis=0)
        state = attend_part(by_head(q_rows[:, at]), keys, values, twice(table))
        for which in range(3):
            local_ref[which, place] = jnp.where(
                head_lane == 0, state[which][0:tokens], state[which][tokens:]
            )

    tile_lane = lax.broadcasted_iota(jnp.int32, (tile, slab), 1)
    spread_row = lax.broadcasted_iota(jnp.int32, (slab, slab), 0)
    spread_column = lax.broadcasted_iota(jnp.int32, (slab, slab), 1)
    spread = jnp.where(
        (spread_row // width == spread_column // width)
        & (spread_row % (width // 4) == 0)
        & (spread_row % width < 3 * (width // 4)),
        1.0,
        0.0,
    ).astype(jnp.bfloat16)

    def far_part():
        top, total, summed = far_block(0, 0, 1)[0]
        lane = lax.broadcasted_iota(jnp.int32, (2, tile, slab), 2)
        top, total, summed = (
            jnp.where(lane < width, part[0:2], part[2:4]) for part in (top, total, summed)
        )
        lse = top + jnp.log2(total)
        place = lane % width // (width // 4)
        high = lse.astype(jnp.bfloat16).astype(jnp.float32)
        middle = (lse - high).astype(jnp.bfloat16).astype(jnp.float32)
        low = lse - high - middle
        packed = jnp.where(
            place == 0, high, jnp.where(place == 1, middle, jnp.where(place == 2, low, 0.0))
        )
        result = summed / total
        for peer in range(2):
            far_out[peer, 0] = result[peer].astype(jnp.bfloat16)
            far_out[peer, 1] = packed[peer].astype(jnp.bfloat16)
            partbound(peer).start()

    def local_join(place):
        at = slice(place * slab, (place + 1) * slab)
        result = far_landed[0, :, at].astype(jnp.float32)
        lse = jnp.dot(far_landed[1, :, at], spread, preferred_element_type=jnp.float32)
        top, total, summed = (local_ref[which, place, 0:tile] for which in range(3))
        top, total, summed = join((top, total, summed), (lse, jnp.ones_like(lse), result))
        local_ref[1, place, 0:tile] = total
        local_ref[2, place, 0:tile] = summed

    def local_finish(place):
        first = (half + place) * 4 // inner
        order = (at_row == row_place(square, 1, first)).astype(jnp.float32).astype(jnp.bfloat16)
        result = local_ref[2, place] / local_ref[1, place]
        coarse = result.astype(jnp.bfloat16)
        fine = (result - coarse.astype(jnp.float32)).astype(jnp.bfloat16)
        moved = jnp.dot(order, coarse, preferred_element_type=jnp.float32)
        moved = moved + jnp.dot(order, fine, preferred_element_type=jnp.float32)
        out_ref[:, (half + place) * slab : (half + place + 1) * slab] = moved

    drain(in_sem.at[0], (half - 1) * 2 * tile)

    @pl.when(chip == chips - 1)
    def _():
        pass_on(1, 1, rest_count)

    forward(side)

    @pl.when(chip == 0)
    def _():
        @pl.when(core == 1)
        def _():
            drain(in_sem.at[6], 2 * tokens * half)

        for place in range(half):
            local_part(place)

    drain(in_sem.at[2], half * 2 * tile)
    forward(1 - side)
    drain(in_sem.at[1], (half - 1) * (3 * tokens - 2 * tile))

    def wait_far():
        for other in range(outer - 1):

            @pl.when(mine > other)
            def _():
                drain(far_sem.at[other], 2 * far_rows)

    @pl.when(side == 0)
    def _():
        for pair in range(pairs):
            keep_state(0, pair, edge(0, pair))
        drain(in_sem.at[3], half * tokens)
        for pair in range(pairs):
            keep_state(1, pair, below_block(pair))
        wait_far()
        near_far = far_block(0, 0, pairs)
        apart_far = far_block(1, 0, pairs)
        for pair in range(pairs):
            keep_state(1, pair, join_tile(load_state(1, pair), apart_far[pair]))
        for pair in range(pairs):
            keep_exact(0, pair, join_tile(load_state(0, pair), near_far[pair]))
        for step in range(1, half):
            backbound(lax.rem(me + step, half), me).start()
        out_ref[:, columns(me)] = ready[me]
        for pair in range(pairs):
            drain(in_sem.at[4 + pair], 4 * (tokens - tile))
            send_half(1, pair, join(load_state(1, pair), edge(1, pair)), 1 + me // 2)

    @pl.when(side == 1)
    def _():
        for pair in range(pairs):
            keep_state(1, pair, edge(1, pair))

        drain(in_sem.at[4], 4 * (tokens - tile) + 2 * tile)
        drain(in_sem.at[3], 4 * (tokens - tile))
        for pair in range(pairs):
            keep_state(1, pair, join(load_state(1, pair), below_block(pair)))
        wait_far()

        @pl.when(mine > 0)
        def _():
            far_part()

        def near_block(own):
            away = 1 - own
            near_far = far_block(1, 0, pairs)
            send_half(1, away, join_tile(load_state(1, away), near_far[away]), 0)
            keep_exact(1, own, join_tile(load_state(1, own), near_far[own]))
            backbound(partner, me).start()
            out_ref[:, columns(me)] = ready[me]

        @pl.when(chip < chips - 1)
        def _():
            near_block(0)

        drain(in_sem.at[5], 2 * tokens)
        send_half(0, 1, join_tile(edge(0, 1), far_block(0, 1, 2)[0]), chip - 1)

        @pl.when(chip == chips - 1)
        def _():
            near_block(1)

    @pl.when(side == 0)
    def _():
        drain(back_sem.at[0], (half - 1) * 2 * tokens)

    @pl.when(side == 1)
    def _():
        drain(back_sem.at[0], 4 * tokens)
        for step in range(2):
            owner = (chips - 1 - chip + chips // 2) * 2 + step
            out_ref[:, columns(owner)] = landed[:, columns(owner)].astype(jnp.float32)

    @pl.when(chip == 0)
    def _():
        @pl.when(mine > 0)
        def _():
            drain(back_sem.at[1], half * 2 * tile)
            for place in range(half):
                local_join(place)

        for place in range(half):
            local_finish(place)

    @pl.when(chip > 0)
    def _():
        for pair in range(pairs):
            drain(back_sem.at[1 + pair], 2 * tokens)
            for step in (2 * pair, 2 * pair + 1):
                owner = (1 - side) * half + step
                out_ref[:, columns(owner)] = landed[:, columns(owner)].astype(jnp.float32)

        drain(send_sem.at[0], (inner - 1) * 3 * tokens)

    sent_near = (half - 1) * 3 * tokens + half * (2 * tokens + tile)

    @pl.when((chip == 0) & (core == 0))
    def _():
        drain(send_sem.at[0], sent_near + 2 * tokens * half)

    @pl.when((chip == 0) & (core == 1))
    def _():
        drain(send_sem.at[0], sent_near)

    @pl.when(side == 0)
    def _():
        drain(send_sem.at[2], (half - 1) * 2 * tokens + half * tokens)

    @pl.when((side == 1) & (mine == 0))
    def _():
        drain(send_sem.at[2], 6 * tokens)

    @pl.when((side == 1) & (mine > 0))
    def _():
        drain(send_sem.at[2], 6 * tokens + 4 * tile)

    for count in range(1, outer):

        @pl.when(outer - 1 - mine == count)
        def _():
            drain(send_sem.at[1], count * 2 * far_rows)


def fused(queries, key_rows, value_rows):
    tokens, features = queries.shape
    inner = lax.axis_size("inner")
    outer = lax.axis_size("outer")
    slab = features // inner
    tile = tokens // 4
    pairs = inner // 4
    any_space = pl.BlockSpec(memory_space=pl.ANY)
    dims = (inner, outer, tokens, slab, features // HEADS)
    return pl.pallas_call(
        partial(fused_kernel, dims),
        out_shape=pltpu.VMEM((tokens, features), jnp.float32),
        in_specs=[any_space] * 3,
        out_specs=pl.BlockSpec(memory_space=pltpu.VMEM),
        scratch_shapes=[
            *[pltpu.VMEM((tokens, features), jnp.bfloat16)] * 6,
            *[pltpu.VMEM((inner, tokens, slab), jnp.bfloat16)] * 3,
            *[pltpu.VMEM((outer - 1, inner, tile, slab), jnp.bfloat16)] * 2,
            pltpu.VMEM((3, 2, pairs, 4 * tokens, slab), jnp.float32),
            pltpu.VMEM((inner, tokens, slab), jnp.float32),
            pltpu.VMEM((inner, tokens, slab), jnp.bfloat16),
            pltpu.VMEM((tokens, features), jnp.bfloat16),
            *[pltpu.VMEM((tokens, features // 2), jnp.bfloat16)] * 2,
            pltpu.VMEM((3, inner // 2, tokens, slab), jnp.float32),
            pltpu.VMEM((2, 2, tile, slab), jnp.bfloat16),
            pltpu.VMEM((2, tile, features // 2), jnp.bfloat16),
            pltpu.VMEM((inner * 2 * tokens, slab), jnp.float32),
            pltpu.SemaphoreType.DMA((3,)),
            pltpu.SemaphoreType.DMA((5 + pairs,)),
            pltpu.SemaphoreType.DMA((outer - 1,)),
            pltpu.SemaphoreType.DMA((1 + pairs,)),
            pltpu.SemaphoreType.DMA((3,)),
            pltpu.SemaphoreType.REGULAR((2,)),
        ],
        compiler_params=pltpu.CompilerParams(collective_id=0, has_side_effects=True),
    )(queries, key_rows, value_rows)


def device_program(queries, key_rows, value_rows):
    tokens, features = queries.shape
    inner = lax.axis_size("inner")
    outer = lax.axis_size("outer")
    width = features // HEADS
    fits = (
        inner * 2 == HEADS
        and outer > 1
        and inner % 4 == 0
        and width * 2 == 128
        and tokens % 64 == 0
        and inner * tokens <= 1024
        and (outer - 1) * inner * tokens // 4 <= 1024
    )
    if fits:
        return fused(queries, key_rows, value_rows)
    return on_device(queries, key_rows, value_rows)


def solution(mesh):
    placed = (P(("outer", "inner"), None), P(("outer", "inner"), None), P(("outer", "inner"), None))
    return jax.shard_map(
        device_program,
        mesh=mesh,
        in_specs=placed,
        out_specs=P(("outer", "inner"), None),
        check_vma=False,
    )
```

```python
import math
from functools import partial, reduce

import jax
import jax.numpy as jnp
import numpy as np
from jax import lax
from jax.experimental import pallas as pl
from jax.experimental.pallas import tpu as pltpu
from jax.sharding import PartitionSpec as P

HEADS = 16


FLOOR_SCORE = -1e30


def divisor_block(length, limit):
    extent = min(length, limit)
    while length % extent:
        extent -= 1
    return extent


def fresh_state(count, rows, width):
    return (
        jnp.full((count, rows), FLOOR_SCORE, jnp.float32),
        jnp.zeros((count, rows), jnp.float32),
        jnp.zeros((count, rows, width), jnp.float32),
    )


def finish_state(state):
    row_max, denominator, summed = state
    return (summed / denominator[..., None], row_max + jnp.log(denominator))


def online_step(state, query_rows, query_rank, key_rows, value_rows, key_rank):
    row_max, denominator, summed = state
    scale = query_rows.shape[-1] ** (-0.5)
    scores = (
        jnp.einsum("inh,ibh->inb", query_rows, key_rows, preferred_element_type=jnp.float32) * scale
    )
    scores = jnp.where(key_rank[None, None, :] <= query_rank[None, :, None], scores, FLOOR_SCORE)
    new_max = jnp.maximum(row_max, jnp.max(scores, axis=2))
    weights = jnp.exp(scores - new_max[..., None])
    rescale = jnp.exp(row_max - new_max)
    denominator = denominator * rescale + jnp.sum(weights, axis=2)
    summed = summed * rescale[..., None] + jnp.einsum(
        "inb,ibh->inh", weights.astype(jnp.bfloat16), value_rows, preferred_element_type=jnp.float32
    )
    return (new_max, denominator, summed)


def attend_keys(state, query_rows, query_rank, key_rows, value_rows, key_rank, stop=None):
    length = key_rows.shape[1]
    block = divisor_block(length, 512)

    def advance(index, carry):
        start = index * block
        piece_keys = lax.dynamic_slice_in_dim(key_rows, start, block, 1)
        piece_values = lax.dynamic_slice_in_dim(value_rows, start, block, 1)
        piece_rank = lax.dynamic_slice_in_dim(key_rank, start, block, 0)
        return online_step(carry, query_rows, query_rank, piece_keys, piece_values, piece_rank)

    upper = length // block if stop is None else stop
    return lax.fori_loop(0, upper, advance, state)


def attend(query_rows, query_rank, key_rows, value_rows, key_rank):
    count, length, width = query_rows.shape
    block = divisor_block(length, 512)
    steps = length // block
    query_split = query_rows.reshape(count, steps, block, width).swapaxes(0, 1)
    rank_split = query_rank.reshape(steps, block)

    def one_block(pieces):
        state = attend_keys(
            fresh_state(count, block, width),
            pieces[0],
            pieces[1],
            key_rows,
            value_rows,
            key_rank,
            pieces[2] + 1,
        )
        return finish_state(state)

    outputs, lses = lax.map(
        one_block, (query_split, rank_split, jnp.arange(steps, dtype=jnp.int32))
    )
    return (
        outputs.swapaxes(0, 1).reshape(count, length, width),
        lses.swapaxes(0, 1).reshape(count, length),
    )


def merge_levels(parts):
    row_max = reduce(jnp.maximum, [lse for _, lse in parts])
    weights = [jnp.exp(lse - row_max) for _, lse in parts]
    denominator = reduce(jnp.add, weights)
    summed = reduce(
        jnp.add, [weight[..., None] * output for weight, (output, _) in zip(weights, parts)]
    )
    return (summed / denominator[..., None], row_max + jnp.log(denominator))


def on_device(queries, key_rows, value_rows):
    tokens, features = queries.shape
    heads = HEADS
    width = features // heads
    outer_count = lax.axis_size("outer")
    inner_count = lax.axis_size("inner")
    outer_index = lax.axis_index("outer")
    inner_index = lax.axis_index("inner")
    per_device = 4 * heads // inner_count
    quarter = tokens // 4
    sixteenth = tokens // 16
    class_len = quarter * inner_count
    far_len = sixteenth * inner_count

    def to_items(array):
        return (
            array.reshape(quarter, 4, heads, width)
            .transpose(2, 1, 0, 3)
            .reshape(4 * heads, quarter, width)
        )

    local_ranks = jnp.arange(tokens, dtype=jnp.int32)
    head_major = [
        a.reshape(tokens, heads, width).transpose(1, 0, 2) for a in (queries, key_rows, value_rows)
    ]
    near_out, near_lse = attend(
        head_major[0], local_ranks, head_major[1], head_major[2], local_ranks
    )
    near_out = near_out.transpose(1, 0, 2)
    near_lse = near_lse.T
    item_index = inner_index * per_device + jnp.arange(per_device, dtype=jnp.int32)
    band = item_index // 16
    far_query_rank = outer_index * far_len + jnp.arange(far_len, dtype=jnp.int32)
    pick = np.array(
        [head * 16 + head // 4 * 4 + residue for head in range(heads) for residue in range(4)],
        np.int32,
    )

    def to_sixteen(array):
        spread = (
            array.reshape(sixteenth, 16, heads, width)
            .transpose(2, 1, 0, 3)
            .reshape(16 * heads, sixteenth, width)
        )
        return jnp.take(spread, pick, axis=0)

    gathered_k, gathered_v = (
        lax.all_gather(to_sixteen(key_rows), "outer", axis=1, tiled=True),
        lax.all_gather(to_sixteen(value_rows), "outer", axis=1, tiled=True),
    )
    mid_q, mid_k, mid_v, far_k, far_v = (
        lax.all_to_all(to_items(queries), "inner", split_axis=0, concat_axis=1, tiled=True),
        lax.all_to_all(to_items(key_rows), "inner", split_axis=0, concat_axis=1, tiled=True),
        lax.all_to_all(to_items(value_rows), "inner", split_axis=0, concat_axis=1, tiled=True),
        lax.all_to_all(gathered_k, "inner", split_axis=0, concat_axis=1, tiled=True),
        lax.all_to_all(gathered_v, "inner", split_axis=0, concat_axis=1, tiled=True),
    )
    split = mid_q.reshape(per_device, far_len, 4, width)
    picker = jnp.broadcast_to(band[:, None, None, None], (per_device, far_len, 1, width))
    far_q = jnp.take_along_axis(split, picker, axis=2)[:, :, 0, :]
    position = jnp.arange(far_k.shape[1], dtype=jnp.int32)
    far_key_rank = (
        position // sixteenth % outer_count * far_len
        + position // (outer_count * sixteenth) * sixteenth
        + position % sixteenth
    )
    far_state = attend_keys(
        fresh_state(per_device, far_len, width), far_q, far_query_rank, far_k, far_v, far_key_rank
    )
    far_out, far_lse = finish_state(far_state)
    class_ranks = jnp.arange(class_len, dtype=jnp.int32)
    mid_out, mid_lse = attend(mid_q, class_ranks, mid_k, mid_v, class_ranks)
    back_mid, back_mid_lse, back_far, back_far_lse = (
        lax.all_to_all(mid_out, "inner", split_axis=1, concat_axis=0, tiled=True),
        lax.all_to_all(mid_lse, "inner", split_axis=1, concat_axis=0, tiled=True),
        lax.all_to_all(far_out, "inner", split_axis=1, concat_axis=0, tiled=True),
        lax.all_to_all(far_lse, "inner", split_axis=1, concat_axis=0, tiled=True),
    )
    selector = np.array(
        [[band_index == head // 4 for band_index in range(4)] for head in range(heads)]
    )
    spread_out = jnp.where(
        selector[:, :, None, None, None], back_far.reshape(heads, 1, 4, sixteenth, width), 0.0
    )
    spread_lse = jnp.where(
        selector[:, :, None, None], back_far_lse.reshape(heads, 1, 4, sixteenth), FLOOR_SCORE
    )
    far_placed = (
        spread_out.reshape(heads, 16, sixteenth, width)
        .transpose(2, 1, 0, 3)
        .reshape(tokens, heads, width)
    )
    far_placed_lse = (
        spread_lse.reshape(heads, 16, sixteenth).transpose(2, 1, 0).reshape(tokens, heads)
    )
    placed = (
        back_mid.reshape(heads, 4, quarter, width)
        .transpose(2, 1, 0, 3)
        .reshape(tokens, heads, width)
    )
    placed_lse = back_mid_lse.reshape(heads, 4, quarter).transpose(2, 1, 0).reshape(tokens, heads)
    combined, _ = merge_levels(
        [(near_out, near_lse), (placed, placed_lse), (far_placed, far_placed_lse)]
    )
    return combined.reshape(tokens, features)


def fused_kernel(
    dims, q_ref, k_ref, v_ref, out_ref, q_held, k_held, v_held, q_rows, k_rows, v_rows, q_buf, k_buf, v_buf, far_k, far_v,
    state_ref, ready, ready_half, landed, side_k, side_v, local_ref, far_out, far_landed,
    spare, send_sem, in_sem, far_sem, back_sem, held_sem, stage_sem,
):
    inner, outer, tokens, slab, width = dims
    chips = inner // 2
    half = inner // 2
    pairs = half // 2
    run = tokens // 16
    tile = tokens // 4
    wide = slab * inner // 4
    me = lax.axis_index("inner")
    mine = lax.axis_index("outer")
    chip = me // 2
    core = lax.rem(me, 2)
    side = me // half
    band = me * 4 // inner
    mesh_id = pl.DeviceIdType.MESH
    sources = (k_ref, v_ref, q_ref)
    held = (k_held, v_held, q_held)
    placed = (k_rows, v_rows, q_rows)
    buffers = (k_buf, v_buf, q_buf)
    pick_k, pick_v, rest_k, rest_v, whole_q, pick_q = range(6)
    pieces = (
        (0, 0, tile),
        (1, 0, tile),
        (0, tile, tokens),
        (1, tile, tokens),
        (2, 0, tokens),
        (2, 0, tile),
    )

    def columns(index):
        return pl.ds(pl.multiple_of(index * slab, slab), slab)

    def drain(semaphore, rows):
        place = spare.at[0 : rows // 2]
        pltpu.make_async_copy(place, place, semaphore).wait()

    def inbound(which, peer, owner, arrival):
        array, start, stop = pieces[which]
        return pltpu.make_async_remote_copy(
            src_ref=placed[array].at[start:stop, columns(peer)],
            dst_ref=buffers[array].at[owner, start:stop, :],
            send_sem=send_sem.at[0],
            recv_sem=in_sem.at[arrival],
            device_id={"inner": peer},
            device_id_type=mesh_id,
        )

    def farbound(which, part, peer, owner):
        blocks = pl.ds(part * half, half)
        return pltpu.make_async_remote_copy(
            src_ref=buffers[which].at[blocks, 0:tile, :],
            dst_ref=(far_k, far_v)[which].at[owner, blocks],
            send_sem=send_sem.at[1],
            recv_sem=far_sem.at[owner],
            device_id={"outer": peer},
            device_id_type=mesh_id,
        )

    def backbound(peer, owner):
        return pltpu.make_async_remote_copy(
            src_ref=ready.at[peer],
            dst_ref=out_ref.at[:, columns(owner)],
            send_sem=send_sem.at[2],
            recv_sem=back_sem.at[0],
            device_id={"inner": peer},
            device_id_type=mesh_id,
        )

    def sidebound(which):
        return pltpu.make_async_remote_copy(
            src_ref=placed[which].at[:, half * slab : inner * slab],
            dst_ref=(side_k, side_v)[which],
            send_sem=send_sem.at[0],
            recv_sem=in_sem.at[6],
            device_id={"inner": 1},
            device_id_type=mesh_id,
        )

    def partbound(peer):
        return pltpu.make_async_remote_copy(
            src_ref=far_out.at[peer],
            dst_ref=far_landed.at[:, :, columns(me - half)],
            send_sem=send_sem.at[2],
            recv_sem=back_sem.at[1],
            device_id={"inner": peer},
            device_id_type=mesh_id,
        )

    def crossbound(peer, owner, arrival):
        return pltpu.make_async_remote_copy(
            src_ref=ready_half.at[peer],
            dst_ref=landed.at[:, columns(owner)],
            send_sem=send_sem.at[2],
            recv_sem=back_sem.at[arrival],
            device_id={"inner": peer},
            device_id_type=mesh_id,
        )

    own_held = [
        pltpu.make_async_copy(sources[which], held[which], held_sem.at[which]) for which in range(3)
    ]
    for copy in own_held:
        copy.start()

    barrier = pltpu.get_barrier_semaphore()
    partner = chip * 2 + 1 - core

    def greet(place):
        pl.semaphore_signal(barrier, inc=1, device_id=place, device_id_type=mesh_id)

    greet({"inner": partner})
    for step in range(1, outer):
        greet({"inner": chip * 2 + 1, "outer": lax.rem(mine + step, outer)})
    for other in range(chips):
        if other < chips // 2:
            counter = jnp.where(jnp.abs(chip - other) > 1, 1, 0)
        else:
            counter = jnp.where((chip > other) & (mine > 0), 1, 0)

        @pl.when(chip != other)
        def _():
            greet({"inner": other * 2 + counter})

    def row_place(shape, axis, first):
        row = lax.broadcasted_iota(jnp.int32, shape, axis)
        residue = 4 * lax.rem(first + row // tile, 4) + row % tile // run
        return row % run * 16 + residue

    square = (tokens, tokens)
    at_row = lax.broadcasted_iota(jnp.int32, square, 0)
    at_column = lax.broadcasted_iota(jnp.int32, square, 1)
    orders = [
        (row_place(square, 0, first) == at_column).astype(jnp.float32).astype(jnp.bfloat16)
        for first in range(4)
    ]

    def place_rows(which):
        own_held[which].wait()
        for first in range(4):
            place = slice(first * wide, (first + 1) * wide)
            placed[which][:, place] = jnp.dot(
                orders[first], held[which][:, place], preferred_element_type=jnp.float32
            ).astype(jnp.bfloat16)
        buffers[which][me] = placed[which][:, columns(me)]

    adjacent = jnp.where(chip == 0, 1, 2)
    near_chips = jnp.where(side == 0, adjacent, jnp.where(mine == 0, chips - 1, chip))
    near_count = 1 + 2 * near_chips
    rest_count = 1 + 2 * (outer - 1) + 2 * (chips - 1 - near_chips)

    def pass_on(first, stage, count):
        @pl.when(core == first)
        def _():
            pl.semaphore_wait(barrier, count)
            pl.semaphore_signal(
                stage_sem.at[stage], inc=1, device_id={"inner": partner}, device_id_type=mesh_id
            )

        @pl.when(core != first)
        def _():
            pl.semaphore_wait(stage_sem.at[stage], 1)

    picks = (pick_k, pick_v)
    rest = (rest_k, rest_v)
    query = (whole_q,)

    def arrival_of(which, source, target):
        low = chips // 2
        apart = (source < low) != (target < low)
        if which in picks:
            return 2 if apart else 0
        if not apart:
            return 1
        if target < low:
            return 3 if which == whole_q else 4 + source % low
        if source == 0:
            return 4
        return 5 if which == whole_q else 3

    def send(source, batches):
        for group, targets in batches:
            for target in targets:
                for other in range(2):
                    for which in group:
                        arrival = arrival_of(which, source, target)
                        inbound(which, target * 2 + other, me, arrival).start()

    def send_partner(group):
        for which in group:
            inbound(which, partner, me, 0 if which in picks else 1).start()

    place_rows(0)
    place_rows(1)
    pass_on(0, 0, near_count)
    send_partner(picks + rest)

    @pl.when(chip == 0)
    def _():
        send(0, ((picks, (1,)), (rest, (1,))))

        @pl.when(core == 0)
        def _():
            for which in range(2):
                sidebound(which).start()


    @pl.when(chip == 1)
    def _():
        send(1, ((picks, (2, 0)), ((rest_k,), (2,)), (rest, (0,))))

    @pl.when(chip == 2)
    def _():
        send(2, ((picks, (0, 1)),))

    @pl.when(chip == 3)
    def _():
        send(3, ((picks, (0, 1, 2)),))

    place_rows(2)
    send_partner(query)

    @pl.when(chip == 0)
    def _():
        send(0, ((query, (1,)),))
        pass_on(1, 1, rest_count)
        send(0, ((picks, (3, 2)), ((pick_q,) + rest, (3, 2))))

    @pl.when(chip == 1)
    def _():
        send(1, ((query, (0,)),))
        pass_on(1, 1, rest_count)
        send(1, ((picks, (3,)), (rest, (3,)), ((rest_v,), (2,)), (query, (3, 2))))

    @pl.when(chip == 2)
    def _():
        @pl.when(mine == 0)
        def _():
            send(2, ((query, (0, 1)),))

        @pl.when(mine > 0)
        def _():
            pass_on(1, 1, rest_count)

        send(2, ((picks, (3,)),))

        @pl.when(mine > 0)
        def _():
            send(2, ((query, (0, 1)),))

        send(2, ((rest, (0, 1)), (query, (3,)), (rest, (3,))))

        @pl.when(mine == 0)
        def _():
            pass_on(1, 1, rest_count)


    @pl.when(chip == 3)
    def _():
        send(3, ((query, (0, 1, 2)), (rest, (2,)), (rest, (0, 1))))
        pass_on(1, 1, rest_count)

    @pl.when(me == 0)
    def _():
        side_k[...] = k_rows[:, half * slab : inner * slab]
        side_v[...] = v_rows[:, half * slab : inner * slab]

    for other in range(outer - 1):

        @pl.when(mine <= other)
        def _():
            far_k[other] = jnp.zeros((inner, tile, slab), jnp.bfloat16)
            far_v[other] = jnp.zeros((inner, tile, slab), jnp.bfloat16)

    def forward(part):
        for other in range(outer - 1, 0, -1):

            @pl.when(mine < other)
            def _():
                for which in range(2):
                    farbound(which, part, other, mine).start()

    same = at_row % tile // run == at_column % tile // run
    both = (at_row < tile) & (at_column < tile)
    below = jnp.where(same, jnp.where(both, 1.0, 0.0), FLOOR_SCORE)
    before = row_place(square, 1, band) <= row_place(square, 0, band)
    diagonal = jnp.where(
        before, jnp.where(same, jnp.where(both, math.log2(3.0), 1.0), 0.0), FLOOR_SCORE
    )
    never = jnp.full(square, FLOOR_SCORE, jnp.float32)

    def twice(table):
        return jnp.concatenate([table, table], axis=0)

    below_pair = twice(jnp.concatenate([below, below], axis=1))
    below_pair = jnp.concatenate([below_pair, below_pair], axis=0)
    edge_pair = jnp.concatenate(
        [jnp.concatenate([diagonal, never], axis=1), jnp.concatenate([below, diagonal], axis=1)], axis=0
    )
    edge_pair = twice(edge_pair)
    far_rows = inner * tile
    far_shape = (pairs * 4 * tile, (outer - 1) * far_rows)
    far_query = lax.broadcasted_iota(jnp.int32, far_shape, 0)
    far_key = lax.broadcasted_iota(jnp.int32, far_shape, 1)
    far_table = jnp.where(
        (far_query % tile // run == far_key % tile // run) & (far_key // far_rows < mine), 0.0, FLOOR_SCORE
    )
    factor = width ** (-0.5) * math.log2(math.e)
    contract = (((1,), (1,)), ((), ()))

    def by_head(rows):
        lane_head = lax.broadcasted_iota(jnp.int32, rows.shape, 1) // width
        return jnp.concatenate(
            [jnp.where(lane_head == head, rows, jnp.zeros_like(rows)) for head in range(2)], axis=0
        )

    def across(column):
        return jnp.broadcast_to(column, (column.shape[0], slab))

    def attend_part(rows, keys, values, table):
        scores = lax.dot_general(rows, keys, contract, preferred_element_type=jnp.float32)
        scores = scores * factor + table
        top = jnp.max(scores, axis=1, keepdims=True)
        weights = jnp.exp2(scores - top)
        total = jnp.sum(weights, axis=1, keepdims=True)
        summed = jnp.dot(weights.astype(jnp.bfloat16), values, preferred_element_type=jnp.float32)
        return across(top), across(total), summed

    def join(one, two):
        top = jnp.maximum(one[0], two[0])
        first = jnp.exp2(one[0] - top)
        second = jnp.exp2(two[0] - top)
        return top, one[1] * first + two[1] * second, one[2] * first + two[2] * second

    def join_tile(state, far):
        cut = [part.reshape(4, tokens, slab) for part in state]
        met = join([part[:, 0:tile] for part in cut], far)
        return [
            jnp.concatenate([new, old[:, tile:]], axis=1).reshape(4 * tokens, slab)
            for new, old in zip(met, cut)
        ]

    def load_state(index, pair):
        return [state_ref[which, index, pair] for which in range(3)]

    def keep_state(index, pair, state):
        for which in range(3):
            state_ref[which, index, pair] = state[which]

    def pair_queries(index, pair):
        rows = q_buf[index * half + 2 * pair : index * half + 2 * pair + 2]
        return by_head(rows.reshape(2 * tokens, slab))

    def span_of(buffer, start, stop):
        return buffer[start:stop].reshape((stop - start) * tokens, slab)

    def edge(index, pair):
        start = index * half
        stop = start + 2 * pair + 2
        table = jnp.concatenate([below_pair] * pair + [edge_pair], axis=1)
        return attend_part(
            pair_queries(index, pair), span_of(k_buf, start, stop), span_of(v_buf, start, stop), table
        )

    def below_block(pair):
        table = jnp.concatenate([below_pair] * pairs, axis=1)
        return attend_part(
            pair_queries(1, pair), span_of(k_buf, 0, half), span_of(v_buf, 0, half), table
        )

    def far_block(index, first, stop):
        span = stop - first
        rows = [
            by_head(
                q_buf[index * half + 2 * pair : index * half + 2 * pair + 2, 0:tile].reshape(2 * tile, slab)
            )
            for pair in range(first, stop)
        ]
        count = span * 4 * tile
        keys = far_k[...].reshape((outer - 1) * far_rows, slab)
        values = far_v[...].reshape((outer - 1) * far_rows, slab)
        state = attend_part(jnp.concatenate(rows, axis=0), keys, values, far_table[0:count])
        return [
            [part.reshape(span, 4, tile, slab)[place] for part in state] for place in range(span)
        ]

    pair_rows = (2 * tokens, 2 * tokens)
    natural = lax.broadcasted_iota(jnp.int32, pair_rows, 0)
    stored = lax.broadcasted_iota(jnp.int32, pair_rows, 1)
    stored_place = stored // tokens * tokens + row_place(pair_rows, 1, band) % tokens
    restore = (natural == stored_place).astype(jnp.float32).astype(jnp.bfloat16)
    lane_head = lax.broadcasted_iota(jnp.int32, (2 * tokens, slab), 1) // width

    def finish(state):
        total, summed = (part.reshape(2, 2 * tokens, slab) for part in state[1:])
        return jnp.where(lane_head == 0, summed[0], summed[1]) / jnp.where(
            lane_head == 0, total[0], total[1]
        )

    def restored(result, exact):
        coarse = result.astype(jnp.bfloat16)
        moved = jnp.dot(restore, coarse, preferred_element_type=jnp.float32)
        if exact:
            rest = (result - coarse.astype(jnp.float32)).astype(jnp.bfloat16)
            moved = moved + jnp.dot(restore, rest, preferred_element_type=jnp.float32)
        return moved.reshape(2, tokens, slab)

    def keep_exact(index, pair, state):
        moved = restored(finish(state), True)
        for step in range(2):
            ready[index * half + 2 * pair + step] = moved[step]

    def send_half(index, pair, state, arrival):
        moved = restored(finish(state), False).astype(jnp.bfloat16)
        for step in range(2):
            peer = index * half + 2 * pair + step
            ready_half[peer] = moved[step]
            crossbound(peer, me, arrival).start()

    head_lane = lax.broadcasted_iota(jnp.int32, (tokens, slab), 1) // width

    def local_part(place):
        first = (half + place) * 4 // inner
        at = slice((half + place) * slab, (half + place + 1) * slab)
        side_at = slice(place * slab, (place + 1) * slab)
        before = row_place(square, 1, first) <= row_place(square, 0, first)
        own = jnp.where(
            before, jnp.where(same, jnp.where(both, math.log2(3.0), 1.0), 0.0), FLOOR_SCORE
        )
        table = jnp.concatenate([jnp.where(core == 1, below, FLOOR_SCORE), own], axis=1)
        keys = jnp.concatenate([side_k[:, side_at], k_rows[:, at]], axis=0)
        values = jnp.concatenate([side_v[:, side_at], v_rows[:, at]], axis=0)
        state = attend_part(by_head(q_rows[:, at]), keys, values, twice(table))
        for which in range(3):
            local_ref[which, place] = jnp.where(
                head_lane == 0, state[which][0:tokens], state[which][tokens:]
            )

    tile_lane = lax.broadcasted_iota(jnp.int32, (tile, slab), 1)
    spread_row = lax.broadcasted_iota(jnp.int32, (slab, slab), 0)
    spread_column = lax.broadcasted_iota(jnp.int32, (slab, slab), 1)
    spread = jnp.where(
        (spread_row // width == spread_column // width)
        & (spread_row % (width // 4) == 0)
        & (spread_row % width < 3 * (width // 4)),
        1.0,
        0.0,
    ).astype(jnp.bfloat16)

    def far_part():
        top, total, summed = far_block(0, 0, 1)[0]
        lane = lax.broadcasted_iota(jnp.int32, (2, tile, slab), 2)
        top, total, summed = (
            jnp.where(lane < width, part[0:2], part[2:4]) for part in (top, total, summed)
        )
        lse = top + jnp.log2(total)
        place = lane % width // (width // 4)
        high = lse.astype(jnp.bfloat16).astype(jnp.float32)
        middle = (lse - high).astype(jnp.bfloat16).astype(jnp.float32)
        low = lse - high - middle
        packed = jnp.where(
            place == 0, high, jnp.where(place == 1, middle, jnp.where(place == 2, low, 0.0))
        )
        result = summed / total
        for peer in range(2):
            far_out[peer, 0] = result[peer].astype(jnp.bfloat16)
            far_out[peer, 1] = packed[peer].astype(jnp.bfloat16)
            partbound(peer).start()

    def local_join(place):
        at = slice(place * slab, (place + 1) * slab)
        result = far_landed[0, :, at].astype(jnp.float32)
        lse = jnp.dot(far_landed[1, :, at], spread, preferred_element_type=jnp.float32)
        top, total, summed = (local_ref[which, place, 0:tile] for which in range(3))
        top, total, summed = join((top, total, summed), (lse, jnp.ones_like(lse), result))
        local_ref[1, place, 0:tile] = total
        local_ref[2, place, 0:tile] = summed

    def local_finish(place):
        first = (half + place) * 4 // inner
        order = (at_row == row_place(square, 1, first)).astype(jnp.float32).astype(jnp.bfloat16)
        result = local_ref[2, place] / local_ref[1, place]
        coarse = result.astype(jnp.bfloat16)
        fine = (result - coarse.astype(jnp.float32)).astype(jnp.bfloat16)
        moved = jnp.dot(order, coarse, preferred_element_type=jnp.float32)
        moved = moved + jnp.dot(order, fine, preferred_element_type=jnp.float32)
        out_ref[:, (half + place) * slab : (half + place + 1) * slab] = moved

    drain(in_sem.at[0], (half - 1) * 2 * tile)

    forward(side)

    @pl.when(chip == 0)
    def _():
        @pl.when(core == 1)
        def _():
            drain(in_sem.at[6], 2 * tokens * half)

        for place in range(half):
            local_part(place)

    drain(in_sem.at[2], half * 2 * tile)
    forward(1 - side)
    drain(in_sem.at[1], (half - 1) * (3 * tokens - 2 * tile))

    def wait_far():
        for other in range(outer - 1):

            @pl.when(mine > other)
            def _():
                drain(far_sem.at[other], 2 * far_rows)

    @pl.when(side == 0)
    def _():
        for pair in range(pairs):
            keep_state(0, pair, edge(0, pair))
        drain(in_sem.at[3], half * tokens)
        for pair in range(pairs):
            keep_state(1, pair, below_block(pair))
        wait_far()
        near_far = far_block(0, 0, pairs)
        apart_far = far_block(1, 0, pairs)
        for pair in range(pairs):
            keep_state(1, pair, join_tile(load_state(1, pair), apart_far[pair]))
        for pair in range(pairs):
            keep_exact(0, pair, join_tile(load_state(0, pair), near_far[pair]))
        for step in range(1, half):
            backbound(lax.rem(me + step, half), me).start()
        out_ref[:, columns(me)] = ready[me]
        for pair in range(pairs):
            drain(in_sem.at[4 + pair], 4 * (tokens - tile))
            send_half(1, pair, join(load_state(1, pair), edge(1, pair)), 1 + me // 2)

    @pl.when(side == 1)
    def _():
        for pair in range(pairs):
            keep_state(1, pair, edge(1, pair))

        drain(in_sem.at[4], 4 * (tokens - tile) + 2 * tile)
        drain(in_sem.at[3], 4 * (tokens - tile))
        for pair in range(pairs):
            keep_state(1, pair, join(load_state(1, pair), below_block(pair)))
        wait_far()

        @pl.when(mine > 0)
        def _():
            far_part()

        def near_block(own):
            away = 1 - own
            near_far = far_block(1, 0, pairs)
            send_half(1, away, join_tile(load_state(1, away), near_far[away]), 0)
            keep_exact(1, own, join_tile(load_state(1, own), near_far[own]))
            backbound(partner, me).start()
            out_ref[:, columns(me)] = ready[me]

        @pl.when(chip < chips - 1)
        def _():
            near_block(0)

        drain(in_sem.at[5], 2 * tokens)
        send_half(0, 1, join_tile(edge(0, 1), far_block(0, 1, 2)[0]), chip - 1)

        @pl.when(chip == chips - 1)
        def _():
            near_block(1)

    @pl.when(side == 0)
    def _():
        drain(back_sem.at[0], (half - 1) * 2 * tokens)

    @pl.when(side == 1)
    def _():
        drain(back_sem.at[0], 4 * tokens)
        for step in range(2):
            owner = (chips - 1 - chip + chips // 2) * 2 + step
            out_ref[:, columns(owner)] = landed[:, columns(owner)].astype(jnp.float32)

    @pl.when(chip == 0)
    def _():
        @pl.when(mine > 0)
        def _():
            drain(back_sem.at[1], half * 2 * tile)
            for place in range(half):
                local_join(place)

        for place in range(half):
            local_finish(place)

    @pl.when(chip > 0)
    def _():
        for pair in range(pairs):
            drain(back_sem.at[1 + pair], 2 * tokens)
            for step in (2 * pair, 2 * pair + 1):
                owner = (1 - side) * half + step
                out_ref[:, columns(owner)] = landed[:, columns(owner)].astype(jnp.float32)

        drain(send_sem.at[0], (inner - 1) * 3 * tokens)

    sent_near = (half - 1) * 3 * tokens + half * (2 * tokens + tile)

    @pl.when((chip == 0) & (core == 0))
    def _():
        drain(send_sem.at[0], sent_near + 2 * tokens * half)

    @pl.when((chip == 0) & (core == 1))
    def _():
        drain(send_sem.at[0], sent_near)

    @pl.when(side == 0)
    def _():
        drain(send_sem.at[2], (half - 1) * 2 * tokens + half * tokens)

    @pl.when((side == 1) & (mine == 0))
    def _():
        drain(send_sem.at[2], 6 * tokens)

    @pl.when((side == 1) & (mine > 0))
    def _():
        drain(send_sem.at[2], 6 * tokens + 4 * tile)

    for count in range(1, outer):

        @pl.when(outer - 1 - mine == count)
        def _():
            drain(send_sem.at[1], count * 2 * far_rows)


def fused(queries, key_rows, value_rows):
    tokens, features = queries.shape
    inner = lax.axis_size("inner")
    outer = lax.axis_size("outer")
    slab = features // inner
    tile = tokens // 4
    pairs = inner // 4
    any_space = pl.BlockSpec(memory_space=pl.ANY)
    dims = (inner, outer, tokens, slab, features // HEADS)
    return pl.pallas_call(
        partial(fused_kernel, dims),
        out_shape=pltpu.VMEM((tokens, features), jnp.float32),
        in_specs=[any_space] * 3,
        out_specs=pl.BlockSpec(memory_space=pltpu.VMEM),
        scratch_shapes=[
            *[pltpu.VMEM((tokens, features), jnp.bfloat16)] * 6,
            *[pltpu.VMEM((inner, tokens, slab), jnp.bfloat16)] * 3,
            *[pltpu.VMEM((outer - 1, inner, tile, slab), jnp.bfloat16)] * 2,
            pltpu.VMEM((3, 2, pairs, 4 * tokens, slab), jnp.float32),
            pltpu.VMEM((inner, tokens, slab), jnp.float32),
            pltpu.VMEM((inner, tokens, slab), jnp.bfloat16),
            pltpu.VMEM((tokens, features), jnp.bfloat16),
            *[pltpu.VMEM((tokens, features // 2), jnp.bfloat16)] * 2,
            pltpu.VMEM((3, inner // 2, tokens, slab), jnp.float32),
            pltpu.VMEM((2, 2, tile, slab), jnp.bfloat16),
            pltpu.VMEM((2, tile, features // 2), jnp.bfloat16),
            pltpu.VMEM((inner * 2 * tokens, slab), jnp.float32),
            pltpu.SemaphoreType.DMA((3,)),
            pltpu.SemaphoreType.DMA((5 + pairs,)),
            pltpu.SemaphoreType.DMA((outer - 1,)),
            pltpu.SemaphoreType.DMA((1 + pairs,)),
            pltpu.SemaphoreType.DMA((3,)),
            pltpu.SemaphoreType.REGULAR((2,)),
        ],
        compiler_params=pltpu.CompilerParams(collective_id=0, has_side_effects=True),
    )(queries, key_rows, value_rows)


def device_program(queries, key_rows, value_rows):
    tokens, features = queries.shape
    inner = lax.axis_size("inner")
    outer = lax.axis_size("outer")
    width = features // HEADS
    fits = (
        inner * 2 == HEADS
        and outer > 1
        and inner % 4 == 0
        and width * 2 == 128
        and tokens % 64 == 0
        and inner * tokens <= 1024
        and (outer - 1) * inner * tokens // 4 <= 1024
    )
    if fits:
        return fused(queries, key_rows, value_rows)
    return on_device(queries, key_rows, value_rows)


def solution(mesh):
    placed = (P(("outer", "inner"), None), P(("outer", "inner"), None), P(("outer", "inner"), None))
    return jax.shard_map(
        device_program,
        mesh=mesh,
        in_specs=placed,
        out_specs=P(("outer", "inner"), None),
        check_vma=False,
    )
```

```python
import math
from functools import partial, reduce

import jax
import jax.numpy as jnp
import numpy as np
from jax import lax
from jax.experimental import pallas as pl
from jax.experimental.pallas import tpu as pltpu
from jax.sharding import PartitionSpec as P

HEADS = 16


FLOOR_SCORE = -1e30


def divisor_block(length, limit):
    extent = min(length, limit)
    while length % extent:
        extent -= 1
    return extent


def fresh_state(count, rows, width):
    return (
        jnp.full((count, rows), FLOOR_SCORE, jnp.float32),
        jnp.zeros((count, rows), jnp.float32),
        jnp.zeros((count, rows, width), jnp.float32),
    )


def finish_state(state):
    row_max, denominator, summed = state
    return (summed / denominator[..., None], row_max + jnp.log(denominator))


def online_step(state, query_rows, query_rank, key_rows, value_rows, key_rank):
    row_max, denominator, summed = state
    scale = query_rows.shape[-1] ** (-0.5)
    scores = (
        jnp.einsum("inh,ibh->inb", query_rows, key_rows, preferred_element_type=jnp.float32) * scale
    )
    scores = jnp.where(key_rank[None, None, :] <= query_rank[None, :, None], scores, FLOOR_SCORE)
    new_max = jnp.maximum(row_max, jnp.max(scores, axis=2))
    weights = jnp.exp(scores - new_max[..., None])
    rescale = jnp.exp(row_max - new_max)
    denominator = denominator * rescale + jnp.sum(weights, axis=2)
    summed = summed * rescale[..., None] + jnp.einsum(
        "inb,ibh->inh", weights.astype(jnp.bfloat16), value_rows, preferred_element_type=jnp.float32
    )
    return (new_max, denominator, summed)


def attend_keys(state, query_rows, query_rank, key_rows, value_rows, key_rank, stop=None):
    length = key_rows.shape[1]
    block = divisor_block(length, 512)

    def advance(index, carry):
        start = index * block
        piece_keys = lax.dynamic_slice_in_dim(key_rows, start, block, 1)
        piece_values = lax.dynamic_slice_in_dim(value_rows, start, block, 1)
        piece_rank = lax.dynamic_slice_in_dim(key_rank, start, block, 0)
        return online_step(carry, query_rows, query_rank, piece_keys, piece_values, piece_rank)

    upper = length // block if stop is None else stop
    return lax.fori_loop(0, upper, advance, state)


def attend(query_rows, query_rank, key_rows, value_rows, key_rank):
    count, length, width = query_rows.shape
    block = divisor_block(length, 512)
    steps = length // block
    query_split = query_rows.reshape(count, steps, block, width).swapaxes(0, 1)
    rank_split = query_rank.reshape(steps, block)

    def one_block(pieces):
        state = attend_keys(
            fresh_state(count, block, width),
            pieces[0],
            pieces[1],
            key_rows,
            value_rows,
            key_rank,
            pieces[2] + 1,
        )
        return finish_state(state)

    outputs, lses = lax.map(
        one_block, (query_split, rank_split, jnp.arange(steps, dtype=jnp.int32))
    )
    return (
        outputs.swapaxes(0, 1).reshape(count, length, width),
        lses.swapaxes(0, 1).reshape(count, length),
    )


def merge_levels(parts):
    row_max = reduce(jnp.maximum, [lse for _, lse in parts])
    weights = [jnp.exp(lse - row_max) for _, lse in parts]
    denominator = reduce(jnp.add, weights)
    summed = reduce(
        jnp.add, [weight[..., None] * output for weight, (output, _) in zip(weights, parts)]
    )
    return (summed / denominator[..., None], row_max + jnp.log(denominator))


def on_device(queries, key_rows, value_rows):
    tokens, features = queries.shape
    heads = HEADS
    width = features // heads
    outer_count = lax.axis_size("outer")
    inner_count = lax.axis_size("inner")
    outer_index = lax.axis_index("outer")
    inner_index = lax.axis_index("inner")
    per_device = 4 * heads // inner_count
    quarter = tokens // 4
    sixteenth = tokens // 16
    class_len = quarter * inner_count
    far_len = sixteenth * inner_count

    def to_items(array):
        return (
            array.reshape(quarter, 4, heads, width)
            .transpose(2, 1, 0, 3)
            .reshape(4 * heads, quarter, width)
        )

    local_ranks = jnp.arange(tokens, dtype=jnp.int32)
    head_major = [
        a.reshape(tokens, heads, width).transpose(1, 0, 2) for a in (queries, key_rows, value_rows)
    ]
    near_out, near_lse = attend(
        head_major[0], local_ranks, head_major[1], head_major[2], local_ranks
    )
    near_out = near_out.transpose(1, 0, 2)
    near_lse = near_lse.T
    item_index = inner_index * per_device + jnp.arange(per_device, dtype=jnp.int32)
    band = item_index // 16
    far_query_rank = outer_index * far_len + jnp.arange(far_len, dtype=jnp.int32)
    pick = np.array(
        [head * 16 + head // 4 * 4 + residue for head in range(heads) for residue in range(4)],
        np.int32,
    )

    def to_sixteen(array):
        spread = (
            array.reshape(sixteenth, 16, heads, width)
            .transpose(2, 1, 0, 3)
            .reshape(16 * heads, sixteenth, width)
        )
        return jnp.take(spread, pick, axis=0)

    gathered_k, gathered_v = (
        lax.all_gather(to_sixteen(key_rows), "outer", axis=1, tiled=True),
        lax.all_gather(to_sixteen(value_rows), "outer", axis=1, tiled=True),
    )
    mid_q, mid_k, mid_v, far_k, far_v = (
        lax.all_to_all(to_items(queries), "inner", split_axis=0, concat_axis=1, tiled=True),
        lax.all_to_all(to_items(key_rows), "inner", split_axis=0, concat_axis=1, tiled=True),
        lax.all_to_all(to_items(value_rows), "inner", split_axis=0, concat_axis=1, tiled=True),
        lax.all_to_all(gathered_k, "inner", split_axis=0, concat_axis=1, tiled=True),
        lax.all_to_all(gathered_v, "inner", split_axis=0, concat_axis=1, tiled=True),
    )
    split = mid_q.reshape(per_device, far_len, 4, width)
    picker = jnp.broadcast_to(band[:, None, None, None], (per_device, far_len, 1, width))
    far_q = jnp.take_along_axis(split, picker, axis=2)[:, :, 0, :]
    position = jnp.arange(far_k.shape[1], dtype=jnp.int32)
    far_key_rank = (
        position // sixteenth % outer_count * far_len
        + position // (outer_count * sixteenth) * sixteenth
        + position % sixteenth
    )
    far_state = attend_keys(
        fresh_state(per_device, far_len, width), far_q, far_query_rank, far_k, far_v, far_key_rank
    )
    far_out, far_lse = finish_state(far_state)
    class_ranks = jnp.arange(class_len, dtype=jnp.int32)
    mid_out, mid_lse = attend(mid_q, class_ranks, mid_k, mid_v, class_ranks)
    back_mid, back_mid_lse, back_far, back_far_lse = (
        lax.all_to_all(mid_out, "inner", split_axis=1, concat_axis=0, tiled=True),
        lax.all_to_all(mid_lse, "inner", split_axis=1, concat_axis=0, tiled=True),
        lax.all_to_all(far_out, "inner", split_axis=1, concat_axis=0, tiled=True),
        lax.all_to_all(far_lse, "inner", split_axis=1, concat_axis=0, tiled=True),
    )
    selector = np.array(
        [[band_index == head // 4 for band_index in range(4)] for head in range(heads)]
    )
    spread_out = jnp.where(
        selector[:, :, None, None, None], back_far.reshape(heads, 1, 4, sixteenth, width), 0.0
    )
    spread_lse = jnp.where(
        selector[:, :, None, None], back_far_lse.reshape(heads, 1, 4, sixteenth), FLOOR_SCORE
    )
    far_placed = (
        spread_out.reshape(heads, 16, sixteenth, width)
        .transpose(2, 1, 0, 3)
        .reshape(tokens, heads, width)
    )
    far_placed_lse = (
        spread_lse.reshape(heads, 16, sixteenth).transpose(2, 1, 0).reshape(tokens, heads)
    )
    placed = (
        back_mid.reshape(heads, 4, quarter, width)
        .transpose(2, 1, 0, 3)
        .reshape(tokens, heads, width)
    )
    placed_lse = back_mid_lse.reshape(heads, 4, quarter).transpose(2, 1, 0).reshape(tokens, heads)
    combined, _ = merge_levels(
        [(near_out, near_lse), (placed, placed_lse), (far_placed, far_placed_lse)]
    )
    return combined.reshape(tokens, features)


def fused_kernel(
    dims, q_ref, k_ref, v_ref, out_ref, q_held, k_held, v_held, q_rows, k_rows, v_rows, q_buf, k_buf, v_buf, far_k, far_v,
    state_ref, ready, ready_half, landed, side_k, side_v, local_ref, far_out, far_landed, part_out, part_landed,
    spare, send_sem, in_sem, far_sem, back_sem, held_sem, stage_sem,
):
    inner, outer, tokens, slab, width = dims
    chips = inner // 2
    half = inner // 2
    pairs = half // 2
    run = tokens // 16
    tile = tokens // 4
    wide = slab * inner // 4
    me = lax.axis_index("inner")
    mine = lax.axis_index("outer")
    chip = me // 2
    core = lax.rem(me, 2)
    side = me // half
    band = me * 4 // inner
    mesh_id = pl.DeviceIdType.MESH
    sources = (k_ref, v_ref, q_ref)
    held = (k_held, v_held, q_held)
    placed = (k_rows, v_rows, q_rows)
    buffers = (k_buf, v_buf, q_buf)
    pick_k, pick_v, rest_k, rest_v, whole_q, pick_q = range(6)
    pieces = (
        (0, 0, tile),
        (1, 0, tile),
        (0, tile, tokens),
        (1, tile, tokens),
        (2, 0, tokens),
        (2, 0, tile),
    )

    def columns(index):
        return pl.ds(pl.multiple_of(index * slab, slab), slab)

    def drain(semaphore, rows):
        place = spare.at[0 : rows // 2]
        pltpu.make_async_copy(place, place, semaphore).wait()

    def inbound(which, peer, owner, arrival):
        array, start, stop = pieces[which]
        return pltpu.make_async_remote_copy(
            src_ref=placed[array].at[start:stop, columns(peer)],
            dst_ref=buffers[array].at[owner, start:stop, :],
            send_sem=send_sem.at[0],
            recv_sem=in_sem.at[arrival],
            device_id={"inner": peer},
            device_id_type=mesh_id,
        )

    def farbound(which, part, peer, owner):
        blocks = pl.ds(part * half, half)
        return pltpu.make_async_remote_copy(
            src_ref=buffers[which].at[blocks, 0:tile, :],
            dst_ref=(far_k, far_v)[which].at[owner, blocks],
            send_sem=send_sem.at[1],
            recv_sem=far_sem.at[owner],
            device_id={"outer": peer},
            device_id_type=mesh_id,
        )

    def backbound(peer, owner):
        return pltpu.make_async_remote_copy(
            src_ref=ready.at[peer],
            dst_ref=out_ref.at[:, columns(owner)],
            send_sem=send_sem.at[2],
            recv_sem=back_sem.at[0],
            device_id={"inner": peer},
            device_id_type=mesh_id,
        )

    def apart_columns(base):
        return slice(base * slab, (base + half) * slab)

    def sidebound(which, base, peer):
        return pltpu.make_async_remote_copy(
            src_ref=placed[which].at[:, apart_columns(base)],
            dst_ref=(side_k, side_v)[which],
            send_sem=send_sem.at[0],
            recv_sem=in_sem.at[6],
            device_id={"inner": peer},
            device_id_type=mesh_id,
        )

    def partbound(peer):
        return pltpu.make_async_remote_copy(
            src_ref=far_out.at[peer],
            dst_ref=far_landed.at[:, :, columns(me - half)],
            send_sem=send_sem.at[2],
            recv_sem=back_sem.at[1],
            device_id={"inner": peer},
            device_id_type=mesh_id,
        )

    def lastbound(step):
        return pltpu.make_async_remote_copy(
            src_ref=part_out.at[step],
            dst_ref=part_landed.at[:, columns(me)],
            send_sem=send_sem.at[2],
            recv_sem=back_sem.at[1],
            device_id={"inner": inner - 2 + step},
            device_id_type=mesh_id,
        )

    def crossbound(peer, owner, arrival):
        return pltpu.make_async_remote_copy(
            src_ref=ready_half.at[peer],
            dst_ref=landed.at[:, columns(owner)],
            send_sem=send_sem.at[2],
            recv_sem=back_sem.at[arrival],
            device_id={"inner": peer},
            device_id_type=mesh_id,
        )

    own_held = [
        pltpu.make_async_copy(sources[which], held[which], held_sem.at[which]) for which in range(3)
    ]
    for copy in own_held:
        copy.start()

    barrier = pltpu.get_barrier_semaphore()
    partner = chip * 2 + 1 - core

    def greet(place):
        pl.semaphore_signal(barrier, inc=1, device_id=place, device_id_type=mesh_id)

    greet({"inner": partner})
    for step in range(1, outer):
        greet({"inner": chip * 2 + 1, "outer": lax.rem(mine + step, outer)})
    for other in range(chips):
        if other < chips // 2:
            counter = jnp.where(jnp.abs(chip - other) > 1, 1, 0)
        else:
            counter = jnp.where((chip > other) & (mine > 0), 1, 0)

        @pl.when(chip != other)
        def _():
            greet({"inner": other * 2 + counter})

    def row_place(shape, axis, first):
        row = lax.broadcasted_iota(jnp.int32, shape, axis)
        residue = 4 * lax.rem(first + row // tile, 4) + row % tile // run
        return row % run * 16 + residue

    square = (tokens, tokens)
    at_row = lax.broadcasted_iota(jnp.int32, square, 0)
    at_column = lax.broadcasted_iota(jnp.int32, square, 1)
    orders = [
        (row_place(square, 0, first) == at_column).astype(jnp.float32).astype(jnp.bfloat16)
        for first in range(4)
    ]

    def place_rows(which):
        own_held[which].wait()
        for first in range(4):
            place = slice(first * wide, (first + 1) * wide)
            placed[which][:, place] = jnp.dot(
                orders[first], held[which][:, place], preferred_element_type=jnp.float32
            ).astype(jnp.bfloat16)
        buffers[which][me] = placed[which][:, columns(me)]

    adjacent = jnp.where(chip == 0, 1, 2)
    near_chips = jnp.where(side == 0, adjacent, jnp.where(mine == 0, chips - 1, chip))
    near_count = 1 + 2 * near_chips
    rest_count = 1 + 2 * (outer - 1) + 2 * (chips - 1 - near_chips)

    def pass_on(first, stage, count):
        @pl.when(core == first)
        def _():
            pl.semaphore_wait(barrier, count)
            pl.semaphore_signal(
                stage_sem.at[stage], inc=1, device_id={"inner": partner}, device_id_type=mesh_id
            )

        @pl.when(core != first)
        def _():
            pl.semaphore_wait(stage_sem.at[stage], 1)

    picks = (pick_k, pick_v)
    rest = (rest_k, rest_v)
    query = (whole_q,)

    def arrival_of(which, source, target):
        low = chips // 2
        apart = (source < low) != (target < low)
        if which in picks:
            return 2 if apart else 0
        if not apart:
            return 1
        if target < low:
            return 3 if which == whole_q else 4 + source % low
        if source == 0:
            return 4
        return 5 if which == whole_q else 3

    def send(source, batches):
        for group, targets in batches:
            for target in targets:
                for other in range(2):
                    for which in group:
                        arrival = arrival_of(which, source, target)
                        inbound(which, target * 2 + other, me, arrival).start()

    def send_partner(group):
        for which in group:
            inbound(which, partner, me, 0 if which in picks else 1).start()

    place_rows(0)
    place_rows(1)
    pass_on(0, 0, near_count)
    send_partner(picks + rest)

    @pl.when(chip == 0)
    def _():
        send(0, ((picks, (1,)), (rest, (1,))))

        @pl.when(core == 0)
        def _():
            for which in range(2):
                sidebound(which, half, 1).start()


    @pl.when(chip == 1)
    def _():
        send(1, ((picks, (2, 0)), ((rest_k,), (2,)), (rest, (0,))))

    @pl.when(chip == 2)
    def _():
        send(2, ((picks, (0, 1)),))

    @pl.when(chip == 3)
    def _():
        send(3, ((picks, (0, 1, 2)),))

    place_rows(2)
    send_partner(query)

    @pl.when(chip == 0)
    def _():
        send(0, ((query, (1,)),))
        pass_on(1, 1, rest_count)
        send(0, ((picks, (3, 2)), ((pick_q,) + rest, (3, 2))))

    @pl.when(chip == 1)
    def _():
        send(1, ((query, (0,)),))
        pass_on(1, 1, rest_count)
        send(1, ((picks, (3,)), (rest, (3,)), ((rest_v,), (2,)), (query, (3, 2))))

    @pl.when(chip == 2)
    def _():
        @pl.when(mine == 0)
        def _():
            send(2, ((query, (0, 1)),))

        @pl.when(mine > 0)
        def _():
            pass_on(1, 1, rest_count)

        send(2, ((picks, (3,)),))

        @pl.when(mine > 0)
        def _():
            send(2, ((query, (0, 1)),))

        send(2, ((rest, (0, 1)), (query, (3,)), (rest, (3,))))

        @pl.when(mine == 0)
        def _():
            pass_on(1, 1, rest_count)


    @pl.when(chip == 3)
    def _():
        send(3, ((query, (0, 1, 2)), (rest, (2,))))

        @pl.when(core == 0)
        def _():
            for which in range(2):
                sidebound(which, 0, inner - 1).start()

        pass_on(1, 1, rest_count)

    for place, base in ((0, half), (inner - 2, 0)):

        @pl.when(me == place)
        def _():
            side_k[...] = k_rows[:, apart_columns(base)]
            side_v[...] = v_rows[:, apart_columns(base)]

    for other in range(outer - 1):

        @pl.when(mine <= other)
        def _():
            far_k[other] = jnp.zeros((inner, tile, slab), jnp.bfloat16)
            far_v[other] = jnp.zeros((inner, tile, slab), jnp.bfloat16)

    def forward(part):
        for other in range(outer - 1, 0, -1):

            @pl.when(mine < other)
            def _():
                for which in range(2):
                    farbound(which, part, other, mine).start()

    same = at_row % tile // run == at_column % tile // run
    both = (at_row < tile) & (at_column < tile)
    below = jnp.where(same, jnp.where(both, 1.0, 0.0), FLOOR_SCORE)
    before = row_place(square, 1, band) <= row_place(square, 0, band)
    diagonal = jnp.where(
        before, jnp.where(same, jnp.where(both, math.log2(3.0), 1.0), 0.0), FLOOR_SCORE
    )
    never = jnp.full(square, FLOOR_SCORE, jnp.float32)

    def twice(table):
        return jnp.concatenate([table, table], axis=0)

    below_pair = twice(jnp.concatenate([below, below], axis=1))
    below_pair = jnp.concatenate([below_pair, below_pair], axis=0)
    edge_pair = jnp.concatenate(
        [jnp.concatenate([diagonal, never], axis=1), jnp.concatenate([below, diagonal], axis=1)], axis=0
    )
    edge_pair = twice(edge_pair)
    far_rows = inner * tile
    far_shape = (pairs * 4 * tile, (outer - 1) * far_rows)
    far_query = lax.broadcasted_iota(jnp.int32, far_shape, 0)
    far_key = lax.broadcasted_iota(jnp.int32, far_shape, 1)
    far_table = jnp.where(
        (far_query % tile // run == far_key % tile // run) & (far_key // far_rows < mine), 0.0, FLOOR_SCORE
    )
    factor = width ** (-0.5) * math.log2(math.e)
    contract = (((1,), (1,)), ((), ()))

    def by_head(rows):
        lane_head = lax.broadcasted_iota(jnp.int32, rows.shape, 1) // width
        return jnp.concatenate(
            [jnp.where(lane_head == head, rows, jnp.zeros_like(rows)) for head in range(2)], axis=0
        )

    def across(column):
        return jnp.broadcast_to(column, (column.shape[0], slab))

    def attend_part(rows, keys, values, table):
        scores = lax.dot_general(rows, keys, contract, preferred_element_type=jnp.float32)
        scores = scores * factor + table
        top = jnp.max(scores, axis=1, keepdims=True)
        weights = jnp.exp2(scores - top)
        total = jnp.sum(weights, axis=1, keepdims=True)
        summed = jnp.dot(weights.astype(jnp.bfloat16), values, preferred_element_type=jnp.float32)
        return across(top), across(total), summed

    def join(one, two):
        top = jnp.maximum(one[0], two[0])
        first = jnp.exp2(one[0] - top)
        second = jnp.exp2(two[0] - top)
        return top, one[1] * first + two[1] * second, one[2] * first + two[2] * second

    def join_tile(state, far):
        cut = [part.reshape(4, tokens, slab) for part in state]
        met = join([part[:, 0:tile] for part in cut], far)
        return [
            jnp.concatenate([new, old[:, tile:]], axis=1).reshape(4 * tokens, slab)
            for new, old in zip(met, cut)
        ]

    def load_state(index, pair):
        return [state_ref[which, index, pair] for which in range(3)]

    def keep_state(index, pair, state):
        for which in range(3):
            state_ref[which, index, pair] = state[which]

    def pair_queries(index, pair):
        rows = q_buf[index * half + 2 * pair : index * half + 2 * pair + 2]
        return by_head(rows.reshape(2 * tokens, slab))

    def span_of(buffer, start, stop):
        return buffer[start:stop].reshape((stop - start) * tokens, slab)

    def edge(index, pair):
        start = index * half
        stop = start + 2 * pair + 2
        table = jnp.concatenate([below_pair] * pair + [edge_pair], axis=1)
        return attend_part(
            pair_queries(index, pair), span_of(k_buf, start, stop), span_of(v_buf, start, stop), table
        )

    def below_block(pair):
        table = jnp.concatenate([below_pair] * pairs, axis=1)
        return attend_part(
            pair_queries(1, pair), span_of(k_buf, 0, half), span_of(v_buf, 0, half), table
        )

    def far_block(index, first, stop):
        span = stop - first
        rows = [
            by_head(
                q_buf[index * half + 2 * pair : index * half + 2 * pair + 2, 0:tile].reshape(2 * tile, slab)
            )
            for pair in range(first, stop)
        ]
        count = span * 4 * tile
        keys = far_k[...].reshape((outer - 1) * far_rows, slab)
        values = far_v[...].reshape((outer - 1) * far_rows, slab)
        state = attend_part(jnp.concatenate(rows, axis=0), keys, values, far_table[0:count])
        return [
            [part.reshape(span, 4, tile, slab)[place] for part in state] for place in range(span)
        ]

    pair_rows = (2 * tokens, 2 * tokens)
    natural = lax.broadcasted_iota(jnp.int32, pair_rows, 0)
    stored = lax.broadcasted_iota(jnp.int32, pair_rows, 1)
    stored_place = stored // tokens * tokens + row_place(pair_rows, 1, band) % tokens
    restore = (natural == stored_place).astype(jnp.float32).astype(jnp.bfloat16)
    lane_head = lax.broadcasted_iota(jnp.int32, (2 * tokens, slab), 1) // width

    def finish(state):
        total, summed = (part.reshape(2, 2 * tokens, slab) for part in state[1:])
        return jnp.where(lane_head == 0, summed[0], summed[1]) / jnp.where(
            lane_head == 0, total[0], total[1]
        )

    def restored(result, exact):
        coarse = result.astype(jnp.bfloat16)
        moved = jnp.dot(restore, coarse, preferred_element_type=jnp.float32)
        if exact:
            rest = (result - coarse.astype(jnp.float32)).astype(jnp.bfloat16)
            moved = moved + jnp.dot(restore, rest, preferred_element_type=jnp.float32)
        return moved.reshape(2, tokens, slab)

    def keep_exact(index, pair, state):
        moved = restored(finish(state), True)
        for step in range(2):
            ready[index * half + 2 * pair + step] = moved[step]

    def send_half(index, pair, state, arrival):
        moved = restored(finish(state), False).astype(jnp.bfloat16)
        for step in range(2):
            peer = index * half + 2 * pair + step
            ready_half[peer] = moved[step]
            crossbound(peer, me, arrival).start()

    head_lane = lax.broadcasted_iota(jnp.int32, (tokens, slab), 1) // width

    def local_part(base, place):
        first = (base + place) * 4 // inner
        at = slice((base + place) * slab, (base + place + 1) * slab)
        side_at = slice(place * slab, (place + 1) * slab)
        before = row_place(square, 1, first) <= row_place(square, 0, first)
        own = jnp.where(
            before, jnp.where(same, jnp.where(both, math.log2(3.0), 1.0), 0.0), FLOOR_SCORE
        )
        table = jnp.concatenate([jnp.where(core == 1, below, FLOOR_SCORE), own], axis=1)
        keys = jnp.concatenate([side_k[:, side_at], k_rows[:, at]], axis=0)
        values = jnp.concatenate([side_v[:, side_at], v_rows[:, at]], axis=0)
        state = attend_part(by_head(q_rows[:, at]), keys, values, twice(table))
        for which in range(3):
            local_ref[which, place] = jnp.where(
                head_lane == 0, state[which][0:tokens], state[which][tokens:]
            )

    tile_lane = lax.broadcasted_iota(jnp.int32, (tile, slab), 1)
    spread_row = lax.broadcasted_iota(jnp.int32, (slab, slab), 0)
    spread_column = lax.broadcasted_iota(jnp.int32, (slab, slab), 1)
    spread = jnp.where(
        (spread_row // width == spread_column // width)
        & (spread_row % (width // 4) == 0)
        & (spread_row % width < 3 * (width // 4)),
        1.0,
        0.0,
    ).astype(jnp.bfloat16)

    def far_part():
        top, total, summed = far_block(0, 0, 1)[0]
        lane = lax.broadcasted_iota(jnp.int32, (2, tile, slab), 2)
        top, total, summed = (
            jnp.where(lane < width, part[0:2], part[2:4]) for part in (top, total, summed)
        )
        lse = top + jnp.log2(total)
        place = lane % width // (width // 4)
        high = lse.astype(jnp.bfloat16).astype(jnp.float32)
        middle = (lse - high).astype(jnp.bfloat16).astype(jnp.float32)
        low = lse - high - middle
        packed = jnp.where(
            place == 0, high, jnp.where(place == 1, middle, jnp.where(place == 2, low, 0.0))
        )
        result = summed / total
        for peer in range(2):
            far_out[peer, 0] = result[peer].astype(jnp.bfloat16)
            far_out[peer, 1] = packed[peer].astype(jnp.bfloat16)
            partbound(peer).start()

    def local_join(place):
        at = slice(place * slab, (place + 1) * slab)
        result = far_landed[0, :, at].astype(jnp.float32)
        lse = jnp.dot(far_landed[1, :, at], spread, preferred_element_type=jnp.float32)
        top, total, summed = (local_ref[which, place, 0:tile] for which in range(3))
        top, total, summed = join((top, total, summed), (lse, jnp.ones_like(lse), result))
        local_ref[1, place, 0:tile] = total
        local_ref[2, place, 0:tile] = summed

    def thirds(value):
        high = value.astype(jnp.bfloat16).astype(jnp.float32)
        middle = (value - high).astype(jnp.bfloat16).astype(jnp.float32)
        return high, middle, value - high - middle

    lanes = width // 4

    def send_last(state):
        top, total, summed = (part.reshape(2, 2, tokens, slab) for part in state)
        lse = top + jnp.log2(total)
        lane = lax.broadcasted_iota(jnp.int32, (tokens, slab), 1)
        term = lane % lanes // (lanes // 4)
        for step in range(2):
            result = jnp.where(lane < width, summed[0, step], summed[1, step]) / jnp.where(
                lane < width, total[0, step], total[1, step]
            )
            kept = jnp.where(lane % (2 * lanes) < lanes, lse[0, step], lse[1, step])
            high, middle, low = thirds(kept)
            packed = jnp.where(
                term == 0, high, jnp.where(term == 1, middle, jnp.where(term == 2, low, 0.0))
            )
            group = lax.broadcasted_iota(jnp.int32, (tile, slab), 1) // (2 * lanes)
            folded = packed[0:tile]
            for part in range(1, 4):
                folded = jnp.where(group == part, packed[part * tile : (part + 1) * tile], folded)
            part_out[step, 0:tokens] = result.astype(jnp.bfloat16)
            part_out[step, tokens : tokens + tile] = folded.astype(jnp.bfloat16)
            lastbound(step).start()

    unfold_shape = (slab, 4 * slab)
    unfold_row = lax.broadcasted_iota(jnp.int32, unfold_shape, 0)
    unfold_column = lax.broadcasted_iota(jnp.int32, unfold_shape, 1)
    unfold = jnp.where(
        (unfold_row // (2 * lanes) == unfold_column // slab)
        & (unfold_row % (2 * lanes) // lanes == unfold_column % slab // width)
        & (unfold_row % (lanes // 4) == 0)
        & (unfold_row % lanes < 3 * (lanes // 4)),
        1.0,
        0.0,
    ).astype(jnp.bfloat16)

    def last_join(place):
        at = slice(place * slab, (place + 1) * slab)
        result = part_landed[0:tokens, at].astype(jnp.float32)
        wide_lse = jnp.dot(
            part_landed[tokens : tokens + tile, at], unfold, preferred_element_type=jnp.float32
        )
        lse = jnp.concatenate(
            [wide_lse[:, part * slab : (part + 1) * slab] for part in range(4)], axis=0
        )
        state = [local_ref[which, place] for which in range(3)]
        top, total, summed = join(state, (lse, jnp.ones_like(lse), result))
        local_ref[1, place] = total
        local_ref[2, place] = summed

    def local_finish(base, place):
        first = (base + place) * 4 // inner
        order = (at_row == row_place(square, 1, first)).astype(jnp.float32).astype(jnp.bfloat16)
        result = local_ref[2, place] / local_ref[1, place]
        coarse = result.astype(jnp.bfloat16)
        fine = (result - coarse.astype(jnp.float32)).astype(jnp.bfloat16)
        moved = jnp.dot(order, coarse, preferred_element_type=jnp.float32)
        moved = moved + jnp.dot(order, fine, preferred_element_type=jnp.float32)
        out_ref[:, (base + place) * slab : (base + place + 1) * slab] = moved

    drain(in_sem.at[0], (half - 1) * 2 * tile)

    forward(side)

    @pl.when(chip == 0)
    def _():
        @pl.when(core == 1)
        def _():
            drain(in_sem.at[6], 2 * tokens * half)

        for place in range(half):
            local_part(half, place)

    drain(in_sem.at[2], half * 2 * tile)
    forward(1 - side)

    @pl.when(chip == chips - 1)
    def _():
        @pl.when(core == 1)
        def _():
            drain(in_sem.at[6], 2 * tokens * half)

        for place in range(half):
            local_part(0, place)

    drain(in_sem.at[1], (half - 1) * (3 * tokens - 2 * tile))

    def wait_far():
        for other in range(outer - 1):

            @pl.when(mine > other)
            def _():
                drain(far_sem.at[other], 2 * far_rows)

    @pl.when(side == 0)
    def _():
        for pair in range(pairs):
            keep_state(0, pair, edge(0, pair))
        drain(in_sem.at[3], half * tokens)
        for pair in range(pairs):
            keep_state(1, pair, below_block(pair))
        wait_far()
        near_far = far_block(0, 0, pairs)
        apart_far = far_block(1, 0, pairs)
        for pair in range(pairs):
            keep_state(1, pair, join_tile(load_state(1, pair), apart_far[pair]))
        for pair in range(pairs):
            keep_exact(0, pair, join_tile(load_state(0, pair), near_far[pair]))
        for step in range(1, half):
            backbound(lax.rem(me + step, half), me).start()
        out_ref[:, columns(me)] = ready[me]
        drain(in_sem.at[4], 4 * (tokens - tile))
        send_last(
            join(
                load_state(1, 1),
                attend_part(
                    pair_queries(1, 1),
                    span_of(k_buf, half, half + 2),
                    span_of(v_buf, half, half + 2),
                    below_pair,
                ),
            )
        )
        send_half(1, 0, join(load_state(1, 0), edge(1, 0)), 1 + me // 2)

    @pl.when(side == 1)
    def _():
        for pair in range(pairs):
            keep_state(1, pair, edge(1, pair))

        drain(in_sem.at[4], 4 * (tokens - tile) + 2 * tile)
        drain(in_sem.at[3], 4 * (tokens - tile))
        for pair in range(pairs):
            keep_state(1, pair, join(load_state(1, pair), below_block(pair)))
        wait_far()

        @pl.when(mine > 0)
        def _():
            far_part()

        def near_block(own):
            away = 1 - own
            near_far = far_block(1, 0, pairs)
            send_half(1, away, join_tile(load_state(1, away), near_far[away]), 0)
            keep_exact(1, own, join_tile(load_state(1, own), near_far[own]))
            backbound(partner, me).start()
            out_ref[:, columns(me)] = ready[me]

        @pl.when(chip < chips - 1)
        def _():
            near_block(0)

        drain(in_sem.at[5], 2 * tokens)
        send_half(0, 1, join_tile(edge(0, 1), far_block(0, 1, 2)[0]), chip - 1)

        @pl.when(chip == chips - 1)
        def _():
            near_block(1)

    @pl.when(side == 0)
    def _():
        drain(back_sem.at[0], (half - 1) * 2 * tokens)

    @pl.when(side == 1)
    def _():
        drain(back_sem.at[0], 4 * tokens)
        for step in range(2):
            owner = (chips - 1 - chip + chips // 2) * 2 + step
            out_ref[:, columns(owner)] = landed[:, columns(owner)].astype(jnp.float32)

    @pl.when(chip == 0)
    def _():
        @pl.when(mine > 0)
        def _():
            drain(back_sem.at[1], half * 2 * tile)
            for place in range(half):
                local_join(place)

        for place in range(half):
            local_finish(half, place)

    @pl.when(chip == chips - 1)
    def _():
        drain(back_sem.at[1], half * (tokens + tile))
        for place in range(half):
            last_join(place)
        for place in range(half):
            local_finish(0, place)

    @pl.when((chip > 0) & (chip < chips - 1))
    def _():
        for pair in range(pairs):
            drain(back_sem.at[1 + pair], 2 * tokens)
            for step in (2 * pair, 2 * pair + 1):
                owner = (1 - side) * half + step
                out_ref[:, columns(owner)] = landed[:, columns(owner)].astype(jnp.float32)

        drain(send_sem.at[0], (inner - 1) * 3 * tokens)

    sent_near = (half - 1) * 3 * tokens + half * (2 * tokens + tile)

    @pl.when((chip == 0) & (core == 0))
    def _():
        drain(send_sem.at[0], sent_near + 2 * tokens * half)

    @pl.when((chip == 0) & (core == 1))
    def _():
        drain(send_sem.at[0], sent_near)

    sent_last = (half - 1) * 3 * tokens + half * (tokens + 2 * tile)

    @pl.when((chip == chips - 1) & (core == 0))
    def _():
        drain(send_sem.at[0], sent_last + 2 * tokens * half)

    @pl.when((chip == chips - 1) & (core == 1))
    def _():
        drain(send_sem.at[0], sent_last)

    @pl.when(side == 0)
    def _():
        drain(send_sem.at[2], (half - 1) * 2 * tokens + half * tokens + 2 * tile)

    @pl.when((side == 1) & (mine == 0))
    def _():
        drain(send_sem.at[2], 6 * tokens)

    @pl.when((side == 1) & (mine > 0))
    def _():
        drain(send_sem.at[2], 6 * tokens + 4 * tile)

    for count in range(1, outer):

        @pl.when(outer - 1 - mine == count)
        def _():
            drain(send_sem.at[1], count * 2 * far_rows)


def fused(queries, key_rows, value_rows):
    tokens, features = queries.shape
    inner = lax.axis_size("inner")
    outer = lax.axis_size("outer")
    slab = features // inner
    tile = tokens // 4
    pairs = inner // 4
    any_space = pl.BlockSpec(memory_space=pl.ANY)
    dims = (inner, outer, tokens, slab, features // HEADS)
    return pl.pallas_call(
        partial(fused_kernel, dims),
        out_shape=pltpu.VMEM((tokens, features), jnp.float32),
        in_specs=[any_space] * 3,
        out_specs=pl.BlockSpec(memory_space=pltpu.VMEM),
        scratch_shapes=[
            *[pltpu.VMEM((tokens, features), jnp.bfloat16)] * 6,
            *[pltpu.VMEM((inner, tokens, slab), jnp.bfloat16)] * 3,
            *[pltpu.VMEM((outer - 1, inner, tile, slab), jnp.bfloat16)] * 2,
            pltpu.VMEM((3, 2, pairs, 4 * tokens, slab), jnp.float32),
            pltpu.VMEM((inner, tokens, slab), jnp.float32),
            pltpu.VMEM((inner, tokens, slab), jnp.bfloat16),
            pltpu.VMEM((tokens, features), jnp.bfloat16),
            *[pltpu.VMEM((tokens, features // 2), jnp.bfloat16)] * 2,
            pltpu.VMEM((3, inner // 2, tokens, slab), jnp.float32),
            pltpu.VMEM((2, 2, tile, slab), jnp.bfloat16),
            pltpu.VMEM((2, tile, features // 2), jnp.bfloat16),
            pltpu.VMEM((2, tokens + tile, slab), jnp.bfloat16),
            pltpu.VMEM((tokens + tile, features // 2), jnp.bfloat16),
            pltpu.VMEM((inner * 2 * tokens, slab), jnp.float32),
            pltpu.SemaphoreType.DMA((3,)),
            pltpu.SemaphoreType.DMA((5 + pairs,)),
            pltpu.SemaphoreType.DMA((outer - 1,)),
            pltpu.SemaphoreType.DMA((1 + pairs,)),
            pltpu.SemaphoreType.DMA((3,)),
            pltpu.SemaphoreType.REGULAR((2,)),
        ],
        compiler_params=pltpu.CompilerParams(collective_id=0, has_side_effects=True),
    )(queries, key_rows, value_rows)


def device_program(queries, key_rows, value_rows):
    tokens, features = queries.shape
    inner = lax.axis_size("inner")
    outer = lax.axis_size("outer")
    width = features // HEADS
    fits = (
        inner * 2 == HEADS
        and outer > 1
        and inner % 4 == 0
        and width * 2 == 128
        and tokens % 64 == 0
        and inner * tokens <= 1024
        and (outer - 1) * inner * tokens // 4 <= 1024
    )
    if fits:
        return fused(queries, key_rows, value_rows)
    return on_device(queries, key_rows, value_rows)


def solution(mesh):
    placed = (P(("outer", "inner"), None), P(("outer", "inner"), None), P(("outer", "inner"), None))
    return jax.shard_map(
        device_program,
        mesh=mesh,
        in_specs=placed,
        out_specs=P(("outer", "inner"), None),
        check_vma=False,
    )
```

```python
import math
from functools import partial, reduce

import jax
import jax.numpy as jnp
import numpy as np
from jax import lax
from jax.experimental import pallas as pl
from jax.experimental.pallas import tpu as pltpu
from jax.sharding import PartitionSpec as P

HEADS = 16


FLOOR_SCORE = -1e30


def divisor_block(length, limit):
    extent = min(length, limit)
    while length % extent:
        extent -= 1
    return extent


def fresh_state(count, rows, width):
    return (
        jnp.full((count, rows), FLOOR_SCORE, jnp.float32),
        jnp.zeros((count, rows), jnp.float32),
        jnp.zeros((count, rows, width), jnp.float32),
    )


def finish_state(state):
    row_max, denominator, summed = state
    return (summed / denominator[..., None], row_max + jnp.log(denominator))


def online_step(state, query_rows, query_rank, key_rows, value_rows, key_rank):
    row_max, denominator, summed = state
    scale = query_rows.shape[-1] ** (-0.5)
    scores = (
        jnp.einsum("inh,ibh->inb", query_rows, key_rows, preferred_element_type=jnp.float32) * scale
    )
    scores = jnp.where(key_rank[None, None, :] <= query_rank[None, :, None], scores, FLOOR_SCORE)
    new_max = jnp.maximum(row_max, jnp.max(scores, axis=2))
    weights = jnp.exp(scores - new_max[..., None])
    rescale = jnp.exp(row_max - new_max)
    denominator = denominator * rescale + jnp.sum(weights, axis=2)
    summed = summed * rescale[..., None] + jnp.einsum(
        "inb,ibh->inh", weights.astype(jnp.bfloat16), value_rows, preferred_element_type=jnp.float32
    )
    return (new_max, denominator, summed)


def attend_keys(state, query_rows, query_rank, key_rows, value_rows, key_rank, stop=None):
    length = key_rows.shape[1]
    block = divisor_block(length, 512)

    def advance(index, carry):
        start = index * block
        piece_keys = lax.dynamic_slice_in_dim(key_rows, start, block, 1)
        piece_values = lax.dynamic_slice_in_dim(value_rows, start, block, 1)
        piece_rank = lax.dynamic_slice_in_dim(key_rank, start, block, 0)
        return online_step(carry, query_rows, query_rank, piece_keys, piece_values, piece_rank)

    upper = length // block if stop is None else stop
    return lax.fori_loop(0, upper, advance, state)


def attend(query_rows, query_rank, key_rows, value_rows, key_rank):
    count, length, width = query_rows.shape
    block = divisor_block(length, 512)
    steps = length // block
    query_split = query_rows.reshape(count, steps, block, width).swapaxes(0, 1)
    rank_split = query_rank.reshape(steps, block)

    def one_block(pieces):
        state = attend_keys(
            fresh_state(count, block, width),
            pieces[0],
            pieces[1],
            key_rows,
            value_rows,
            key_rank,
            pieces[2] + 1,
        )
        return finish_state(state)

    outputs, lses = lax.map(
        one_block, (query_split, rank_split, jnp.arange(steps, dtype=jnp.int32))
    )
    return (
        outputs.swapaxes(0, 1).reshape(count, length, width),
        lses.swapaxes(0, 1).reshape(count, length),
    )


def merge_levels(parts):
    row_max = reduce(jnp.maximum, [lse for _, lse in parts])
    weights = [jnp.exp(lse - row_max) for _, lse in parts]
    denominator = reduce(jnp.add, weights)
    summed = reduce(
        jnp.add, [weight[..., None] * output for weight, (output, _) in zip(weights, parts)]
    )
    return (summed / denominator[..., None], row_max + jnp.log(denominator))


def on_device(queries, key_rows, value_rows):
    tokens, features = queries.shape
    heads = HEADS
    width = features // heads
    outer_count = lax.axis_size("outer")
    inner_count = lax.axis_size("inner")
    outer_index = lax.axis_index("outer")
    inner_index = lax.axis_index("inner")
    per_device = 4 * heads // inner_count
    quarter = tokens // 4
    sixteenth = tokens // 16
    class_len = quarter * inner_count
    far_len = sixteenth * inner_count

    def to_items(array):
        return (
            array.reshape(quarter, 4, heads, width)
            .transpose(2, 1, 0, 3)
            .reshape(4 * heads, quarter, width)
        )

    local_ranks = jnp.arange(tokens, dtype=jnp.int32)
    head_major = [
        a.reshape(tokens, heads, width).transpose(1, 0, 2) for a in (queries, key_rows, value_rows)
    ]
    near_out, near_lse = attend(
        head_major[0], local_ranks, head_major[1], head_major[2], local_ranks
    )
    near_out = near_out.transpose(1, 0, 2)
    near_lse = near_lse.T
    item_index = inner_index * per_device + jnp.arange(per_device, dtype=jnp.int32)
    band = item_index // 16
    far_query_rank = outer_index * far_len + jnp.arange(far_len, dtype=jnp.int32)
    pick = np.array(
        [head * 16 + head // 4 * 4 + residue for head in range(heads) for residue in range(4)],
        np.int32,
    )

    def to_sixteen(array):
        spread = (
            array.reshape(sixteenth, 16, heads, width)
            .transpose(2, 1, 0, 3)
            .reshape(16 * heads, sixteenth, width)
        )
        return jnp.take(spread, pick, axis=0)

    gathered_k, gathered_v = (
        lax.all_gather(to_sixteen(key_rows), "outer", axis=1, tiled=True),
        lax.all_gather(to_sixteen(value_rows), "outer", axis=1, tiled=True),
    )
    mid_q, mid_k, mid_v, far_k, far_v = (
        lax.all_to_all(to_items(queries), "inner", split_axis=0, concat_axis=1, tiled=True),
        lax.all_to_all(to_items(key_rows), "inner", split_axis=0, concat_axis=1, tiled=True),
        lax.all_to_all(to_items(value_rows), "inner", split_axis=0, concat_axis=1, tiled=True),
        lax.all_to_all(gathered_k, "inner", split_axis=0, concat_axis=1, tiled=True),
        lax.all_to_all(gathered_v, "inner", split_axis=0, concat_axis=1, tiled=True),
    )
    split = mid_q.reshape(per_device, far_len, 4, width)
    picker = jnp.broadcast_to(band[:, None, None, None], (per_device, far_len, 1, width))
    far_q = jnp.take_along_axis(split, picker, axis=2)[:, :, 0, :]
    position = jnp.arange(far_k.shape[1], dtype=jnp.int32)
    far_key_rank = (
        position // sixteenth % outer_count * far_len
        + position // (outer_count * sixteenth) * sixteenth
        + position % sixteenth
    )
    far_state = attend_keys(
        fresh_state(per_device, far_len, width), far_q, far_query_rank, far_k, far_v, far_key_rank
    )
    far_out, far_lse = finish_state(far_state)
    class_ranks = jnp.arange(class_len, dtype=jnp.int32)
    mid_out, mid_lse = attend(mid_q, class_ranks, mid_k, mid_v, class_ranks)
    back_mid, back_mid_lse, back_far, back_far_lse = (
        lax.all_to_all(mid_out, "inner", split_axis=1, concat_axis=0, tiled=True),
        lax.all_to_all(mid_lse, "inner", split_axis=1, concat_axis=0, tiled=True),
        lax.all_to_all(far_out, "inner", split_axis=1, concat_axis=0, tiled=True),
        lax.all_to_all(far_lse, "inner", split_axis=1, concat_axis=0, tiled=True),
    )
    selector = np.array(
        [[band_index == head // 4 for band_index in range(4)] for head in range(heads)]
    )
    spread_out = jnp.where(
        selector[:, :, None, None, None], back_far.reshape(heads, 1, 4, sixteenth, width), 0.0
    )
    spread_lse = jnp.where(
        selector[:, :, None, None], back_far_lse.reshape(heads, 1, 4, sixteenth), FLOOR_SCORE
    )
    far_placed = (
        spread_out.reshape(heads, 16, sixteenth, width)
        .transpose(2, 1, 0, 3)
        .reshape(tokens, heads, width)
    )
    far_placed_lse = (
        spread_lse.reshape(heads, 16, sixteenth).transpose(2, 1, 0).reshape(tokens, heads)
    )
    placed = (
        back_mid.reshape(heads, 4, quarter, width)
        .transpose(2, 1, 0, 3)
        .reshape(tokens, heads, width)
    )
    placed_lse = back_mid_lse.reshape(heads, 4, quarter).transpose(2, 1, 0).reshape(tokens, heads)
    combined, _ = merge_levels(
        [(near_out, near_lse), (placed, placed_lse), (far_placed, far_placed_lse)]
    )
    return combined.reshape(tokens, features)


def fused_kernel(
    dims, q_ref, k_ref, v_ref, out_ref, q_held, k_held, v_held, q_rows, k_rows, v_rows, q_buf, k_buf, v_buf, far_k, far_v,
    state_ref, ready, ready_half, landed, side_k, side_v, local_ref, far_out, far_landed, part_out, part_landed,
    spare, send_sem, in_sem, far_sem, back_sem, held_sem, stage_sem,
):
    inner, outer, tokens, slab, width = dims
    chips = inner // 2
    half = inner // 2
    pairs = half // 2
    run = tokens // 16
    tile = tokens // 4
    wide = slab * inner // 4
    me = lax.axis_index("inner")
    mine = lax.axis_index("outer")
    chip = me // 2
    core = lax.rem(me, 2)
    side = me // half
    band = me * 4 // inner
    mesh_id = pl.DeviceIdType.MESH
    sources = (k_ref, v_ref, q_ref)
    held = (k_held, v_held, q_held)
    placed = (k_rows, v_rows, q_rows)
    buffers = (k_buf, v_buf, q_buf)
    pick_k, pick_v, rest_k, rest_v, whole_q, pick_q = range(6)
    pieces = (
        (0, 0, tile),
        (1, 0, tile),
        (0, tile, tokens),
        (1, tile, tokens),
        (2, 0, tokens),
        (2, 0, tile),
    )

    def columns(index):
        return pl.ds(pl.multiple_of(index * slab, slab), slab)

    def drain(semaphore, rows):
        place = spare.at[0 : rows // 2]
        pltpu.make_async_copy(place, place, semaphore).wait()

    def inbound(which, peer, owner, arrival):
        array, start, stop = pieces[which]
        return pltpu.make_async_remote_copy(
            src_ref=placed[array].at[start:stop, columns(peer)],
            dst_ref=buffers[array].at[owner, start:stop, :],
            send_sem=send_sem.at[0],
            recv_sem=in_sem.at[arrival],
            device_id={"inner": peer},
            device_id_type=mesh_id,
        )

    def farbound(which, part, peer, owner):
        blocks = pl.ds(part * half, half)
        return pltpu.make_async_remote_copy(
            src_ref=buffers[which].at[blocks, 0:tile, :],
            dst_ref=(far_k, far_v)[which].at[owner, blocks],
            send_sem=send_sem.at[1],
            recv_sem=far_sem.at[owner],
            device_id={"outer": peer},
            device_id_type=mesh_id,
        )

    def backbound(peer, owner):
        return pltpu.make_async_remote_copy(
            src_ref=ready.at[peer],
            dst_ref=out_ref.at[:, columns(owner)],
            send_sem=send_sem.at[2],
            recv_sem=back_sem.at[0],
            device_id={"inner": peer},
            device_id_type=mesh_id,
        )

    def apart_columns(base):
        return slice(base * slab, (base + half) * slab)

    def sidebound(which, base, peer):
        return pltpu.make_async_remote_copy(
            src_ref=placed[which].at[:, apart_columns(base)],
            dst_ref=(side_k, side_v)[which],
            send_sem=send_sem.at[0],
            recv_sem=in_sem.at[6],
            device_id={"inner": peer},
            device_id_type=mesh_id,
        )

    def partbound(peer):
        return pltpu.make_async_remote_copy(
            src_ref=far_out.at[peer],
            dst_ref=far_landed.at[:, :, columns(me - half)],
            send_sem=send_sem.at[2],
            recv_sem=back_sem.at[1],
            device_id={"inner": peer},
            device_id_type=mesh_id,
        )

    def lastbound(step):
        return pltpu.make_async_remote_copy(
            src_ref=part_out.at[step],
            dst_ref=part_landed.at[:, columns(me)],
            send_sem=send_sem.at[2],
            recv_sem=back_sem.at[1],
            device_id={"inner": inner - 2 + step},
            device_id_type=mesh_id,
        )

    def crossbound(peer, owner, arrival):
        return pltpu.make_async_remote_copy(
            src_ref=ready_half.at[peer],
            dst_ref=landed.at[:, columns(owner)],
            send_sem=send_sem.at[2],
            recv_sem=back_sem.at[arrival],
            device_id={"inner": peer},
            device_id_type=mesh_id,
        )

    own_held = [
        pltpu.make_async_copy(sources[which], held[which], held_sem.at[which]) for which in range(3)
    ]
    for copy in own_held:
        copy.start()

    barrier = pltpu.get_barrier_semaphore()
    partner = chip * 2 + 1 - core

    def greet(place):
        pl.semaphore_signal(barrier, inc=1, device_id=place, device_id_type=mesh_id)

    greet({"inner": partner})
    for step in range(1, outer):
        greet({"inner": chip * 2 + 1, "outer": lax.rem(mine + step, outer)})
    for other in range(chips):
        if other < chips // 2:
            counter = jnp.where(jnp.abs(chip - other) > 1, 1, 0)
        else:
            counter = jnp.where((chip > other) & (mine > 0), 1, 0)

        @pl.when(chip != other)
        def _():
            greet({"inner": other * 2 + counter})

    def row_place(shape, axis, first):
        row = lax.broadcasted_iota(jnp.int32, shape, axis)
        residue = 4 * lax.rem(first + row // tile, 4) + row % tile // run
        return row % run * 16 + residue

    square = (tokens, tokens)
    at_row = lax.broadcasted_iota(jnp.int32, square, 0)
    at_column = lax.broadcasted_iota(jnp.int32, square, 1)
    orders = [
        (row_place(square, 0, first) == at_column).astype(jnp.float32).astype(jnp.bfloat16)
        for first in range(4)
    ]

    def place_rows(which):
        own_held[which].wait()
        for first in range(4):
            place = slice(first * wide, (first + 1) * wide)
            placed[which][:, place] = jnp.dot(
                orders[first], held[which][:, place], preferred_element_type=jnp.float32
            ).astype(jnp.bfloat16)
        buffers[which][me] = placed[which][:, columns(me)]

    adjacent = jnp.where(chip == 0, 1, 2)
    near_chips = jnp.where(side == 0, adjacent, jnp.where(mine == 0, chips - 1, chip))
    near_count = 1 + 2 * near_chips
    rest_count = 1 + 2 * (outer - 1) + 2 * (chips - 1 - near_chips)

    def pass_on(first, stage, count):
        @pl.when(core == first)
        def _():
            pl.semaphore_wait(barrier, count)
            pl.semaphore_signal(
                stage_sem.at[stage], inc=1, device_id={"inner": partner}, device_id_type=mesh_id
            )

        @pl.when(core != first)
        def _():
            pl.semaphore_wait(stage_sem.at[stage], 1)

    picks = (pick_k, pick_v)
    rest = (rest_k, rest_v)
    query = (whole_q,)

    def arrival_of(which, source, target):
        low = chips // 2
        apart = (source < low) != (target < low)
        if which in picks:
            return 2 if apart else 0
        if not apart:
            return 1
        if target < low:
            return 3 if which == whole_q else 4 + source % low
        if source == 0:
            return 4
        return 5 if which == whole_q else 3

    def send(source, batches):
        for group, targets in batches:
            for target in targets:
                for other in range(2):
                    for which in group:
                        arrival = arrival_of(which, source, target)
                        inbound(which, target * 2 + other, me, arrival).start()

    def send_partner(group):
        for which in group:
            inbound(which, partner, me, 0 if which in picks else 1).start()

    place_rows(0)
    place_rows(1)
    pass_on(0, 0, near_count)
    send_partner(picks + rest)

    @pl.when(chip == 0)
    def _():
        send(0, ((picks, (1,)), (rest, (1,))))

        @pl.when(core == 0)
        def _():
            for which in range(2):
                sidebound(which, half, 1).start()


    @pl.when(chip == 1)
    def _():
        send(1, ((picks, (2, 0)), ((rest_k,), (2,)), (rest, (0,))))

    @pl.when(chip == 2)
    def _():
        send(2, ((picks, (0, 1)),))

    @pl.when(chip == 3)
    def _():
        send(3, ((picks, (0, 1, 2)),))

    place_rows(2)
    send_partner(query)

    @pl.when(chip == 0)
    def _():
        send(0, ((query, (1,)),))
        pass_on(1, 1, rest_count)
        send(0, ((picks, (3, 2)), ((pick_q,) + rest, (2, 3))))

    @pl.when(chip == 1)
    def _():
        send(1, ((query, (0,)),))
        pass_on(1, 1, rest_count)
        send(1, ((picks, (3,)), (rest, (3,)), ((rest_v,), (2,)), (query, (3, 2))))

    @pl.when(chip == 2)
    def _():
        @pl.when(mine == 0)
        def _():
            send(2, ((query, (0, 1)),))

        @pl.when(mine > 0)
        def _():
            pass_on(1, 1, rest_count)

        send(2, ((picks, (3,)),))

        @pl.when(mine > 0)
        def _():
            send(2, ((query, (0, 1)),))

        send(2, ((rest, (0, 1)), (query, (3,)), (rest, (3,))))

        @pl.when(mine == 0)
        def _():
            pass_on(1, 1, rest_count)


    @pl.when(chip == 3)
    def _():
        send(3, ((query, (0, 1, 2)), (rest, (2,))))

        @pl.when(core == 0)
        def _():
            for which in range(2):
                sidebound(which, 0, inner - 1).start()

        pass_on(1, 1, rest_count)

    for place, base in ((0, half), (inner - 2, 0)):

        @pl.when(me == place)
        def _():
            side_k[...] = k_rows[:, apart_columns(base)]
            side_v[...] = v_rows[:, apart_columns(base)]

    for other in range(outer - 1):

        @pl.when(mine <= other)
        def _():
            far_k[other] = jnp.zeros((inner, tile, slab), jnp.bfloat16)
            far_v[other] = jnp.zeros((inner, tile, slab), jnp.bfloat16)

    def forward(part):
        for other in range(outer - 1, 0, -1):

            @pl.when(mine < other)
            def _():
                for which in range(2):
                    farbound(which, part, other, mine).start()

    same = at_row % tile // run == at_column % tile // run
    both = (at_row < tile) & (at_column < tile)
    below = jnp.where(same, jnp.where(both, 1.0, 0.0), FLOOR_SCORE)
    before = row_place(square, 1, band) <= row_place(square, 0, band)
    diagonal = jnp.where(
        before, jnp.where(same, jnp.where(both, math.log2(3.0), 1.0), 0.0), FLOOR_SCORE
    )
    never = jnp.full(square, FLOOR_SCORE, jnp.float32)

    def twice(table):
        return jnp.concatenate([table, table], axis=0)

    below_pair = twice(jnp.concatenate([below, below], axis=1))
    below_pair = jnp.concatenate([below_pair, below_pair], axis=0)
    edge_pair = jnp.concatenate(
        [jnp.concatenate([diagonal, never], axis=1), jnp.concatenate([below, diagonal], axis=1)], axis=0
    )
    edge_pair = twice(edge_pair)
    far_rows = inner * tile
    far_shape = (pairs * 4 * tile, (outer - 1) * far_rows)
    far_query = lax.broadcasted_iota(jnp.int32, far_shape, 0)
    far_key = lax.broadcasted_iota(jnp.int32, far_shape, 1)
    far_table = jnp.where(
        (far_query % tile // run == far_key % tile // run) & (far_key // far_rows < mine), 0.0, FLOOR_SCORE
    )
    factor = width ** (-0.5) * math.log2(math.e)
    contract = (((1,), (1,)), ((), ()))

    def by_head(rows):
        lane_head = lax.broadcasted_iota(jnp.int32, rows.shape, 1) // width
        return jnp.concatenate(
            [jnp.where(lane_head == head, rows, jnp.zeros_like(rows)) for head in range(2)], axis=0
        )

    def across(column):
        return jnp.broadcast_to(column, (column.shape[0], slab))

    def attend_part(rows, keys, values, table):
        scores = lax.dot_general(rows, keys, contract, preferred_element_type=jnp.float32)
        scores = scores * factor + table
        top = jnp.max(scores, axis=1, keepdims=True)
        weights = jnp.exp2(scores - top)
        total = jnp.sum(weights, axis=1, keepdims=True)
        summed = jnp.dot(weights.astype(jnp.bfloat16), values, preferred_element_type=jnp.float32)
        return across(top), across(total), summed

    def join(one, two):
        top = jnp.maximum(one[0], two[0])
        first = jnp.exp2(one[0] - top)
        second = jnp.exp2(two[0] - top)
        return top, one[1] * first + two[1] * second, one[2] * first + two[2] * second

    def join_tile(state, far):
        cut = [part.reshape(4, tokens, slab) for part in state]
        met = join([part[:, 0:tile] for part in cut], far)
        return [
            jnp.concatenate([new, old[:, tile:]], axis=1).reshape(4 * tokens, slab)
            for new, old in zip(met, cut)
        ]

    def load_state(index, pair):
        return [state_ref[which, index, pair] for which in range(3)]

    def keep_state(index, pair, state):
        for which in range(3):
            state_ref[which, index, pair] = state[which]

    def pair_queries(index, pair):
        rows = q_buf[index * half + 2 * pair : index * half + 2 * pair + 2]
        return by_head(rows.reshape(2 * tokens, slab))

    def span_of(buffer, start, stop):
        return buffer[start:stop].reshape((stop - start) * tokens, slab)

    def edge(index, pair):
        start = index * half
        stop = start + 2 * pair + 2
        table = jnp.concatenate([below_pair] * pair + [edge_pair], axis=1)
        return attend_part(
            pair_queries(index, pair), span_of(k_buf, start, stop), span_of(v_buf, start, stop), table
        )

    def below_block(pair):
        table = jnp.concatenate([below_pair] * pairs, axis=1)
        return attend_part(
            pair_queries(1, pair), span_of(k_buf, 0, half), span_of(v_buf, 0, half), table
        )

    def far_block(index, first, stop):
        span = stop - first
        rows = [
            by_head(
                q_buf[index * half + 2 * pair : index * half + 2 * pair + 2, 0:tile].reshape(2 * tile, slab)
            )
            for pair in range(first, stop)
        ]
        count = span * 4 * tile
        keys = far_k[...].reshape((outer - 1) * far_rows, slab)
        values = far_v[...].reshape((outer - 1) * far_rows, slab)
        state = attend_part(jnp.concatenate(rows, axis=0), keys, values, far_table[0:count])
        return [
            [part.reshape(span, 4, tile, slab)[place] for part in state] for place in range(span)
        ]

    pair_rows = (2 * tokens, 2 * tokens)
    natural = lax.broadcasted_iota(jnp.int32, pair_rows, 0)
    stored = lax.broadcasted_iota(jnp.int32, pair_rows, 1)
    stored_place = stored // tokens * tokens + row_place(pair_rows, 1, band) % tokens
    restore = (natural == stored_place).astype(jnp.float32).astype(jnp.bfloat16)
    lane_head = lax.broadcasted_iota(jnp.int32, (2 * tokens, slab), 1) // width

    def finish(state):
        total, summed = (part.reshape(2, 2 * tokens, slab) for part in state[1:])
        return jnp.where(lane_head == 0, summed[0], summed[1]) / jnp.where(
            lane_head == 0, total[0], total[1]
        )

    def restored(result, exact):
        coarse = result.astype(jnp.bfloat16)
        moved = jnp.dot(restore, coarse, preferred_element_type=jnp.float32)
        if exact:
            rest = (result - coarse.astype(jnp.float32)).astype(jnp.bfloat16)
            moved = moved + jnp.dot(restore, rest, preferred_element_type=jnp.float32)
        return moved.reshape(2, tokens, slab)

    def keep_exact(index, pair, state):
        moved = restored(finish(state), True)
        for step in range(2):
            ready[index * half + 2 * pair + step] = moved[step]

    def send_half(index, pair, state, arrival):
        moved = restored(finish(state), False).astype(jnp.bfloat16)
        for step in range(2):
            peer = index * half + 2 * pair + step
            ready_half[peer] = moved[step]
            crossbound(peer, me, arrival).start()

    head_lane = lax.broadcasted_iota(jnp.int32, (tokens, slab), 1) // width

    def local_part(base, place):
        first = (base + place) * 4 // inner
        at = slice((base + place) * slab, (base + place + 1) * slab)
        side_at = slice(place * slab, (place + 1) * slab)
        before = row_place(square, 1, first) <= row_place(square, 0, first)
        own = jnp.where(
            before, jnp.where(same, jnp.where(both, math.log2(3.0), 1.0), 0.0), FLOOR_SCORE
        )
        table = jnp.concatenate([jnp.where(core == 1, below, FLOOR_SCORE), own], axis=1)
        keys = jnp.concatenate([side_k[:, side_at], k_rows[:, at]], axis=0)
        values = jnp.concatenate([side_v[:, side_at], v_rows[:, at]], axis=0)
        state = attend_part(by_head(q_rows[:, at]), keys, values, twice(table))
        for which in range(3):
            local_ref[which, place] = jnp.where(
                head_lane == 0, state[which][0:tokens], state[which][tokens:]
            )

    tile_lane = lax.broadcasted_iota(jnp.int32, (tile, slab), 1)
    spread_row = lax.broadcasted_iota(jnp.int32, (slab, slab), 0)
    spread_column = lax.broadcasted_iota(jnp.int32, (slab, slab), 1)
    spread = jnp.where(
        (spread_row // width == spread_column // width)
        & (spread_row % (width // 4) == 0)
        & (spread_row % width < 3 * (width // 4)),
        1.0,
        0.0,
    ).astype(jnp.bfloat16)

    def far_part():
        top, total, summed = far_block(0, 0, 1)[0]
        lane = lax.broadcasted_iota(jnp.int32, (2, tile, slab), 2)
        top, total, summed = (
            jnp.where(lane < width, part[0:2], part[2:4]) for part in (top, total, summed)
        )
        lse = top + jnp.log2(total)
        place = lane % width // (width // 4)
        high = lse.astype(jnp.bfloat16).astype(jnp.float32)
        middle = (lse - high).astype(jnp.bfloat16).astype(jnp.float32)
        low = lse - high - middle
        packed = jnp.where(
            place == 0, high, jnp.where(place == 1, middle, jnp.where(place == 2, low, 0.0))
        )
        result = summed / total
        for peer in range(2):
            far_out[peer, 0] = result[peer].astype(jnp.bfloat16)
            far_out[peer, 1] = packed[peer].astype(jnp.bfloat16)
            partbound(peer).start()

    def local_join(place):
        at = slice(place * slab, (place + 1) * slab)
        result = far_landed[0, :, at].astype(jnp.float32)
        lse = jnp.dot(far_landed[1, :, at], spread, preferred_element_type=jnp.float32)
        top, total, summed = (local_ref[which, place, 0:tile] for which in range(3))
        top, total, summed = join((top, total, summed), (lse, jnp.ones_like(lse), result))
        local_ref[1, place, 0:tile] = total
        local_ref[2, place, 0:tile] = summed

    def thirds(value):
        high = value.astype(jnp.bfloat16).astype(jnp.float32)
        middle = (value - high).astype(jnp.bfloat16).astype(jnp.float32)
        return high, middle, value - high - middle

    lanes = width // 4

    def send_last(state):
        top, total, summed = (part.reshape(2, 2, tokens, slab) for part in state)
        lse = top + jnp.log2(total)
        lane = lax.broadcasted_iota(jnp.int32, (tokens, slab), 1)
        term = lane % lanes // (lanes // 4)
        for step in range(2):
            result = jnp.where(lane < width, summed[0, step], summed[1, step]) / jnp.where(
                lane < width, total[0, step], total[1, step]
            )
            kept = jnp.where(lane % (2 * lanes) < lanes, lse[0, step], lse[1, step])
            high, middle, low = thirds(kept)
            packed = jnp.where(
                term == 0, high, jnp.where(term == 1, middle, jnp.where(term == 2, low, 0.0))
            )
            group = lax.broadcasted_iota(jnp.int32, (tile, slab), 1) // (2 * lanes)
            folded = packed[0:tile]
            for part in range(1, 4):
                folded = jnp.where(group == part, packed[part * tile : (part + 1) * tile], folded)
            part_out[step, 0:tokens] = result.astype(jnp.bfloat16)
            part_out[step, tokens : tokens + tile] = folded.astype(jnp.bfloat16)
            lastbound(step).start()

    unfold_shape = (slab, 4 * slab)
    unfold_row = lax.broadcasted_iota(jnp.int32, unfold_shape, 0)
    unfold_column = lax.broadcasted_iota(jnp.int32, unfold_shape, 1)
    unfold = jnp.where(
        (unfold_row // (2 * lanes) == unfold_column // slab)
        & (unfold_row % (2 * lanes) // lanes == unfold_column % slab // width)
        & (unfold_row % (lanes // 4) == 0)
        & (unfold_row % lanes < 3 * (lanes // 4)),
        1.0,
        0.0,
    ).astype(jnp.bfloat16)

    def last_join(place):
        at = slice(place * slab, (place + 1) * slab)
        result = part_landed[0:tokens, at].astype(jnp.float32)
        wide_lse = jnp.dot(
            part_landed[tokens : tokens + tile, at], unfold, preferred_element_type=jnp.float32
        )
        lse = jnp.concatenate(
            [wide_lse[:, part * slab : (part + 1) * slab] for part in range(4)], axis=0
        )
        state = [local_ref[which, place] for which in range(3)]
        top, total, summed = join(state, (lse, jnp.ones_like(lse), result))
        local_ref[1, place] = total
        local_ref[2, place] = summed

    def local_finish(base, place):
        first = (base + place) * 4 // inner
        order = (at_row == row_place(square, 1, first)).astype(jnp.float32).astype(jnp.bfloat16)
        result = local_ref[2, place] / local_ref[1, place]
        coarse = result.astype(jnp.bfloat16)
        fine = (result - coarse.astype(jnp.float32)).astype(jnp.bfloat16)
        moved = jnp.dot(order, coarse, preferred_element_type=jnp.float32)
        moved = moved + jnp.dot(order, fine, preferred_element_type=jnp.float32)
        out_ref[:, (base + place) * slab : (base + place + 1) * slab] = moved

    drain(in_sem.at[0], (half - 1) * 2 * tile)

    forward(side)

    @pl.when(chip == 0)
    def _():
        @pl.when(core == 1)
        def _():
            drain(in_sem.at[6], 2 * tokens * half)

        for place in range(half):
            local_part(half, place)

    drain(in_sem.at[2], half * 2 * tile)
    forward(1 - side)

    @pl.when(chip == chips - 1)
    def _():
        @pl.when(core == 1)
        def _():
            drain(in_sem.at[6], 2 * tokens * half)

        for place in range(half):
            local_part(0, place)

    drain(in_sem.at[1], (half - 1) * (3 * tokens - 2 * tile))

    def wait_far():
        for other in range(outer - 1):

            @pl.when(mine > other)
            def _():
                drain(far_sem.at[other], 2 * far_rows)

    @pl.when(side == 0)
    def _():
        for pair in range(pairs):
            keep_state(0, pair, edge(0, pair))
        drain(in_sem.at[3], half * tokens)
        for pair in range(pairs):
            keep_state(1, pair, below_block(pair))
        wait_far()
        near_far = far_block(0, 0, pairs)
        apart_far = far_block(1, 0, pairs)
        for pair in range(pairs):
            keep_state(1, pair, join_tile(load_state(1, pair), apart_far[pair]))
        for pair in range(pairs):
            keep_exact(0, pair, join_tile(load_state(0, pair), near_far[pair]))
        for step in range(1, half):
            backbound(lax.rem(me + step, half), me).start()
        out_ref[:, columns(me)] = ready[me]
        drain(in_sem.at[4], 4 * (tokens - tile))
        send_last(
            join(
                load_state(1, 1),
                attend_part(
                    pair_queries(1, 1),
                    span_of(k_buf, half, half + 2),
                    span_of(v_buf, half, half + 2),
                    below_pair,
                ),
            )
        )
        send_half(1, 0, join(load_state(1, 0), edge(1, 0)), 1 + me // 2)

    @pl.when(side == 1)
    def _():
        for pair in range(pairs):
            keep_state(1, pair, edge(1, pair))

        drain(in_sem.at[4], 4 * (tokens - tile) + 2 * tile)
        drain(in_sem.at[3], 4 * (tokens - tile))
        for pair in range(pairs):
            keep_state(1, pair, join(load_state(1, pair), below_block(pair)))
        wait_far()

        @pl.when(mine > 0)
        def _():
            far_part()

        def near_block(own):
            away = 1 - own
            near_far = far_block(1, 0, pairs)
            send_half(1, away, join_tile(load_state(1, away), near_far[away]), 0)
            keep_exact(1, own, join_tile(load_state(1, own), near_far[own]))
            backbound(partner, me).start()
            out_ref[:, columns(me)] = ready[me]

        drain(in_sem.at[5], 2 * tokens)
        send_half(0, 1, join_tile(edge(0, 1), far_block(0, 1, 2)[0]), chip - 1)

        @pl.when(chip < chips - 1)
        def _():
            near_block(0)

        @pl.when(chip == chips - 1)
        def _():
            near_block(1)

    @pl.when(side == 0)
    def _():
        drain(back_sem.at[0], (half - 1) * 2 * tokens)

    @pl.when(side == 1)
    def _():
        drain(back_sem.at[0], 4 * tokens)
        for step in range(2):
            owner = (chips - 1 - chip + chips // 2) * 2 + step
            out_ref[:, columns(owner)] = landed[:, columns(owner)].astype(jnp.float32)

    @pl.when(chip == 0)
    def _():
        @pl.when(mine > 0)
        def _():
            drain(back_sem.at[1], half * 2 * tile)
            for place in range(half):
                local_join(place)

        for place in range(half):
            local_finish(half, place)

    @pl.when(chip == chips - 1)
    def _():
        drain(back_sem.at[1], half * (tokens + tile))
        for place in range(half):
            last_join(place)
        for place in range(half):
            local_finish(0, place)

    @pl.when((chip > 0) & (chip < chips - 1))
    def _():
        for pair in range(pairs):
            drain(back_sem.at[1 + pair], 2 * tokens)
            for step in (2 * pair, 2 * pair + 1):
                owner = (1 - side) * half + step
                out_ref[:, columns(owner)] = landed[:, columns(owner)].astype(jnp.float32)

        drain(send_sem.at[0], (inner - 1) * 3 * tokens)

    sent_near = (half - 1) * 3 * tokens + half * (2 * tokens + tile)

    @pl.when((chip == 0) & (core == 0))
    def _():
        drain(send_sem.at[0], sent_near + 2 * tokens * half)

    @pl.when((chip == 0) & (core == 1))
    def _():
        drain(send_sem.at[0], sent_near)

    sent_last = (half - 1) * 3 * tokens + half * (tokens + 2 * tile)

    @pl.when((chip == chips - 1) & (core == 0))
    def _():
        drain(send_sem.at[0], sent_last + 2 * tokens * half)

    @pl.when((chip == chips - 1) & (core == 1))
    def _():
        drain(send_sem.at[0], sent_last)

    @pl.when(side == 0)
    def _():
        drain(send_sem.at[2], (half - 1) * 2 * tokens + half * tokens + 2 * tile)

    @pl.when((side == 1) & (mine == 0))
    def _():
        drain(send_sem.at[2], 6 * tokens)

    @pl.when((side == 1) & (mine > 0))
    def _():
        drain(send_sem.at[2], 6 * tokens + 4 * tile)

    for count in range(1, outer):

        @pl.when(outer - 1 - mine == count)
        def _():
            drain(send_sem.at[1], count * 2 * far_rows)


def fused(queries, key_rows, value_rows):
    tokens, features = queries.shape
    inner = lax.axis_size("inner")
    outer = lax.axis_size("outer")
    slab = features // inner
    tile = tokens // 4
    pairs = inner // 4
    any_space = pl.BlockSpec(memory_space=pl.ANY)
    dims = (inner, outer, tokens, slab, features // HEADS)
    return pl.pallas_call(
        partial(fused_kernel, dims),
        out_shape=pltpu.VMEM((tokens, features), jnp.float32),
        in_specs=[any_space] * 3,
        out_specs=pl.BlockSpec(memory_space=pltpu.VMEM),
        scratch_shapes=[
            *[pltpu.VMEM((tokens, features), jnp.bfloat16)] * 6,
            *[pltpu.VMEM((inner, tokens, slab), jnp.bfloat16)] * 3,
            *[pltpu.VMEM((outer - 1, inner, tile, slab), jnp.bfloat16)] * 2,
            pltpu.VMEM((3, 2, pairs, 4 * tokens, slab), jnp.float32),
            pltpu.VMEM((inner, tokens, slab), jnp.float32),
            pltpu.VMEM((inner, tokens, slab), jnp.bfloat16),
            pltpu.VMEM((tokens, features), jnp.bfloat16),
            *[pltpu.VMEM((tokens, features // 2), jnp.bfloat16)] * 2,
            pltpu.VMEM((3, inner // 2, tokens, slab), jnp.float32),
            pltpu.VMEM((2, 2, tile, slab), jnp.bfloat16),
            pltpu.VMEM((2, tile, features // 2), jnp.bfloat16),
            pltpu.VMEM((2, tokens + tile, slab), jnp.bfloat16),
            pltpu.VMEM((tokens + tile, features // 2), jnp.bfloat16),
            pltpu.VMEM((inner * 2 * tokens, slab), jnp.float32),
            pltpu.SemaphoreType.DMA((3,)),
            pltpu.SemaphoreType.DMA((5 + pairs,)),
            pltpu.SemaphoreType.DMA((outer - 1,)),
            pltpu.SemaphoreType.DMA((1 + pairs,)),
            pltpu.SemaphoreType.DMA((3,)),
            pltpu.SemaphoreType.REGULAR((2,)),
        ],
        compiler_params=pltpu.CompilerParams(collective_id=0, has_side_effects=True),
    )(queries, key_rows, value_rows)


def device_program(queries, key_rows, value_rows):
    tokens, features = queries.shape
    inner = lax.axis_size("inner")
    outer = lax.axis_size("outer")
    width = features // HEADS
    fits = (
        inner * 2 == HEADS
        and outer > 1
        and inner % 4 == 0
        and width * 2 == 128
        and tokens % 64 == 0
        and inner * tokens <= 1024
        and (outer - 1) * inner * tokens // 4 <= 1024
    )
    if fits:
        return fused(queries, key_rows, value_rows)
    return on_device(queries, key_rows, value_rows)


def solution(mesh):
    placed = (P(("outer", "inner"), None), P(("outer", "inner"), None), P(("outer", "inner"), None))
    return jax.shard_map(
        device_program,
        mesh=mesh,
        in_specs=placed,
        out_specs=P(("outer", "inner"), None),
        check_vma=False,
    )
```

```python
import math
from functools import partial, reduce

import jax
import jax.numpy as jnp
import numpy as np
from jax import lax
from jax.experimental import pallas as pl
from jax.experimental.pallas import tpu as pltpu
from jax.sharding import PartitionSpec as P

HEADS = 16


FLOOR_SCORE = -1e30


def divisor_block(length, limit):
    extent = min(length, limit)
    while length % extent:
        extent -= 1
    return extent


def fresh_state(count, rows, width):
    return (
        jnp.full((count, rows), FLOOR_SCORE, jnp.float32),
        jnp.zeros((count, rows), jnp.float32),
        jnp.zeros((count, rows, width), jnp.float32),
    )


def finish_state(state):
    row_max, denominator, summed = state
    return (summed / denominator[..., None], row_max + jnp.log(denominator))


def online_step(state, query_rows, query_rank, key_rows, value_rows, key_rank):
    row_max, denominator, summed = state
    scale = query_rows.shape[-1] ** (-0.5)
    scores = (
        jnp.einsum("inh,ibh->inb", query_rows, key_rows, preferred_element_type=jnp.float32) * scale
    )
    scores = jnp.where(key_rank[None, None, :] <= query_rank[None, :, None], scores, FLOOR_SCORE)
    new_max = jnp.maximum(row_max, jnp.max(scores, axis=2))
    weights = jnp.exp(scores - new_max[..., None])
    rescale = jnp.exp(row_max - new_max)
    denominator = denominator * rescale + jnp.sum(weights, axis=2)
    summed = summed * rescale[..., None] + jnp.einsum(
        "inb,ibh->inh", weights.astype(jnp.bfloat16), value_rows, preferred_element_type=jnp.float32
    )
    return (new_max, denominator, summed)


def attend_keys(state, query_rows, query_rank, key_rows, value_rows, key_rank, stop=None):
    length = key_rows.shape[1]
    block = divisor_block(length, 512)

    def advance(index, carry):
        start = index * block
        piece_keys = lax.dynamic_slice_in_dim(key_rows, start, block, 1)
        piece_values = lax.dynamic_slice_in_dim(value_rows, start, block, 1)
        piece_rank = lax.dynamic_slice_in_dim(key_rank, start, block, 0)
        return online_step(carry, query_rows, query_rank, piece_keys, piece_values, piece_rank)

    upper = length // block if stop is None else stop
    return lax.fori_loop(0, upper, advance, state)


def attend(query_rows, query_rank, key_rows, value_rows, key_rank):
    count, length, width = query_rows.shape
    block = divisor_block(length, 512)
    steps = length // block
    query_split = query_rows.reshape(count, steps, block, width).swapaxes(0, 1)
    rank_split = query_rank.reshape(steps, block)

    def one_block(pieces):
        state = attend_keys(
            fresh_state(count, block, width),
            pieces[0],
            pieces[1],
            key_rows,
            value_rows,
            key_rank,
            pieces[2] + 1,
        )
        return finish_state(state)

    outputs, lses = lax.map(
        one_block, (query_split, rank_split, jnp.arange(steps, dtype=jnp.int32))
    )
    return (
        outputs.swapaxes(0, 1).reshape(count, length, width),
        lses.swapaxes(0, 1).reshape(count, length),
    )


def merge_levels(parts):
    row_max = reduce(jnp.maximum, [lse for _, lse in parts])
    weights = [jnp.exp(lse - row_max) for _, lse in parts]
    denominator = reduce(jnp.add, weights)
    summed = reduce(
        jnp.add, [weight[..., None] * output for weight, (output, _) in zip(weights, parts)]
    )
    return (summed / denominator[..., None], row_max + jnp.log(denominator))


def on_device(queries, key_rows, value_rows):
    tokens, features = queries.shape
    heads = HEADS
    width = features // heads
    outer_count = lax.axis_size("outer")
    inner_count = lax.axis_size("inner")
    outer_index = lax.axis_index("outer")
    inner_index = lax.axis_index("inner")
    per_device = 4 * heads // inner_count
    quarter = tokens // 4
    sixteenth = tokens // 16
    class_len = quarter * inner_count
    far_len = sixteenth * inner_count

    def to_items(array):
        return (
            array.reshape(quarter, 4, heads, width)
            .transpose(2, 1, 0, 3)
            .reshape(4 * heads, quarter, width)
        )

    local_ranks = jnp.arange(tokens, dtype=jnp.int32)
    head_major = [
        a.reshape(tokens, heads, width).transpose(1, 0, 2) for a in (queries, key_rows, value_rows)
    ]
    near_out, near_lse = attend(
        head_major[0], local_ranks, head_major[1], head_major[2], local_ranks
    )
    near_out = near_out.transpose(1, 0, 2)
    near_lse = near_lse.T
    item_index = inner_index * per_device + jnp.arange(per_device, dtype=jnp.int32)
    band = item_index // 16
    far_query_rank = outer_index * far_len + jnp.arange(far_len, dtype=jnp.int32)
    pick = np.array(
        [head * 16 + head // 4 * 4 + residue for head in range(heads) for residue in range(4)],
        np.int32,
    )

    def to_sixteen(array):
        spread = (
            array.reshape(sixteenth, 16, heads, width)
            .transpose(2, 1, 0, 3)
            .reshape(16 * heads, sixteenth, width)
        )
        return jnp.take(spread, pick, axis=0)

    gathered_k, gathered_v = (
        lax.all_gather(to_sixteen(key_rows), "outer", axis=1, tiled=True),
        lax.all_gather(to_sixteen(value_rows), "outer", axis=1, tiled=True),
    )
    mid_q, mid_k, mid_v, far_k, far_v = (
        lax.all_to_all(to_items(queries), "inner", split_axis=0, concat_axis=1, tiled=True),
        lax.all_to_all(to_items(key_rows), "inner", split_axis=0, concat_axis=1, tiled=True),
        lax.all_to_all(to_items(value_rows), "inner", split_axis=0, concat_axis=1, tiled=True),
        lax.all_to_all(gathered_k, "inner", split_axis=0, concat_axis=1, tiled=True),
        lax.all_to_all(gathered_v, "inner", split_axis=0, concat_axis=1, tiled=True),
    )
    split = mid_q.reshape(per_device, far_len, 4, width)
    picker = jnp.broadcast_to(band[:, None, None, None], (per_device, far_len, 1, width))
    far_q = jnp.take_along_axis(split, picker, axis=2)[:, :, 0, :]
    position = jnp.arange(far_k.shape[1], dtype=jnp.int32)
    far_key_rank = (
        position // sixteenth % outer_count * far_len
        + position // (outer_count * sixteenth) * sixteenth
        + position % sixteenth
    )
    far_state = attend_keys(
        fresh_state(per_device, far_len, width), far_q, far_query_rank, far_k, far_v, far_key_rank
    )
    far_out, far_lse = finish_state(far_state)
    class_ranks = jnp.arange(class_len, dtype=jnp.int32)
    mid_out, mid_lse = attend(mid_q, class_ranks, mid_k, mid_v, class_ranks)
    back_mid, back_mid_lse, back_far, back_far_lse = (
        lax.all_to_all(mid_out, "inner", split_axis=1, concat_axis=0, tiled=True),
        lax.all_to_all(mid_lse, "inner", split_axis=1, concat_axis=0, tiled=True),
        lax.all_to_all(far_out, "inner", split_axis=1, concat_axis=0, tiled=True),
        lax.all_to_all(far_lse, "inner", split_axis=1, concat_axis=0, tiled=True),
    )
    selector = np.array(
        [[band_index == head // 4 for band_index in range(4)] for head in range(heads)]
    )
    spread_out = jnp.where(
        selector[:, :, None, None, None], back_far.reshape(heads, 1, 4, sixteenth, width), 0.0
    )
    spread_lse = jnp.where(
        selector[:, :, None, None], back_far_lse.reshape(heads, 1, 4, sixteenth), FLOOR_SCORE
    )
    far_placed = (
        spread_out.reshape(heads, 16, sixteenth, width)
        .transpose(2, 1, 0, 3)
        .reshape(tokens, heads, width)
    )
    far_placed_lse = (
        spread_lse.reshape(heads, 16, sixteenth).transpose(2, 1, 0).reshape(tokens, heads)
    )
    placed = (
        back_mid.reshape(heads, 4, quarter, width)
        .transpose(2, 1, 0, 3)
        .reshape(tokens, heads, width)
    )
    placed_lse = back_mid_lse.reshape(heads, 4, quarter).transpose(2, 1, 0).reshape(tokens, heads)
    combined, _ = merge_levels(
        [(near_out, near_lse), (placed, placed_lse), (far_placed, far_placed_lse)]
    )
    return combined.reshape(tokens, features)


def fused_kernel(
    dims, q_ref, k_ref, v_ref, out_ref, q_held, k_held, v_held, q_rows, k_rows, v_rows, q_buf, k_buf, v_buf, far_k, far_v,
    state_ref, ready, ready_half, landed, side_k, side_v, local_ref, far_out, far_landed, part_out, part_landed,
    spare, send_sem, in_sem, far_sem, back_sem, held_sem, stage_sem,
):
    inner, outer, tokens, slab, width = dims
    chips = inner // 2
    half = inner // 2
    pairs = half // 2
    run = tokens // 16
    tile = tokens // 4
    wide = slab * inner // 4
    me = lax.axis_index("inner")
    mine = lax.axis_index("outer")
    chip = me // 2
    core = lax.rem(me, 2)
    side = me // half
    band = me * 4 // inner
    mesh_id = pl.DeviceIdType.MESH
    sources = (k_ref, v_ref, q_ref)
    held = (k_held, v_held, q_held)
    placed = (k_rows, v_rows, q_rows)
    buffers = (k_buf, v_buf, q_buf)
    pick_k, pick_v, rest_k, rest_v, whole_q, pick_q = range(6)
    pieces = (
        (0, 0, tile),
        (1, 0, tile),
        (0, tile, tokens),
        (1, tile, tokens),
        (2, 0, tokens),
        (2, 0, tile),
    )

    def columns(index):
        return pl.ds(pl.multiple_of(index * slab, slab), slab)

    def drain(semaphore, rows):
        place = spare.at[0 : rows // 2]
        pltpu.make_async_copy(place, place, semaphore).wait()

    def inbound(which, peer, owner, arrival):
        array, start, stop = pieces[which]
        return pltpu.make_async_remote_copy(
            src_ref=placed[array].at[start:stop, columns(peer)],
            dst_ref=buffers[array].at[owner, start:stop, :],
            send_sem=send_sem.at[0],
            recv_sem=in_sem.at[arrival],
            device_id={"inner": peer},
            device_id_type=mesh_id,
        )

    def farbound(which, part, peer, owner):
        blocks = pl.ds(part * half, half)
        return pltpu.make_async_remote_copy(
            src_ref=buffers[which].at[blocks, 0:tile, :],
            dst_ref=(far_k, far_v)[which].at[owner, blocks],
            send_sem=send_sem.at[1],
            recv_sem=far_sem.at[owner],
            device_id={"outer": peer},
            device_id_type=mesh_id,
        )

    def backbound(peer, owner):
        return pltpu.make_async_remote_copy(
            src_ref=ready.at[peer],
            dst_ref=out_ref.at[:, columns(owner)],
            send_sem=send_sem.at[2],
            recv_sem=back_sem.at[0],
            device_id={"inner": peer},
            device_id_type=mesh_id,
        )

    def apart_columns(base):
        return slice(base * slab, (base + half) * slab)

    def sidebound(which, base, peer):
        return pltpu.make_async_remote_copy(
            src_ref=placed[which].at[:, apart_columns(base)],
            dst_ref=(side_k, side_v)[which],
            send_sem=send_sem.at[0],
            recv_sem=in_sem.at[6],
            device_id={"inner": peer},
            device_id_type=mesh_id,
        )

    def partbound(peer):
        return pltpu.make_async_remote_copy(
            src_ref=far_out.at[peer],
            dst_ref=far_landed.at[:, :, columns(me - half)],
            send_sem=send_sem.at[2],
            recv_sem=back_sem.at[1],
            device_id={"inner": peer},
            device_id_type=mesh_id,
        )

    def lastbound(step):
        return pltpu.make_async_remote_copy(
            src_ref=part_out.at[step],
            dst_ref=part_landed.at[:, columns(me)],
            send_sem=send_sem.at[2],
            recv_sem=back_sem.at[1],
            device_id={"inner": inner - 2 + step},
            device_id_type=mesh_id,
        )

    def crossbound(peer, owner, arrival):
        return pltpu.make_async_remote_copy(
            src_ref=ready_half.at[peer],
            dst_ref=landed.at[:, columns(owner)],
            send_sem=send_sem.at[2],
            recv_sem=back_sem.at[arrival],
            device_id={"inner": peer},
            device_id_type=mesh_id,
        )

    own_held = [
        pltpu.make_async_copy(sources[which], held[which], held_sem.at[which]) for which in range(3)
    ]
    for copy in own_held:
        copy.start()

    barrier = pltpu.get_barrier_semaphore()
    partner = chip * 2 + 1 - core

    def greet(place):
        pl.semaphore_signal(barrier, inc=1, device_id=place, device_id_type=mesh_id)

    greet({"inner": partner})
    for step in range(1, outer):
        greet({"inner": chip * 2, "outer": lax.rem(mine + step, outer)})
    for other in range(chips):
        if other < chips // 2:
            counter = jnp.where(jnp.abs(chip - other) > 1, 1, 0)
        else:
            counter = jnp.where((chip > other) & (mine > 0), 1, 0)

        @pl.when(chip != other)
        def _():
            greet({"inner": other * 2 + 1 - counter})

    def row_place(shape, axis, first):
        row = lax.broadcasted_iota(jnp.int32, shape, axis)
        residue = 4 * lax.rem(first + row // tile, 4) + row % tile // run
        return row % run * 16 + residue

    square = (tokens, tokens)
    at_row = lax.broadcasted_iota(jnp.int32, square, 0)
    at_column = lax.broadcasted_iota(jnp.int32, square, 1)
    orders = [
        (row_place(square, 0, first) == at_column).astype(jnp.float32).astype(jnp.bfloat16)
        for first in range(4)
    ]

    def place_rows(which):
        own_held[which].wait()
        for first in range(4):
            place = slice(first * wide, (first + 1) * wide)
            placed[which][:, place] = jnp.dot(
                orders[first], held[which][:, place], preferred_element_type=jnp.float32
            ).astype(jnp.bfloat16)
        buffers[which][me] = placed[which][:, columns(me)]

    adjacent = jnp.where(chip == 0, 1, 2)
    near_chips = jnp.where(side == 0, adjacent, jnp.where(mine == 0, chips - 1, chip))
    near_count = 1 + 2 * near_chips
    rest_count = 1 + 2 * (outer - 1) + 2 * (chips - 1 - near_chips)

    def pass_on(first, stage, count):
        @pl.when(core == first)
        def _():
            pl.semaphore_wait(barrier, count)
            pl.semaphore_signal(
                stage_sem.at[stage], inc=1, device_id={"inner": partner}, device_id_type=mesh_id
            )

        @pl.when(core != first)
        def _():
            pl.semaphore_wait(stage_sem.at[stage], 1)

    picks = (pick_k, pick_v)
    rest = (rest_k, rest_v)
    query = (whole_q,)

    def arrival_of(which, source, target):
        low = chips // 2
        apart = (source < low) != (target < low)
        if which in picks:
            return 2 if apart else 0
        if not apart:
            return 1
        if target < low:
            return 3 if which == whole_q else 4 + source % low
        if source == 0:
            return 4
        return 5 if which == whole_q else 3

    def send(source, batches):
        for group, targets in batches:
            for target in targets:
                for other in range(2):
                    for which in group:
                        arrival = arrival_of(which, source, target)
                        inbound(which, target * 2 + other, me, arrival).start()

    def send_partner(group):
        for which in group:
            inbound(which, partner, me, 0 if which in picks else 1).start()

    place_rows(0)
    place_rows(1)
    pass_on(1, 0, near_count)
    send_partner(picks + rest)

    @pl.when(chip == 0)
    def _():
        send(0, ((picks, (1,)), (rest, (1,))))

        @pl.when(core == 0)
        def _():
            for which in range(2):
                sidebound(which, half, 1).start()


    @pl.when(chip == 1)
    def _():
        send(1, ((picks, (2, 0)), ((rest_k,), (2,)), (rest, (0,))))

    @pl.when(chip == 2)
    def _():
        send(2, ((picks, (0, 1)),))

    @pl.when(chip == 3)
    def _():
        send(3, ((picks, (0, 1, 2)),))

    place_rows(2)
    send_partner(query)

    @pl.when(chip == 0)
    def _():
        send(0, ((query, (1,)),))
        pass_on(0, 1, rest_count)
        send(0, ((picks, (3, 2)), ((pick_q,) + rest, (2, 3))))

    @pl.when(chip == 1)
    def _():
        send(1, ((query, (0,)),))
        pass_on(0, 1, rest_count)
        send(1, ((picks, (3,)), (rest, (3,)), ((rest_v,), (2,)), (query, (3, 2))))

    @pl.when(chip == 2)
    def _():
        @pl.when(mine == 0)
        def _():
            send(2, ((query, (0, 1)),))

        @pl.when(mine > 0)
        def _():
            pass_on(0, 1, rest_count)

        send(2, ((picks, (3,)),))

        @pl.when(mine > 0)
        def _():
            send(2, ((query, (0, 1)),))

        send(2, ((rest, (0, 1)), (query, (3,)), (rest, (3,))))

        @pl.when(mine == 0)
        def _():
            pass_on(0, 1, rest_count)


    @pl.when(chip == 3)
    def _():
        send(3, ((query, (0, 1, 2)), (rest, (2,))))

        @pl.when(core == 0)
        def _():
            for which in range(2):
                sidebound(which, 0, inner - 1).start()

        pass_on(0, 1, rest_count)

    for place, base in ((0, half), (inner - 2, 0)):

        @pl.when(me == place)
        def _():
            side_k[...] = k_rows[:, apart_columns(base)]
            side_v[...] = v_rows[:, apart_columns(base)]

    for other in range(outer - 1):

        @pl.when(mine <= other)
        def _():
            far_k[other] = jnp.zeros((inner, tile, slab), jnp.bfloat16)
            far_v[other] = jnp.zeros((inner, tile, slab), jnp.bfloat16)

    def forward(part):
        for other in range(outer - 1, 0, -1):

            @pl.when(mine < other)
            def _():
                for which in range(2):
                    farbound(which, part, other, mine).start()

    same = at_row % tile // run == at_column % tile // run
    both = (at_row < tile) & (at_column < tile)
    below = jnp.where(same, jnp.where(both, 1.0, 0.0), FLOOR_SCORE)
    before = row_place(square, 1, band) <= row_place(square, 0, band)
    diagonal = jnp.where(
        before, jnp.where(same, jnp.where(both, math.log2(3.0), 1.0), 0.0), FLOOR_SCORE
    )
    never = jnp.full(square, FLOOR_SCORE, jnp.float32)

    def twice(table):
        return jnp.concatenate([table, table], axis=0)

    below_pair = twice(jnp.concatenate([below, below], axis=1))
    below_pair = jnp.concatenate([below_pair, below_pair], axis=0)
    edge_pair = jnp.concatenate(
        [jnp.concatenate([diagonal, never], axis=1), jnp.concatenate([below, diagonal], axis=1)], axis=0
    )
    edge_pair = twice(edge_pair)
    far_rows = inner * tile
    far_shape = (pairs * 4 * tile, (outer - 1) * far_rows)
    far_query = lax.broadcasted_iota(jnp.int32, far_shape, 0)
    far_key = lax.broadcasted_iota(jnp.int32, far_shape, 1)
    far_table = jnp.where(
        (far_query % tile // run == far_key % tile // run) & (far_key // far_rows < mine), 0.0, FLOOR_SCORE
    )
    factor = width ** (-0.5) * math.log2(math.e)
    contract = (((1,), (1,)), ((), ()))

    def by_head(rows):
        lane_head = lax.broadcasted_iota(jnp.int32, rows.shape, 1) // width
        return jnp.concatenate(
            [jnp.where(lane_head == head, rows, jnp.zeros_like(rows)) for head in range(2)], axis=0
        )

    def across(column):
        return jnp.broadcast_to(column, (column.shape[0], slab))

    def attend_part(rows, keys, values, table):
        scores = lax.dot_general(rows, keys, contract, preferred_element_type=jnp.float32)
        scores = scores * factor + table
        top = jnp.max(scores, axis=1, keepdims=True)
        weights = jnp.exp2(scores - top)
        total = jnp.sum(weights, axis=1, keepdims=True)
        summed = jnp.dot(weights.astype(jnp.bfloat16), values, preferred_element_type=jnp.float32)
        return across(top), across(total), summed

    def join(one, two):
        top = jnp.maximum(one[0], two[0])
        first = jnp.exp2(one[0] - top)
        second = jnp.exp2(two[0] - top)
        return top, one[1] * first + two[1] * second, one[2] * first + two[2] * second

    def join_tile(state, far):
        cut = [part.reshape(4, tokens, slab) for part in state]
        met = join([part[:, 0:tile] for part in cut], far)
        return [
            jnp.concatenate([new, old[:, tile:]], axis=1).reshape(4 * tokens, slab)
            for new, old in zip(met, cut)
        ]

    def load_state(index, pair):
        return [state_ref[which, index, pair] for which in range(3)]

    def keep_state(index, pair, state):
        for which in range(3):
            state_ref[which, index, pair] = state[which]

    def pair_queries(index, pair):
        rows = q_buf[index * half + 2 * pair : index * half + 2 * pair + 2]
        return by_head(rows.reshape(2 * tokens, slab))

    def span_of(buffer, start, stop):
        return buffer[start:stop].reshape((stop - start) * tokens, slab)

    def edge(index, pair):
        start = index * half
        stop = start + 2 * pair + 2
        table = jnp.concatenate([below_pair] * pair + [edge_pair], axis=1)
        return attend_part(
            pair_queries(index, pair), span_of(k_buf, start, stop), span_of(v_buf, start, stop), table
        )

    def below_block(pair):
        table = jnp.concatenate([below_pair] * pairs, axis=1)
        return attend_part(
            pair_queries(1, pair), span_of(k_buf, 0, half), span_of(v_buf, 0, half), table
        )

    def far_block(index, first, stop):
        span = stop - first
        rows = [
            by_head(
                q_buf[index * half + 2 * pair : index * half + 2 * pair + 2, 0:tile].reshape(2 * tile, slab)
            )
            for pair in range(first, stop)
        ]
        count = span * 4 * tile
        keys = far_k[...].reshape((outer - 1) * far_rows, slab)
        values = far_v[...].reshape((outer - 1) * far_rows, slab)
        state = attend_part(jnp.concatenate(rows, axis=0), keys, values, far_table[0:count])
        return [
            [part.reshape(span, 4, tile, slab)[place] for part in state] for place in range(span)
        ]

    pair_rows = (2 * tokens, 2 * tokens)
    natural = lax.broadcasted_iota(jnp.int32, pair_rows, 0)
    stored = lax.broadcasted_iota(jnp.int32, pair_rows, 1)
    stored_place = stored // tokens * tokens + row_place(pair_rows, 1, band) % tokens
    restore = (natural == stored_place).astype(jnp.float32).astype(jnp.bfloat16)
    lane_head = lax.broadcasted_iota(jnp.int32, (2 * tokens, slab), 1) // width

    def finish(state):
        total, summed = (part.reshape(2, 2 * tokens, slab) for part in state[1:])
        return jnp.where(lane_head == 0, summed[0], summed[1]) / jnp.where(
            lane_head == 0, total[0], total[1]
        )

    def restored(result, exact):
        coarse = result.astype(jnp.bfloat16)
        moved = jnp.dot(restore, coarse, preferred_element_type=jnp.float32)
        if exact:
            rest = (result - coarse.astype(jnp.float32)).astype(jnp.bfloat16)
            moved = moved + jnp.dot(restore, rest, preferred_element_type=jnp.float32)
        return moved.reshape(2, tokens, slab)

    def keep_exact(index, pair, state):
        moved = restored(finish(state), True)
        for step in range(2):
            ready[index * half + 2 * pair + step] = moved[step]

    def send_half(index, pair, state, arrival):
        moved = restored(finish(state), False).astype(jnp.bfloat16)
        for step in range(2):
            peer = index * half + 2 * pair + step
            ready_half[peer] = moved[step]
            crossbound(peer, me, arrival).start()

    head_lane = lax.broadcasted_iota(jnp.int32, (tokens, slab), 1) // width

    def local_part(base, place):
        first = (base + place) * 4 // inner
        at = slice((base + place) * slab, (base + place + 1) * slab)
        side_at = slice(place * slab, (place + 1) * slab)
        before = row_place(square, 1, first) <= row_place(square, 0, first)
        own = jnp.where(
            before, jnp.where(same, jnp.where(both, math.log2(3.0), 1.0), 0.0), FLOOR_SCORE
        )
        table = jnp.concatenate([jnp.where(core == 1, below, FLOOR_SCORE), own], axis=1)
        keys = jnp.concatenate([side_k[:, side_at], k_rows[:, at]], axis=0)
        values = jnp.concatenate([side_v[:, side_at], v_rows[:, at]], axis=0)
        state = attend_part(by_head(q_rows[:, at]), keys, values, twice(table))
        for which in range(3):
            local_ref[which, place] = jnp.where(
                head_lane == 0, state[which][0:tokens], state[which][tokens:]
            )

    tile_lane = lax.broadcasted_iota(jnp.int32, (tile, slab), 1)
    spread_row = lax.broadcasted_iota(jnp.int32, (slab, slab), 0)
    spread_column = lax.broadcasted_iota(jnp.int32, (slab, slab), 1)
    spread = jnp.where(
        (spread_row // width == spread_column // width)
        & (spread_row % (width // 4) == 0)
        & (spread_row % width < 3 * (width // 4)),
        1.0,
        0.0,
    ).astype(jnp.bfloat16)

    def far_part():
        top, total, summed = far_block(0, 0, 1)[0]
        lane = lax.broadcasted_iota(jnp.int32, (2, tile, slab), 2)
        top, total, summed = (
            jnp.where(lane < width, part[0:2], part[2:4]) for part in (top, total, summed)
        )
        lse = top + jnp.log2(total)
        place = lane % width // (width // 4)
        high = lse.astype(jnp.bfloat16).astype(jnp.float32)
        middle = (lse - high).astype(jnp.bfloat16).astype(jnp.float32)
        low = lse - high - middle
        packed = jnp.where(
            place == 0, high, jnp.where(place == 1, middle, jnp.where(place == 2, low, 0.0))
        )
        result = summed / total
        for peer in range(2):
            far_out[peer, 0] = result[peer].astype(jnp.bfloat16)
            far_out[peer, 1] = packed[peer].astype(jnp.bfloat16)
            partbound(peer).start()

    def local_join(place):
        at = slice(place * slab, (place + 1) * slab)
        result = far_landed[0, :, at].astype(jnp.float32)
        lse = jnp.dot(far_landed[1, :, at], spread, preferred_element_type=jnp.float32)
        top, total, summed = (local_ref[which, place, 0:tile] for which in range(3))
        top, total, summed = join((top, total, summed), (lse, jnp.ones_like(lse), result))
        local_ref[1, place, 0:tile] = total
        local_ref[2, place, 0:tile] = summed

    def thirds(value):
        high = value.astype(jnp.bfloat16).astype(jnp.float32)
        middle = (value - high).astype(jnp.bfloat16).astype(jnp.float32)
        return high, middle, value - high - middle

    lanes = width // 4

    def send_last(state):
        top, total, summed = (part.reshape(2, 2, tokens, slab) for part in state)
        lse = top + jnp.log2(total)
        lane = lax.broadcasted_iota(jnp.int32, (tokens, slab), 1)
        term = lane % lanes // (lanes // 4)
        for step in range(2):
            result = jnp.where(lane < width, summed[0, step], summed[1, step]) / jnp.where(
                lane < width, total[0, step], total[1, step]
            )
            kept = jnp.where(lane % (2 * lanes) < lanes, lse[0, step], lse[1, step])
            high, middle, low = thirds(kept)
            packed = jnp.where(
                term == 0, high, jnp.where(term == 1, middle, jnp.where(term == 2, low, 0.0))
            )
            group = lax.broadcasted_iota(jnp.int32, (tile, slab), 1) // (2 * lanes)
            folded = packed[0:tile]
            for part in range(1, 4):
                folded = jnp.where(group == part, packed[part * tile : (part + 1) * tile], folded)
            part_out[step, 0:tokens] = result.astype(jnp.bfloat16)
            part_out[step, tokens : tokens + tile] = folded.astype(jnp.bfloat16)
            lastbound(step).start()

    unfold_shape = (slab, 4 * slab)
    unfold_row = lax.broadcasted_iota(jnp.int32, unfold_shape, 0)
    unfold_column = lax.broadcasted_iota(jnp.int32, unfold_shape, 1)
    unfold = jnp.where(
        (unfold_row // (2 * lanes) == unfold_column // slab)
        & (unfold_row % (2 * lanes) // lanes == unfold_column % slab // width)
        & (unfold_row % (lanes // 4) == 0)
        & (unfold_row % lanes < 3 * (lanes // 4)),
        1.0,
        0.0,
    ).astype(jnp.bfloat16)

    def last_join(place):
        at = slice(place * slab, (place + 1) * slab)
        result = part_landed[0:tokens, at].astype(jnp.float32)
        wide_lse = jnp.dot(
            part_landed[tokens : tokens + tile, at], unfold, preferred_element_type=jnp.float32
        )
        lse = jnp.concatenate(
            [wide_lse[:, part * slab : (part + 1) * slab] for part in range(4)], axis=0
        )
        state = [local_ref[which, place] for which in range(3)]
        top, total, summed = join(state, (lse, jnp.ones_like(lse), result))
        local_ref[1, place] = total
        local_ref[2, place] = summed

    def local_finish(base, place):
        first = (base + place) * 4 // inner
        order = (at_row == row_place(square, 1, first)).astype(jnp.float32).astype(jnp.bfloat16)
        result = local_ref[2, place] / local_ref[1, place]
        coarse = result.astype(jnp.bfloat16)
        fine = (result - coarse.astype(jnp.float32)).astype(jnp.bfloat16)
        moved = jnp.dot(order, coarse, preferred_element_type=jnp.float32)
        moved = moved + jnp.dot(order, fine, preferred_element_type=jnp.float32)
        out_ref[:, (base + place) * slab : (base + place + 1) * slab] = moved

    drain(in_sem.at[0], (half - 1) * 2 * tile)

    forward(side)

    @pl.when(chip == 0)
    def _():
        @pl.when(core == 1)
        def _():
            drain(in_sem.at[6], 2 * tokens * half)

        for place in range(half):
            local_part(half, place)

    drain(in_sem.at[2], half * 2 * tile)
    forward(1 - side)

    @pl.when(chip == chips - 1)
    def _():
        @pl.when(core == 1)
        def _():
            drain(in_sem.at[6], 2 * tokens * half)

        for place in range(half):
            local_part(0, place)

    drain(in_sem.at[1], (half - 1) * (3 * tokens - 2 * tile))

    def wait_far():
        for other in range(outer - 1):

            @pl.when(mine > other)
            def _():
                drain(far_sem.at[other], 2 * far_rows)

    @pl.when(side == 0)
    def _():
        for pair in range(pairs):
            keep_state(0, pair, edge(0, pair))
        drain(in_sem.at[3], half * tokens)
        for pair in range(pairs):
            keep_state(1, pair, below_block(pair))
        wait_far()
        near_far = far_block(0, 0, pairs)
        apart_far = far_block(1, 0, pairs)
        for pair in range(pairs):
            keep_state(1, pair, join_tile(load_state(1, pair), apart_far[pair]))
        for pair in range(pairs):
            keep_exact(0, pair, join_tile(load_state(0, pair), near_far[pair]))
        for step in range(1, half):
            backbound(lax.rem(me + step, half), me).start()
        out_ref[:, columns(me)] = ready[me]
        drain(in_sem.at[4], 4 * (tokens - tile))
        send_last(
            join(
                load_state(1, 1),
                attend_part(
                    pair_queries(1, 1),
                    span_of(k_buf, half, half + 2),
                    span_of(v_buf, half, half + 2),
                    below_pair,
                ),
            )
        )
        send_half(1, 0, join(load_state(1, 0), edge(1, 0)), 1 + me // 2)

    @pl.when(side == 1)
    def _():
        for pair in range(pairs):
            keep_state(1, pair, edge(1, pair))

        drain(in_sem.at[4], 4 * (tokens - tile) + 2 * tile)
        drain(in_sem.at[3], 4 * (tokens - tile))
        for pair in range(pairs):
            keep_state(1, pair, join(load_state(1, pair), below_block(pair)))
        wait_far()

        @pl.when(mine > 0)
        def _():
            far_part()

        def near_block(own):
            away = 1 - own
            near_far = far_block(1, 0, pairs)
            send_half(1, away, join_tile(load_state(1, away), near_far[away]), 0)
            keep_exact(1, own, join_tile(load_state(1, own), near_far[own]))
            backbound(partner, me).start()
            out_ref[:, columns(me)] = ready[me]

        drain(in_sem.at[5], 2 * tokens)
        send_half(0, 1, join_tile(edge(0, 1), far_block(0, 1, 2)[0]), chip - 1)

        @pl.when(chip < chips - 1)
        def _():
            near_block(0)

        @pl.when(chip == chips - 1)
        def _():
            near_block(1)

    @pl.when(side == 0)
    def _():
        drain(back_sem.at[0], (half - 1) * 2 * tokens)

    @pl.when(side == 1)
    def _():
        drain(back_sem.at[0], 4 * tokens)
        for step in range(2):
            owner = (chips - 1 - chip + chips // 2) * 2 + step
            out_ref[:, columns(owner)] = landed[:, columns(owner)].astype(jnp.float32)

    @pl.when(chip == 0)
    def _():
        @pl.when(mine > 0)
        def _():
            drain(back_sem.at[1], half * 2 * tile)
            for place in range(half):
                local_join(place)

        for place in range(half):
            local_finish(half, place)

    @pl.when(chip == chips - 1)
    def _():
        drain(back_sem.at[1], half * (tokens + tile))
        for place in range(half):
            last_join(place)
        for place in range(half):
            local_finish(0, place)

    @pl.when((chip > 0) & (chip < chips - 1))
    def _():
        for pair in range(pairs):
            drain(back_sem.at[1 + pair], 2 * tokens)
            for step in (2 * pair, 2 * pair + 1):
                owner = (1 - side) * half + step
                out_ref[:, columns(owner)] = landed[:, columns(owner)].astype(jnp.float32)

        drain(send_sem.at[0], (inner - 1) * 3 * tokens)

    sent_near = (half - 1) * 3 * tokens + half * (2 * tokens + tile)

    @pl.when((chip == 0) & (core == 0))
    def _():
        drain(send_sem.at[0], sent_near + 2 * tokens * half)

    @pl.when((chip == 0) & (core == 1))
    def _():
        drain(send_sem.at[0], sent_near)

    sent_last = (half - 1) * 3 * tokens + half * (tokens + 2 * tile)

    @pl.when((chip == chips - 1) & (core == 0))
    def _():
        drain(send_sem.at[0], sent_last + 2 * tokens * half)

    @pl.when((chip == chips - 1) & (core == 1))
    def _():
        drain(send_sem.at[0], sent_last)

    @pl.when(side == 0)
    def _():
        drain(send_sem.at[2], (half - 1) * 2 * tokens + half * tokens + 2 * tile)

    @pl.when((side == 1) & (mine == 0))
    def _():
        drain(send_sem.at[2], 6 * tokens)

    @pl.when((side == 1) & (mine > 0))
    def _():
        drain(send_sem.at[2], 6 * tokens + 4 * tile)

    for count in range(1, outer):

        @pl.when(outer - 1 - mine == count)
        def _():
            drain(send_sem.at[1], count * 2 * far_rows)


def fused(queries, key_rows, value_rows):
    tokens, features = queries.shape
    inner = lax.axis_size("inner")
    outer = lax.axis_size("outer")
    slab = features // inner
    tile = tokens // 4
    pairs = inner // 4
    any_space = pl.BlockSpec(memory_space=pl.ANY)
    dims = (inner, outer, tokens, slab, features // HEADS)
    return pl.pallas_call(
        partial(fused_kernel, dims),
        out_shape=pltpu.VMEM((tokens, features), jnp.float32),
        in_specs=[any_space] * 3,
        out_specs=pl.BlockSpec(memory_space=pltpu.VMEM),
        scratch_shapes=[
            *[pltpu.VMEM((tokens, features), jnp.bfloat16)] * 6,
            *[pltpu.VMEM((inner, tokens, slab), jnp.bfloat16)] * 3,
            *[pltpu.VMEM((outer - 1, inner, tile, slab), jnp.bfloat16)] * 2,
            pltpu.VMEM((3, 2, pairs, 4 * tokens, slab), jnp.float32),
            pltpu.VMEM((inner, tokens, slab), jnp.float32),
            pltpu.VMEM((inner, tokens, slab), jnp.bfloat16),
            pltpu.VMEM((tokens, features), jnp.bfloat16),
            *[pltpu.VMEM((tokens, features // 2), jnp.bfloat16)] * 2,
            pltpu.VMEM((3, inner // 2, tokens, slab), jnp.float32),
            pltpu.VMEM((2, 2, tile, slab), jnp.bfloat16),
            pltpu.VMEM((2, tile, features // 2), jnp.bfloat16),
            pltpu.VMEM((2, tokens + tile, slab), jnp.bfloat16),
            pltpu.VMEM((tokens + tile, features // 2), jnp.bfloat16),
            pltpu.VMEM((inner * 2 * tokens, slab), jnp.float32),
            pltpu.SemaphoreType.DMA((3,)),
            pltpu.SemaphoreType.DMA((5 + pairs,)),
            pltpu.SemaphoreType.DMA((outer - 1,)),
            pltpu.SemaphoreType.DMA((1 + pairs,)),
            pltpu.SemaphoreType.DMA((3,)),
            pltpu.SemaphoreType.REGULAR((2,)),
        ],
        compiler_params=pltpu.CompilerParams(collective_id=0, has_side_effects=True),
    )(queries, key_rows, value_rows)


def device_program(queries, key_rows, value_rows):
    tokens, features = queries.shape
    inner = lax.axis_size("inner")
    outer = lax.axis_size("outer")
    width = features // HEADS
    fits = (
        inner * 2 == HEADS
        and outer > 1
        and inner % 4 == 0
        and width * 2 == 128
        and tokens % 64 == 0
        and inner * tokens <= 1024
        and (outer - 1) * inner * tokens // 4 <= 1024
    )
    if fits:
        return fused(queries, key_rows, value_rows)
    return on_device(queries, key_rows, value_rows)


def solution(mesh):
    placed = (P(("outer", "inner"), None), P(("outer", "inner"), None), P(("outer", "inner"), None))
    return jax.shard_map(
        device_program,
        mesh=mesh,
        in_specs=placed,
        out_specs=P(("outer", "inner"), None),
        check_vma=False,
    )
```

```python
import math
from functools import partial, reduce

import jax
import jax.numpy as jnp
import numpy as np
from jax import lax
from jax.experimental import pallas as pl
from jax.experimental.pallas import tpu as pltpu
from jax.sharding import PartitionSpec as P

HEADS = 16


FLOOR_SCORE = -1e30


def divisor_block(length, limit):
    extent = min(length, limit)
    while length % extent:
        extent -= 1
    return extent


def fresh_state(count, rows, width):
    return (
        jnp.full((count, rows), FLOOR_SCORE, jnp.float32),
        jnp.zeros((count, rows), jnp.float32),
        jnp.zeros((count, rows, width), jnp.float32),
    )


def finish_state(state):
    row_max, denominator, summed = state
    return (summed / denominator[..., None], row_max + jnp.log(denominator))


def online_step(state, query_rows, query_rank, key_rows, value_rows, key_rank):
    row_max, denominator, summed = state
    scale = query_rows.shape[-1] ** (-0.5)
    scores = (
        jnp.einsum("inh,ibh->inb", query_rows, key_rows, preferred_element_type=jnp.float32) * scale
    )
    scores = jnp.where(key_rank[None, None, :] <= query_rank[None, :, None], scores, FLOOR_SCORE)
    new_max = jnp.maximum(row_max, jnp.max(scores, axis=2))
    weights = jnp.exp(scores - new_max[..., None])
    rescale = jnp.exp(row_max - new_max)
    denominator = denominator * rescale + jnp.sum(weights, axis=2)
    summed = summed * rescale[..., None] + jnp.einsum(
        "inb,ibh->inh", weights.astype(jnp.bfloat16), value_rows, preferred_element_type=jnp.float32
    )
    return (new_max, denominator, summed)


def attend_keys(state, query_rows, query_rank, key_rows, value_rows, key_rank, stop=None):
    length = key_rows.shape[1]
    block = divisor_block(length, 512)

    def advance(index, carry):
        start = index * block
        piece_keys = lax.dynamic_slice_in_dim(key_rows, start, block, 1)
        piece_values = lax.dynamic_slice_in_dim(value_rows, start, block, 1)
        piece_rank = lax.dynamic_slice_in_dim(key_rank, start, block, 0)
        return online_step(carry, query_rows, query_rank, piece_keys, piece_values, piece_rank)

    upper = length // block if stop is None else stop
    return lax.fori_loop(0, upper, advance, state)


def attend(query_rows, query_rank, key_rows, value_rows, key_rank):
    count, length, width = query_rows.shape
    block = divisor_block(length, 512)
    steps = length // block
    query_split = query_rows.reshape(count, steps, block, width).swapaxes(0, 1)
    rank_split = query_rank.reshape(steps, block)

    def one_block(pieces):
        state = attend_keys(
            fresh_state(count, block, width),
            pieces[0],
            pieces[1],
            key_rows,
            value_rows,
            key_rank,
            pieces[2] + 1,
        )
        return finish_state(state)

    outputs, lses = lax.map(
        one_block, (query_split, rank_split, jnp.arange(steps, dtype=jnp.int32))
    )
    return (
        outputs.swapaxes(0, 1).reshape(count, length, width),
        lses.swapaxes(0, 1).reshape(count, length),
    )


def merge_levels(parts):
    row_max = reduce(jnp.maximum, [lse for _, lse in parts])
    weights = [jnp.exp(lse - row_max) for _, lse in parts]
    denominator = reduce(jnp.add, weights)
    summed = reduce(
        jnp.add, [weight[..., None] * output for weight, (output, _) in zip(weights, parts)]
    )
    return (summed / denominator[..., None], row_max + jnp.log(denominator))


def on_device(queries, key_rows, value_rows):
    tokens, features = queries.shape
    heads = HEADS
    width = features // heads
    outer_count = lax.axis_size("outer")
    inner_count = lax.axis_size("inner")
    outer_index = lax.axis_index("outer")
    inner_index = lax.axis_index("inner")
    per_device = 4 * heads // inner_count
    quarter = tokens // 4
    sixteenth = tokens // 16
    class_len = quarter * inner_count
    far_len = sixteenth * inner_count

    def to_items(array):
        return (
            array.reshape(quarter, 4, heads, width)
            .transpose(2, 1, 0, 3)
            .reshape(4 * heads, quarter, width)
        )

    local_ranks = jnp.arange(tokens, dtype=jnp.int32)
    head_major = [
        a.reshape(tokens, heads, width).transpose(1, 0, 2) for a in (queries, key_rows, value_rows)
    ]
    near_out, near_lse = attend(
        head_major[0], local_ranks, head_major[1], head_major[2], local_ranks
    )
    near_out = near_out.transpose(1, 0, 2)
    near_lse = near_lse.T
    item_index = inner_index * per_device + jnp.arange(per_device, dtype=jnp.int32)
    band = item_index // 16
    far_query_rank = outer_index * far_len + jnp.arange(far_len, dtype=jnp.int32)
    pick = np.array(
        [head * 16 + head // 4 * 4 + residue for head in range(heads) for residue in range(4)],
        np.int32,
    )

    def to_sixteen(array):
        spread = (
            array.reshape(sixteenth, 16, heads, width)
            .transpose(2, 1, 0, 3)
            .reshape(16 * heads, sixteenth, width)
        )
        return jnp.take(spread, pick, axis=0)

    gathered_k, gathered_v = (
        lax.all_gather(to_sixteen(key_rows), "outer", axis=1, tiled=True),
        lax.all_gather(to_sixteen(value_rows), "outer", axis=1, tiled=True),
    )
    mid_q, mid_k, mid_v, far_k, far_v = (
        lax.all_to_all(to_items(queries), "inner", split_axis=0, concat_axis=1, tiled=True),
        lax.all_to_all(to_items(key_rows), "inner", split_axis=0, concat_axis=1, tiled=True),
        lax.all_to_all(to_items(value_rows), "inner", split_axis=0, concat_axis=1, tiled=True),
        lax.all_to_all(gathered_k, "inner", split_axis=0, concat_axis=1, tiled=True),
        lax.all_to_all(gathered_v, "inner", split_axis=0, concat_axis=1, tiled=True),
    )
    split = mid_q.reshape(per_device, far_len, 4, width)
    picker = jnp.broadcast_to(band[:, None, None, None], (per_device, far_len, 1, width))
    far_q = jnp.take_along_axis(split, picker, axis=2)[:, :, 0, :]
    position = jnp.arange(far_k.shape[1], dtype=jnp.int32)
    far_key_rank = (
        position // sixteenth % outer_count * far_len
        + position // (outer_count * sixteenth) * sixteenth
        + position % sixteenth
    )
    far_state = attend_keys(
        fresh_state(per_device, far_len, width), far_q, far_query_rank, far_k, far_v, far_key_rank
    )
    far_out, far_lse = finish_state(far_state)
    class_ranks = jnp.arange(class_len, dtype=jnp.int32)
    mid_out, mid_lse = attend(mid_q, class_ranks, mid_k, mid_v, class_ranks)
    back_mid, back_mid_lse, back_far, back_far_lse = (
        lax.all_to_all(mid_out, "inner", split_axis=1, concat_axis=0, tiled=True),
        lax.all_to_all(mid_lse, "inner", split_axis=1, concat_axis=0, tiled=True),
        lax.all_to_all(far_out, "inner", split_axis=1, concat_axis=0, tiled=True),
        lax.all_to_all(far_lse, "inner", split_axis=1, concat_axis=0, tiled=True),
    )
    selector = np.array(
        [[band_index == head // 4 for band_index in range(4)] for head in range(heads)]
    )
    spread_out = jnp.where(
        selector[:, :, None, None, None], back_far.reshape(heads, 1, 4, sixteenth, width), 0.0
    )
    spread_lse = jnp.where(
        selector[:, :, None, None], back_far_lse.reshape(heads, 1, 4, sixteenth), FLOOR_SCORE
    )
    far_placed = (
        spread_out.reshape(heads, 16, sixteenth, width)
        .transpose(2, 1, 0, 3)
        .reshape(tokens, heads, width)
    )
    far_placed_lse = (
        spread_lse.reshape(heads, 16, sixteenth).transpose(2, 1, 0).reshape(tokens, heads)
    )
    placed = (
        back_mid.reshape(heads, 4, quarter, width)
        .transpose(2, 1, 0, 3)
        .reshape(tokens, heads, width)
    )
    placed_lse = back_mid_lse.reshape(heads, 4, quarter).transpose(2, 1, 0).reshape(tokens, heads)
    combined, _ = merge_levels(
        [(near_out, near_lse), (placed, placed_lse), (far_placed, far_placed_lse)]
    )
    return combined.reshape(tokens, features)


def fused_kernel(
    dims, q_ref, k_ref, v_ref, out_ref, q_held, k_held, v_held, q_rows, k_rows, v_rows, q_buf, k_buf, v_buf, far_k, far_v,
    state_ref, ready, ready_half, landed, side_k, side_v, local_ref, far_out, far_landed, part_out, part_landed,
    spare, send_sem, in_sem, far_sem, back_sem, held_sem, stage_sem,
):
    inner, outer, tokens, slab, width = dims
    chips = inner // 2
    half = inner // 2
    pairs = half // 2
    run = tokens // 16
    tile = tokens // 4
    wide = slab * inner // 4
    me = lax.axis_index("inner")
    mine = lax.axis_index("outer")
    chip = me // 2
    core = lax.rem(me, 2)
    side = me // half
    band = me * 4 // inner
    mesh_id = pl.DeviceIdType.MESH
    sources = (k_ref, v_ref, q_ref)
    held = (k_held, v_held, q_held)
    placed = (k_rows, v_rows, q_rows)
    buffers = (k_buf, v_buf, q_buf)
    pick_k, pick_v, rest_k, rest_v, whole_q, pick_q = range(6)
    pieces = (
        (0, 0, tile),
        (1, 0, tile),
        (0, tile, tokens),
        (1, tile, tokens),
        (2, 0, tokens),
        (2, 0, tile),
    )

    def columns(index):
        return pl.ds(pl.multiple_of(index * slab, slab), slab)

    def drain(semaphore, rows):
        place = spare.at[0 : rows // 2]
        pltpu.make_async_copy(place, place, semaphore).wait()

    def inbound(which, peer, owner, arrival):
        array, start, stop = pieces[which]
        return pltpu.make_async_remote_copy(
            src_ref=placed[array].at[start:stop, columns(peer)],
            dst_ref=buffers[array].at[owner, start:stop, :],
            send_sem=send_sem.at[0],
            recv_sem=in_sem.at[arrival],
            device_id={"inner": peer},
            device_id_type=mesh_id,
        )

    def farbound(which, part, peer, owner):
        blocks = pl.ds(part * half, half)
        return pltpu.make_async_remote_copy(
            src_ref=buffers[which].at[blocks, 0:tile, :],
            dst_ref=(far_k, far_v)[which].at[owner, blocks],
            send_sem=send_sem.at[1],
            recv_sem=far_sem.at[owner],
            device_id={"outer": peer},
            device_id_type=mesh_id,
        )

    def backbound(peer, owner):
        return pltpu.make_async_remote_copy(
            src_ref=ready.at[peer],
            dst_ref=out_ref.at[:, columns(owner)],
            send_sem=send_sem.at[2],
            recv_sem=back_sem.at[0],
            device_id={"inner": peer},
            device_id_type=mesh_id,
        )

    def apart_columns(base):
        return slice(base * slab, (base + half) * slab)

    def sidebound(which, base, peer):
        return pltpu.make_async_remote_copy(
            src_ref=placed[which].at[:, apart_columns(base)],
            dst_ref=(side_k, side_v)[which],
            send_sem=send_sem.at[0],
            recv_sem=in_sem.at[6],
            device_id={"inner": peer},
            device_id_type=mesh_id,
        )

    def partbound(peer):
        return pltpu.make_async_remote_copy(
            src_ref=far_out.at[peer],
            dst_ref=far_landed.at[:, :, columns(me - half)],
            send_sem=send_sem.at[2],
            recv_sem=back_sem.at[1],
            device_id={"inner": peer},
            device_id_type=mesh_id,
        )

    def lastbound(step):
        return pltpu.make_async_remote_copy(
            src_ref=part_out.at[step],
            dst_ref=part_landed.at[:, columns(me)],
            send_sem=send_sem.at[2],
            recv_sem=back_sem.at[1],
            device_id={"inner": inner - 2 + step},
            device_id_type=mesh_id,
        )

    def crossbound(peer, owner, arrival):
        return pltpu.make_async_remote_copy(
            src_ref=ready_half.at[peer],
            dst_ref=landed.at[:, columns(owner)],
            send_sem=send_sem.at[2],
            recv_sem=back_sem.at[arrival],
            device_id={"inner": peer},
            device_id_type=mesh_id,
        )

    own_held = [
        pltpu.make_async_copy(sources[which], held[which], held_sem.at[which]) for which in range(3)
    ]
    for copy in own_held:
        copy.start()

    barrier = pltpu.get_barrier_semaphore()
    partner = chip * 2 + 1 - core

    def greet(place):
        pl.semaphore_signal(barrier, inc=1, device_id=place, device_id_type=mesh_id)

    greet({"inner": partner})
    for step in range(1, outer):
        greet({"inner": chip * 2, "outer": lax.rem(mine + step, outer)})
    for other in range(chips):
        if other < chips // 2:
            counter = jnp.where(jnp.abs(chip - other) > 1, 1, 0)
        else:
            counter = jnp.where((chip > other) & (mine > 0), 1, 0)

        @pl.when(chip != other)
        def _():
            greet({"inner": other * 2 + 1 - counter})

    def row_place(shape, axis, first):
        row = lax.broadcasted_iota(jnp.int32, shape, axis)
        residue = 4 * lax.rem(first + row // tile, 4) + row % tile // run
        return row % run * 16 + residue

    square = (tokens, tokens)
    at_row = lax.broadcasted_iota(jnp.int32, square, 0)
    at_column = lax.broadcasted_iota(jnp.int32, square, 1)
    orders = [
        (row_place(square, 0, first) == at_column).astype(jnp.float32).astype(jnp.bfloat16)
        for first in range(4)
    ]

    def place_rows(which):
        own_held[which].wait()
        for first in range(4):
            place = slice(first * wide, (first + 1) * wide)
            placed[which][:, place] = jnp.dot(
                orders[first], held[which][:, place], preferred_element_type=jnp.float32
            ).astype(jnp.bfloat16)
        buffers[which][me] = placed[which][:, columns(me)]

    adjacent = jnp.where(chip == 0, 1, 2)
    near_chips = jnp.where(side == 0, adjacent, jnp.where(mine == 0, chips - 1, chip))
    near_count = 1 + 2 * near_chips
    rest_count = 1 + 2 * (outer - 1) + 2 * (chips - 1 - near_chips)

    def pass_on(first, stage, count):
        @pl.when(core == first)
        def _():
            pl.semaphore_wait(barrier, count)
            pl.semaphore_signal(
                stage_sem.at[stage], inc=1, device_id={"inner": partner}, device_id_type=mesh_id
            )

        @pl.when(core != first)
        def _():
            pl.semaphore_wait(stage_sem.at[stage], 1)

    picks = (pick_k, pick_v)
    rest = (rest_k, rest_v)
    query = (whole_q,)

    def arrival_of(which, source, target):
        low = chips // 2
        apart = (source < low) != (target < low)
        if which in picks:
            return 2 if apart else 0
        if not apart:
            return 1
        if target < low:
            return 3 if which == whole_q else 4 + source % low
        if source == 0:
            return 4
        return 5 if which == whole_q else 3

    def send(source, batches):
        for group, targets in batches:
            for target in targets:
                for other in range(2):
                    for which in group:
                        arrival = arrival_of(which, source, target)
                        inbound(which, target * 2 + other, me, arrival).start()

    def send_partner(group):
        for which in group:
            inbound(which, partner, me, 0 if which in picks else 1).start()

    place_rows(0)

    @pl.when(side == 0)
    def _():
        place_rows(1)

    pass_on(1, 0, near_count)

    @pl.when(chip == 2)
    def _():
        send(2, (((pick_k,), (0, 1)),))

    @pl.when(chip == 3)
    def _():
        send(3, (((pick_k,), (0, 1, 2)),))

    @pl.when(side == 1)
    def _():
        place_rows(1)

    send_partner(picks + rest)

    @pl.when(chip == 0)
    def _():
        send(0, ((picks, (1,)), (rest, (1,))))

        @pl.when(core == 0)
        def _():
            for which in range(2):
                sidebound(which, half, 1).start()


    @pl.when(chip == 1)
    def _():
        send(1, ((picks, (2, 0)), ((rest_k,), (2,)), (rest, (0,))))

    @pl.when(chip == 2)
    def _():
        send(2, (((pick_v,), (0, 1)),))

    @pl.when(chip == 3)
    def _():
        send(3, (((pick_v,), (0, 1, 2)),))

    place_rows(2)
    send_partner(query)

    @pl.when(chip == 0)
    def _():
        send(0, ((query, (1,)),))
        pass_on(0, 1, rest_count)
        send(0, ((picks, (3, 2)), ((pick_q,) + rest, (2, 3))))

    @pl.when(chip == 1)
    def _():
        send(1, ((query, (0,)),))
        pass_on(0, 1, rest_count)
        send(1, ((picks, (3,)), (rest, (3,)), ((rest_v,), (2,)), (query, (3, 2))))

    @pl.when(chip == 2)
    def _():
        @pl.when(mine == 0)
        def _():
            send(2, ((query, (0, 1)),))

        @pl.when(mine > 0)
        def _():
            pass_on(0, 1, rest_count)

        send(2, ((picks, (3,)),))

        @pl.when(mine > 0)
        def _():
            send(2, ((query, (0, 1)),))

        send(2, ((rest, (0, 1)), (query, (3,)), (rest, (3,))))

        @pl.when(mine == 0)
        def _():
            pass_on(0, 1, rest_count)


    @pl.when(chip == 3)
    def _():
        send(3, ((query, (0, 1, 2)), (rest, (2,))))

        @pl.when(core == 0)
        def _():
            for which in range(2):
                sidebound(which, 0, inner - 1).start()

        pass_on(0, 1, rest_count)

    for place, base in ((0, half), (inner - 2, 0)):

        @pl.when(me == place)
        def _():
            side_k[...] = k_rows[:, apart_columns(base)]
            side_v[...] = v_rows[:, apart_columns(base)]

    for other in range(outer - 1):

        @pl.when(mine <= other)
        def _():
            far_k[other] = jnp.zeros((inner, tile, slab), jnp.bfloat16)
            far_v[other] = jnp.zeros((inner, tile, slab), jnp.bfloat16)

    def forward(part):
        for other in range(outer - 1, 0, -1):

            @pl.when(mine < other)
            def _():
                for which in range(2):
                    farbound(which, part, other, mine).start()

    same = at_row % tile // run == at_column % tile // run
    both = (at_row < tile) & (at_column < tile)
    below = jnp.where(same, jnp.where(both, 1.0, 0.0), FLOOR_SCORE)
    before = row_place(square, 1, band) <= row_place(square, 0, band)
    diagonal = jnp.where(
        before, jnp.where(same, jnp.where(both, math.log2(3.0), 1.0), 0.0), FLOOR_SCORE
    )
    never = jnp.full(square, FLOOR_SCORE, jnp.float32)

    def twice(table):
        return jnp.concatenate([table, table], axis=0)

    below_pair = twice(jnp.concatenate([below, below], axis=1))
    below_pair = jnp.concatenate([below_pair, below_pair], axis=0)
    edge_pair = jnp.concatenate(
        [jnp.concatenate([diagonal, never], axis=1), jnp.concatenate([below, diagonal], axis=1)], axis=0
    )
    edge_pair = twice(edge_pair)
    far_rows = inner * tile
    far_shape = (pairs * 4 * tile, (outer - 1) * far_rows)
    far_query = lax.broadcasted_iota(jnp.int32, far_shape, 0)
    far_key = lax.broadcasted_iota(jnp.int32, far_shape, 1)
    far_table = jnp.where(
        (far_query % tile // run == far_key % tile // run) & (far_key // far_rows < mine), 0.0, FLOOR_SCORE
    )
    factor = width ** (-0.5) * math.log2(math.e)
    contract = (((1,), (1,)), ((), ()))

    def by_head(rows):
        lane_head = lax.broadcasted_iota(jnp.int32, rows.shape, 1) // width
        return jnp.concatenate(
            [jnp.where(lane_head == head, rows, jnp.zeros_like(rows)) for head in range(2)], axis=0
        )

    def across(column):
        return jnp.broadcast_to(column, (column.shape[0], slab))

    def attend_part(rows, keys, values, table):
        scores = lax.dot_general(rows, keys, contract, preferred_element_type=jnp.float32)
        scores = scores * factor + table
        top = jnp.max(scores, axis=1, keepdims=True)
        weights = jnp.exp2(scores - top)
        total = jnp.sum(weights, axis=1, keepdims=True)
        summed = jnp.dot(weights.astype(jnp.bfloat16), values, preferred_element_type=jnp.float32)
        return across(top), across(total), summed

    def join(one, two):
        top = jnp.maximum(one[0], two[0])
        first = jnp.exp2(one[0] - top)
        second = jnp.exp2(two[0] - top)
        return top, one[1] * first + two[1] * second, one[2] * first + two[2] * second

    def join_tile(state, far):
        cut = [part.reshape(4, tokens, slab) for part in state]
        met = join([part[:, 0:tile] for part in cut], far)
        return [
            jnp.concatenate([new, old[:, tile:]], axis=1).reshape(4 * tokens, slab)
            for new, old in zip(met, cut)
        ]

    def load_state(index, pair):
        return [state_ref[which, index, pair] for which in range(3)]

    def keep_state(index, pair, state):
        for which in range(3):
            state_ref[which, index, pair] = state[which]

    def pair_queries(index, pair):
        rows = q_buf[index * half + 2 * pair : index * half + 2 * pair + 2]
        return by_head(rows.reshape(2 * tokens, slab))

    def span_of(buffer, start, stop):
        return buffer[start:stop].reshape((stop - start) * tokens, slab)

    def edge(index, pair):
        start = index * half
        stop = start + 2 * pair + 2
        table = jnp.concatenate([below_pair] * pair + [edge_pair], axis=1)
        return attend_part(
            pair_queries(index, pair), span_of(k_buf, start, stop), span_of(v_buf, start, stop), table
        )

    def below_block(pair):
        table = jnp.concatenate([below_pair] * pairs, axis=1)
        return attend_part(
            pair_queries(1, pair), span_of(k_buf, 0, half), span_of(v_buf, 0, half), table
        )

    def far_block(index, first, stop):
        span = stop - first
        rows = [
            by_head(
                q_buf[index * half + 2 * pair : index * half + 2 * pair + 2, 0:tile].reshape(2 * tile, slab)
            )
            for pair in range(first, stop)
        ]
        count = span * 4 * tile
        keys = far_k[...].reshape((outer - 1) * far_rows, slab)
        values = far_v[...].reshape((outer - 1) * far_rows, slab)
        state = attend_part(jnp.concatenate(rows, axis=0), keys, values, far_table[0:count])
        return [
            [part.reshape(span, 4, tile, slab)[place] for part in state] for place in range(span)
        ]

    pair_rows = (2 * tokens, 2 * tokens)
    natural = lax.broadcasted_iota(jnp.int32, pair_rows, 0)
    stored = lax.broadcasted_iota(jnp.int32, pair_rows, 1)
    stored_place = stored // tokens * tokens + row_place(pair_rows, 1, band) % tokens
    restore = (natural == stored_place).astype(jnp.float32).astype(jnp.bfloat16)
    lane_head = lax.broadcasted_iota(jnp.int32, (2 * tokens, slab), 1) // width

    def finish(state):
        total, summed = (part.reshape(2, 2 * tokens, slab) for part in state[1:])
        return jnp.where(lane_head == 0, summed[0], summed[1]) / jnp.where(
            lane_head == 0, total[0], total[1]
        )

    def restored(result, exact):
        coarse = result.astype(jnp.bfloat16)
        moved = jnp.dot(restore, coarse, preferred_element_type=jnp.float32)
        if exact:
            rest = (result - coarse.astype(jnp.float32)).astype(jnp.bfloat16)
            moved = moved + jnp.dot(restore, rest, preferred_element_type=jnp.float32)
        return moved.reshape(2, tokens, slab)

    def keep_exact(index, pair, state):
        moved = restored(finish(state), True)
        for step in range(2):
            ready[index * half + 2 * pair + step] = moved[step]

    def send_half(index, pair, state, arrival):
        moved = restored(finish(state), False).astype(jnp.bfloat16)
        for step in range(2):
            peer = index * half + 2 * pair + step
            ready_half[peer] = moved[step]
            crossbound(peer, me, arrival).start()

    head_lane = lax.broadcasted_iota(jnp.int32, (tokens, slab), 1) // width

    def local_part(base, place):
        first = (base + place) * 4 // inner
        at = slice((base + place) * slab, (base + place + 1) * slab)
        side_at = slice(place * slab, (place + 1) * slab)
        before = row_place(square, 1, first) <= row_place(square, 0, first)
        own = jnp.where(
            before, jnp.where(same, jnp.where(both, math.log2(3.0), 1.0), 0.0), FLOOR_SCORE
        )
        table = jnp.concatenate([jnp.where(core == 1, below, FLOOR_SCORE), own], axis=1)
        keys = jnp.concatenate([side_k[:, side_at], k_rows[:, at]], axis=0)
        values = jnp.concatenate([side_v[:, side_at], v_rows[:, at]], axis=0)
        state = attend_part(by_head(q_rows[:, at]), keys, values, twice(table))
        for which in range(3):
            local_ref[which, place] = jnp.where(
                head_lane == 0, state[which][0:tokens], state[which][tokens:]
            )

    tile_lane = lax.broadcasted_iota(jnp.int32, (tile, slab), 1)
    spread_row = lax.broadcasted_iota(jnp.int32, (slab, slab), 0)
    spread_column = lax.broadcasted_iota(jnp.int32, (slab, slab), 1)
    spread = jnp.where(
        (spread_row // width == spread_column // width)
        & (spread_row % (width // 4) == 0)
        & (spread_row % width < 3 * (width // 4)),
        1.0,
        0.0,
    ).astype(jnp.bfloat16)

    def far_part():
        top, total, summed = far_block(0, 0, 1)[0]
        lane = lax.broadcasted_iota(jnp.int32, (2, tile, slab), 2)
        top, total, summed = (
            jnp.where(lane < width, part[0:2], part[2:4]) for part in (top, total, summed)
        )
        lse = top + jnp.log2(total)
        place = lane % width // (width // 4)
        high = lse.astype(jnp.bfloat16).astype(jnp.float32)
        middle = (lse - high).astype(jnp.bfloat16).astype(jnp.float32)
        low = lse - high - middle
        packed = jnp.where(
            place == 0, high, jnp.where(place == 1, middle, jnp.where(place == 2, low, 0.0))
        )
        result = summed / total
        for peer in range(2):
            far_out[peer, 0] = result[peer].astype(jnp.bfloat16)
            far_out[peer, 1] = packed[peer].astype(jnp.bfloat16)
            partbound(peer).start()

    def local_join(place):
        at = slice(place * slab, (place + 1) * slab)
        result = far_landed[0, :, at].astype(jnp.float32)
        lse = jnp.dot(far_landed[1, :, at], spread, preferred_element_type=jnp.float32)
        top, total, summed = (local_ref[which, place, 0:tile] for which in range(3))
        top, total, summed = join((top, total, summed), (lse, jnp.ones_like(lse), result))
        local_ref[1, place, 0:tile] = total
        local_ref[2, place, 0:tile] = summed

    def thirds(value):
        high = value.astype(jnp.bfloat16).astype(jnp.float32)
        middle = (value - high).astype(jnp.bfloat16).astype(jnp.float32)
        return high, middle, value - high - middle

    lanes = width // 4

    def send_last(state):
        top, total, summed = (part.reshape(2, 2, tokens, slab) for part in state)
        lse = top + jnp.log2(total)
        lane = lax.broadcasted_iota(jnp.int32, (tokens, slab), 1)
        term = lane % lanes // (lanes // 4)
        for step in range(2):
            result = jnp.where(lane < width, summed[0, step], summed[1, step]) / jnp.where(
                lane < width, total[0, step], total[1, step]
            )
            kept = jnp.where(lane % (2 * lanes) < lanes, lse[0, step], lse[1, step])
            high, middle, low = thirds(kept)
            packed = jnp.where(
                term == 0, high, jnp.where(term == 1, middle, jnp.where(term == 2, low, 0.0))
            )
            group = lax.broadcasted_iota(jnp.int32, (tile, slab), 1) // (2 * lanes)
            folded = packed[0:tile]
            for part in range(1, 4):
                folded = jnp.where(group == part, packed[part * tile : (part + 1) * tile], folded)
            part_out[step, 0:tokens] = result.astype(jnp.bfloat16)
            part_out[step, tokens : tokens + tile] = folded.astype(jnp.bfloat16)
            lastbound(step).start()

    unfold_shape = (slab, 4 * slab)
    unfold_row = lax.broadcasted_iota(jnp.int32, unfold_shape, 0)
    unfold_column = lax.broadcasted_iota(jnp.int32, unfold_shape, 1)
    unfold = jnp.where(
        (unfold_row // (2 * lanes) == unfold_column // slab)
        & (unfold_row % (2 * lanes) // lanes == unfold_column % slab // width)
        & (unfold_row % (lanes // 4) == 0)
        & (unfold_row % lanes < 3 * (lanes // 4)),
        1.0,
        0.0,
    ).astype(jnp.bfloat16)

    def last_join(place):
        at = slice(place * slab, (place + 1) * slab)
        result = part_landed[0:tokens, at].astype(jnp.float32)
        wide_lse = jnp.dot(
            part_landed[tokens : tokens + tile, at], unfold, preferred_element_type=jnp.float32
        )
        lse = jnp.concatenate(
            [wide_lse[:, part * slab : (part + 1) * slab] for part in range(4)], axis=0
        )
        state = [local_ref[which, place] for which in range(3)]
        top, total, summed = join(state, (lse, jnp.ones_like(lse), result))
        local_ref[1, place] = total
        local_ref[2, place] = summed

    def local_finish(base, place):
        first = (base + place) * 4 // inner
        order = (at_row == row_place(square, 1, first)).astype(jnp.float32).astype(jnp.bfloat16)
        result = local_ref[2, place] / local_ref[1, place]
        coarse = result.astype(jnp.bfloat16)
        fine = (result - coarse.astype(jnp.float32)).astype(jnp.bfloat16)
        moved = jnp.dot(order, coarse, preferred_element_type=jnp.float32)
        moved = moved + jnp.dot(order, fine, preferred_element_type=jnp.float32)
        out_ref[:, (base + place) * slab : (base + place + 1) * slab] = moved

    drain(in_sem.at[0], (half - 1) * 2 * tile)

    forward(side)

    @pl.when(chip == 0)
    def _():
        @pl.when(core == 1)
        def _():
            drain(in_sem.at[6], 2 * tokens * half)

        for place in range(half):
            local_part(half, place)

    drain(in_sem.at[2], half * 2 * tile)
    forward(1 - side)

    @pl.when(chip == chips - 1)
    def _():
        @pl.when(core == 1)
        def _():
            drain(in_sem.at[6], 2 * tokens * half)

        for place in range(half):
            local_part(0, place)

    drain(in_sem.at[1], (half - 1) * (3 * tokens - 2 * tile))

    def wait_far():
        for other in range(outer - 1):

            @pl.when(mine > other)
            def _():
                drain(far_sem.at[other], 2 * far_rows)

    @pl.when(side == 0)
    def _():
        for pair in range(pairs):
            keep_state(0, pair, edge(0, pair))
        drain(in_sem.at[3], half * tokens)
        for pair in range(pairs):
            keep_state(1, pair, below_block(pair))
        wait_far()
        near_far = far_block(0, 0, pairs)
        apart_far = far_block(1, 0, pairs)
        for pair in range(pairs):
            keep_state(1, pair, join_tile(load_state(1, pair), apart_far[pair]))
        for pair in range(pairs):
            keep_exact(0, pair, join_tile(load_state(0, pair), near_far[pair]))
        for step in range(1, half):
            backbound(lax.rem(me + step, half), me).start()
        out_ref[:, columns(me)] = ready[me]
        drain(in_sem.at[4], 4 * (tokens - tile))
        send_last(
            join(
                load_state(1, 1),
                attend_part(
                    pair_queries(1, 1),
                    span_of(k_buf, half, half + 2),
                    span_of(v_buf, half, half + 2),
                    below_pair,
                ),
            )
        )
        send_half(1, 0, join(load_state(1, 0), edge(1, 0)), 1 + me // 2)

    @pl.when(side == 1)
    def _():
        for pair in range(pairs):
            keep_state(1, pair, edge(1, pair))

        drain(in_sem.at[4], 4 * (tokens - tile) + 2 * tile)
        drain(in_sem.at[3], 4 * (tokens - tile))
        for pair in range(pairs):
            keep_state(1, pair, join(load_state(1, pair), below_block(pair)))
        wait_far()

        @pl.when(mine > 0)
        def _():
            far_part()

        def near_block(own):
            away = 1 - own
            near_far = far_block(1, 0, pairs)
            send_half(1, away, join_tile(load_state(1, away), near_far[away]), 0)
            keep_exact(1, own, join_tile(load_state(1, own), near_far[own]))
            backbound(partner, me).start()
            out_ref[:, columns(me)] = ready[me]

        drain(in_sem.at[5], 2 * tokens)
        send_half(0, 1, join_tile(edge(0, 1), far_block(0, 1, 2)[0]), chip - 1)

        @pl.when(chip < chips - 1)
        def _():
            near_block(0)

        @pl.when(chip == chips - 1)
        def _():
            near_block(1)

    @pl.when(side == 0)
    def _():
        drain(back_sem.at[0], (half - 1) * 2 * tokens)

    @pl.when(side == 1)
    def _():
        drain(back_sem.at[0], 4 * tokens)
        for step in range(2):
            owner = (chips - 1 - chip + chips // 2) * 2 + step
            out_ref[:, columns(owner)] = landed[:, columns(owner)].astype(jnp.float32)

    @pl.when(chip == 0)
    def _():
        @pl.when(mine > 0)
        def _():
            drain(back_sem.at[1], half * 2 * tile)
            for place in range(half):
                local_join(place)

        for place in range(half):
            local_finish(half, place)

    @pl.when(chip == chips - 1)
    def _():
        drain(back_sem.at[1], half * (tokens + tile))
        for place in range(half):
            last_join(place)
        for place in range(half):
            local_finish(0, place)

    @pl.when((chip > 0) & (chip < chips - 1))
    def _():
        for pair in range(pairs):
            drain(back_sem.at[1 + pair], 2 * tokens)
            for step in (2 * pair, 2 * pair + 1):
                owner = (1 - side) * half + step
                out_ref[:, columns(owner)] = landed[:, columns(owner)].astype(jnp.float32)

        drain(send_sem.at[0], (inner - 1) * 3 * tokens)

    sent_near = (half - 1) * 3 * tokens + half * (2 * tokens + tile)

    @pl.when((chip == 0) & (core == 0))
    def _():
        drain(send_sem.at[0], sent_near + 2 * tokens * half)

    @pl.when((chip == 0) & (core == 1))
    def _():
        drain(send_sem.at[0], sent_near)

    sent_last = (half - 1) * 3 * tokens + half * (tokens + 2 * tile)

    @pl.when((chip == chips - 1) & (core == 0))
    def _():
        drain(send_sem.at[0], sent_last + 2 * tokens * half)

    @pl.when((chip == chips - 1) & (core == 1))
    def _():
        drain(send_sem.at[0], sent_last)

    @pl.when(side == 0)
    def _():
        drain(send_sem.at[2], (half - 1) * 2 * tokens + half * tokens + 2 * tile)

    @pl.when((side == 1) & (mine == 0))
    def _():
        drain(send_sem.at[2], 6 * tokens)

    @pl.when((side == 1) & (mine > 0))
    def _():
        drain(send_sem.at[2], 6 * tokens + 4 * tile)

    for count in range(1, outer):

        @pl.when(outer - 1 - mine == count)
        def _():
            drain(send_sem.at[1], count * 2 * far_rows)


def fused(queries, key_rows, value_rows):
    tokens, features = queries.shape
    inner = lax.axis_size("inner")
    outer = lax.axis_size("outer")
    slab = features // inner
    tile = tokens // 4
    pairs = inner // 4
    any_space = pl.BlockSpec(memory_space=pl.ANY)
    dims = (inner, outer, tokens, slab, features // HEADS)
    return pl.pallas_call(
        partial(fused_kernel, dims),
        out_shape=pltpu.VMEM((tokens, features), jnp.float32),
        in_specs=[any_space] * 3,
        out_specs=pl.BlockSpec(memory_space=pltpu.VMEM),
        scratch_shapes=[
            *[pltpu.VMEM((tokens, features), jnp.bfloat16)] * 6,
            *[pltpu.VMEM((inner, tokens, slab), jnp.bfloat16)] * 3,
            *[pltpu.VMEM((outer - 1, inner, tile, slab), jnp.bfloat16)] * 2,
            pltpu.VMEM((3, 2, pairs, 4 * tokens, slab), jnp.float32),
            pltpu.VMEM((inner, tokens, slab), jnp.float32),
            pltpu.VMEM((inner, tokens, slab), jnp.bfloat16),
            pltpu.VMEM((tokens, features), jnp.bfloat16),
            *[pltpu.VMEM((tokens, features // 2), jnp.bfloat16)] * 2,
            pltpu.VMEM((3, inner // 2, tokens, slab), jnp.float32),
            pltpu.VMEM((2, 2, tile, slab), jnp.bfloat16),
            pltpu.VMEM((2, tile, features // 2), jnp.bfloat16),
            pltpu.VMEM((2, tokens + tile, slab), jnp.bfloat16),
            pltpu.VMEM((tokens + tile, features // 2), jnp.bfloat16),
            pltpu.VMEM((inner * 2 * tokens, slab), jnp.float32),
            pltpu.SemaphoreType.DMA((3,)),
            pltpu.SemaphoreType.DMA((5 + pairs,)),
            pltpu.SemaphoreType.DMA((outer - 1,)),
            pltpu.SemaphoreType.DMA((1 + pairs,)),
            pltpu.SemaphoreType.DMA((3,)),
            pltpu.SemaphoreType.REGULAR((2,)),
        ],
        compiler_params=pltpu.CompilerParams(collective_id=0, has_side_effects=True),
    )(queries, key_rows, value_rows)


def device_program(queries, key_rows, value_rows):
    tokens, features = queries.shape
    inner = lax.axis_size("inner")
    outer = lax.axis_size("outer")
    width = features // HEADS
    fits = (
        inner * 2 == HEADS
        and outer > 1
        and inner % 4 == 0
        and width * 2 == 128
        and tokens % 64 == 0
        and inner * tokens <= 1024
        and (outer - 1) * inner * tokens // 4 <= 1024
    )
    if fits:
        return fused(queries, key_rows, value_rows)
    return on_device(queries, key_rows, value_rows)


def solution(mesh):
    placed = (P(("outer", "inner"), None), P(("outer", "inner"), None), P(("outer", "inner"), None))
    return jax.shard_map(
        device_program,
        mesh=mesh,
        in_specs=placed,
        out_specs=P(("outer", "inner"), None),
        check_vma=False,
    )
```

```python
import math
from functools import partial, reduce

import jax
import jax.numpy as jnp
import numpy as np
from jax import lax
from jax.experimental import pallas as pl
from jax.experimental.pallas import tpu as pltpu
from jax.sharding import PartitionSpec as P

HEADS = 16


FLOOR_SCORE = -1e30


def divisor_block(length, limit):
    extent = min(length, limit)
    while length % extent:
        extent -= 1
    return extent


def fresh_state(count, rows, width):
    return (
        jnp.full((count, rows), FLOOR_SCORE, jnp.float32),
        jnp.zeros((count, rows), jnp.float32),
        jnp.zeros((count, rows, width), jnp.float32),
    )


def finish_state(state):
    row_max, denominator, summed = state
    return (summed / denominator[..., None], row_max + jnp.log(denominator))


def online_step(state, query_rows, query_rank, key_rows, value_rows, key_rank):
    row_max, denominator, summed = state
    scale = query_rows.shape[-1] ** (-0.5)
    scores = (
        jnp.einsum("inh,ibh->inb", query_rows, key_rows, preferred_element_type=jnp.float32) * scale
    )
    scores = jnp.where(key_rank[None, None, :] <= query_rank[None, :, None], scores, FLOOR_SCORE)
    new_max = jnp.maximum(row_max, jnp.max(scores, axis=2))
    weights = jnp.exp(scores - new_max[..., None])
    rescale = jnp.exp(row_max - new_max)
    denominator = denominator * rescale + jnp.sum(weights, axis=2)
    summed = summed * rescale[..., None] + jnp.einsum(
        "inb,ibh->inh", weights.astype(jnp.bfloat16), value_rows, preferred_element_type=jnp.float32
    )
    return (new_max, denominator, summed)


def attend_keys(state, query_rows, query_rank, key_rows, value_rows, key_rank, stop=None):
    length = key_rows.shape[1]
    block = divisor_block(length, 512)

    def advance(index, carry):
        start = index * block
        piece_keys = lax.dynamic_slice_in_dim(key_rows, start, block, 1)
        piece_values = lax.dynamic_slice_in_dim(value_rows, start, block, 1)
        piece_rank = lax.dynamic_slice_in_dim(key_rank, start, block, 0)
        return online_step(carry, query_rows, query_rank, piece_keys, piece_values, piece_rank)

    upper = length // block if stop is None else stop
    return lax.fori_loop(0, upper, advance, state)


def attend(query_rows, query_rank, key_rows, value_rows, key_rank):
    count, length, width = query_rows.shape
    block = divisor_block(length, 512)
    steps = length // block
    query_split = query_rows.reshape(count, steps, block, width).swapaxes(0, 1)
    rank_split = query_rank.reshape(steps, block)

    def one_block(pieces):
        state = attend_keys(
            fresh_state(count, block, width),
            pieces[0],
            pieces[1],
            key_rows,
            value_rows,
            key_rank,
            pieces[2] + 1,
        )
        return finish_state(state)

    outputs, lses = lax.map(
        one_block, (query_split, rank_split, jnp.arange(steps, dtype=jnp.int32))
    )
    return (
        outputs.swapaxes(0, 1).reshape(count, length, width),
        lses.swapaxes(0, 1).reshape(count, length),
    )


def merge_levels(parts):
    row_max = reduce(jnp.maximum, [lse for _, lse in parts])
    weights = [jnp.exp(lse - row_max) for _, lse in parts]
    denominator = reduce(jnp.add, weights)
    summed = reduce(
        jnp.add, [weight[..., None] * output for weight, (output, _) in zip(weights, parts)]
    )
    return (summed / denominator[..., None], row_max + jnp.log(denominator))


def on_device(queries, key_rows, value_rows):
    tokens, features = queries.shape
    heads = HEADS
    width = features // heads
    outer_count = lax.axis_size("outer")
    inner_count = lax.axis_size("inner")
    outer_index = lax.axis_index("outer")
    inner_index = lax.axis_index("inner")
    per_device = 4 * heads // inner_count
    quarter = tokens // 4
    sixteenth = tokens // 16
    class_len = quarter * inner_count
    far_len = sixteenth * inner_count

    def to_items(array):
        return (
            array.reshape(quarter, 4, heads, width)
            .transpose(2, 1, 0, 3)
            .reshape(4 * heads, quarter, width)
        )

    local_ranks = jnp.arange(tokens, dtype=jnp.int32)
    head_major = [
        a.reshape(tokens, heads, width).transpose(1, 0, 2) for a in (queries, key_rows, value_rows)
    ]
    near_out, near_lse = attend(
        head_major[0], local_ranks, head_major[1], head_major[2], local_ranks
    )
    near_out = near_out.transpose(1, 0, 2)
    near_lse = near_lse.T
    item_index = inner_index * per_device + jnp.arange(per_device, dtype=jnp.int32)
    band = item_index // 16
    far_query_rank = outer_index * far_len + jnp.arange(far_len, dtype=jnp.int32)
    pick = np.array(
        [head * 16 + head // 4 * 4 + residue for head in range(heads) for residue in range(4)],
        np.int32,
    )

    def to_sixteen(array):
        spread = (
            array.reshape(sixteenth, 16, heads, width)
            .transpose(2, 1, 0, 3)
            .reshape(16 * heads, sixteenth, width)
        )
        return jnp.take(spread, pick, axis=0)

    gathered_k, gathered_v = (
        lax.all_gather(to_sixteen(key_rows), "outer", axis=1, tiled=True),
        lax.all_gather(to_sixteen(value_rows), "outer", axis=1, tiled=True),
    )
    mid_q, mid_k, mid_v, far_k, far_v = (
        lax.all_to_all(to_items(queries), "inner", split_axis=0, concat_axis=1, tiled=True),
        lax.all_to_all(to_items(key_rows), "inner", split_axis=0, concat_axis=1, tiled=True),
        lax.all_to_all(to_items(value_rows), "inner", split_axis=0, concat_axis=1, tiled=True),
        lax.all_to_all(gathered_k, "inner", split_axis=0, concat_axis=1, tiled=True),
        lax.all_to_all(gathered_v, "inner", split_axis=0, concat_axis=1, tiled=True),
    )
    split = mid_q.reshape(per_device, far_len, 4, width)
    picker = jnp.broadcast_to(band[:, None, None, None], (per_device, far_len, 1, width))
    far_q = jnp.take_along_axis(split, picker, axis=2)[:, :, 0, :]
    position = jnp.arange(far_k.shape[1], dtype=jnp.int32)
    far_key_rank = (
        position // sixteenth % outer_count * far_len
        + position // (outer_count * sixteenth) * sixteenth
        + position % sixteenth
    )
    far_state = attend_keys(
        fresh_state(per_device, far_len, width), far_q, far_query_rank, far_k, far_v, far_key_rank
    )
    far_out, far_lse = finish_state(far_state)
    class_ranks = jnp.arange(class_len, dtype=jnp.int32)
    mid_out, mid_lse = attend(mid_q, class_ranks, mid_k, mid_v, class_ranks)
    back_mid, back_mid_lse, back_far, back_far_lse = (
        lax.all_to_all(mid_out, "inner", split_axis=1, concat_axis=0, tiled=True),
        lax.all_to_all(mid_lse, "inner", split_axis=1, concat_axis=0, tiled=True),
        lax.all_to_all(far_out, "inner", split_axis=1, concat_axis=0, tiled=True),
        lax.all_to_all(far_lse, "inner", split_axis=1, concat_axis=0, tiled=True),
    )
    selector = np.array(
        [[band_index == head // 4 for band_index in range(4)] for head in range(heads)]
    )
    spread_out = jnp.where(
        selector[:, :, None, None, None], back_far.reshape(heads, 1, 4, sixteenth, width), 0.0
    )
    spread_lse = jnp.where(
        selector[:, :, None, None], back_far_lse.reshape(heads, 1, 4, sixteenth), FLOOR_SCORE
    )
    far_placed = (
        spread_out.reshape(heads, 16, sixteenth, width)
        .transpose(2, 1, 0, 3)
        .reshape(tokens, heads, width)
    )
    far_placed_lse = (
        spread_lse.reshape(heads, 16, sixteenth).transpose(2, 1, 0).reshape(tokens, heads)
    )
    placed = (
        back_mid.reshape(heads, 4, quarter, width)
        .transpose(2, 1, 0, 3)
        .reshape(tokens, heads, width)
    )
    placed_lse = back_mid_lse.reshape(heads, 4, quarter).transpose(2, 1, 0).reshape(tokens, heads)
    combined, _ = merge_levels(
        [(near_out, near_lse), (placed, placed_lse), (far_placed, far_placed_lse)]
    )
    return combined.reshape(tokens, features)


def fused_kernel(
    dims, q_ref, k_ref, v_ref, out_ref, q_held, k_held, v_held, q_rows, k_rows, v_rows, q_buf, k_buf, v_buf, far_k, far_v,
    state_ref, ready, ready_half, landed, side_k, side_v, local_ref, far_out, far_landed, part_out, part_landed,
    spare, send_sem, in_sem, far_sem, back_sem, held_sem, stage_sem,
):
    inner, outer, tokens, slab, width = dims
    chips = inner // 2
    half = inner // 2
    pairs = half // 2
    run = tokens // 16
    tile = tokens // 4
    wide = slab * inner // 4
    me = lax.axis_index("inner")
    mine = lax.axis_index("outer")
    chip = me // 2
    core = lax.rem(me, 2)
    side = me // half
    band = me * 4 // inner
    mesh_id = pl.DeviceIdType.MESH
    sources = (k_ref, v_ref, q_ref)
    held = (k_held, v_held, q_held)
    placed = (k_rows, v_rows, q_rows)
    buffers = (k_buf, v_buf, q_buf)
    pick_k, pick_v, rest_k, rest_v, whole_q, pick_q, rest_q = range(7)
    pieces = (
        (0, 0, tile),
        (1, 0, tile),
        (0, tile, tokens),
        (1, tile, tokens),
        (2, 0, tokens),
        (2, 0, tile),
        (2, tile, tokens),
    )

    def columns(index):
        return pl.ds(pl.multiple_of(index * slab, slab), slab)

    def drain(semaphore, rows):
        place = spare.at[0 : rows // 2]
        pltpu.make_async_copy(place, place, semaphore).wait()

    def inbound(which, peer, owner, arrival):
        array, start, stop = pieces[which]
        return pltpu.make_async_remote_copy(
            src_ref=placed[array].at[start:stop, columns(peer)],
            dst_ref=buffers[array].at[owner, start:stop, :],
            send_sem=send_sem.at[0],
            recv_sem=in_sem.at[arrival],
            device_id={"inner": peer},
            device_id_type=mesh_id,
        )

    def farbound(which, part, peer, owner):
        blocks = pl.ds(part * half, half)
        return pltpu.make_async_remote_copy(
            src_ref=buffers[which].at[blocks, 0:tile, :],
            dst_ref=(far_k, far_v)[which].at[owner, blocks],
            send_sem=send_sem.at[1],
            recv_sem=far_sem.at[owner],
            device_id={"outer": peer},
            device_id_type=mesh_id,
        )

    def backbound(peer, owner):
        return pltpu.make_async_remote_copy(
            src_ref=ready.at[peer],
            dst_ref=out_ref.at[:, columns(owner)],
            send_sem=send_sem.at[2],
            recv_sem=back_sem.at[0],
            device_id={"inner": peer},
            device_id_type=mesh_id,
        )

    def apart_columns(base):
        return slice(base * slab, (base + half) * slab)

    def sidebound(which, base, peer):
        return pltpu.make_async_remote_copy(
            src_ref=placed[which].at[:, apart_columns(base)],
            dst_ref=(side_k, side_v)[which],
            send_sem=send_sem.at[0],
            recv_sem=in_sem.at[6],
            device_id={"inner": peer},
            device_id_type=mesh_id,
        )

    def partbound(peer):
        return pltpu.make_async_remote_copy(
            src_ref=far_out.at[peer],
            dst_ref=far_landed.at[:, :, columns(me - half)],
            send_sem=send_sem.at[2],
            recv_sem=back_sem.at[1],
            device_id={"inner": peer},
            device_id_type=mesh_id,
        )

    def lastbound(step):
        return pltpu.make_async_remote_copy(
            src_ref=part_out.at[step],
            dst_ref=part_landed.at[:, columns(me)],
            send_sem=send_sem.at[2],
            recv_sem=back_sem.at[1],
            device_id={"inner": inner - 2 + step},
            device_id_type=mesh_id,
        )

    def crossbound(peer, owner, arrival):
        return pltpu.make_async_remote_copy(
            src_ref=ready_half.at[peer],
            dst_ref=landed.at[:, columns(owner)],
            send_sem=send_sem.at[2],
            recv_sem=back_sem.at[arrival],
            device_id={"inner": peer},
            device_id_type=mesh_id,
        )

    own_held = [
        pltpu.make_async_copy(sources[which], held[which], held_sem.at[which]) for which in range(3)
    ]
    for copy in own_held:
        copy.start()

    barrier = pltpu.get_barrier_semaphore()
    partner = chip * 2 + 1 - core

    def greet(place):
        pl.semaphore_signal(barrier, inc=1, device_id=place, device_id_type=mesh_id)

    greet({"inner": partner})
    for step in range(1, outer):
        greet({"inner": chip * 2, "outer": lax.rem(mine + step, outer)})
    for other in range(chips):
        if other < chips // 2:
            counter = jnp.where(jnp.abs(chip - other) > 1, 1, 0)
        else:
            counter = jnp.where((chip > other) & (mine > 0), 1, 0)

        @pl.when(chip != other)
        def _():
            greet({"inner": other * 2 + 1 - counter})

    def row_place(shape, axis, first):
        row = lax.broadcasted_iota(jnp.int32, shape, axis)
        residue = 4 * lax.rem(first + row // tile, 4) + row % tile // run
        return row % run * 16 + residue

    square = (tokens, tokens)
    at_row = lax.broadcasted_iota(jnp.int32, square, 0)
    at_column = lax.broadcasted_iota(jnp.int32, square, 1)
    orders = [
        (row_place(square, 0, first) == at_column).astype(jnp.float32).astype(jnp.bfloat16)
        for first in range(4)
    ]

    def place_rows(which):
        own_held[which].wait()
        for first in range(4):
            place = slice(first * wide, (first + 1) * wide)
            placed[which][:, place] = jnp.dot(
                orders[first], held[which][:, place], preferred_element_type=jnp.float32
            ).astype(jnp.bfloat16)
        buffers[which][me] = placed[which][:, columns(me)]

    adjacent = jnp.where(chip == 0, 1, 2)
    near_chips = jnp.where(side == 0, adjacent, jnp.where(mine == 0, chips - 1, chip))
    near_count = 1 + 2 * near_chips
    rest_count = 1 + 2 * (outer - 1) + 2 * (chips - 1 - near_chips)

    def pass_on(first, stage, count):
        @pl.when(core == first)
        def _():
            pl.semaphore_wait(barrier, count)
            pl.semaphore_signal(
                stage_sem.at[stage], inc=1, device_id={"inner": partner}, device_id_type=mesh_id
            )

        @pl.when(core != first)
        def _():
            pl.semaphore_wait(stage_sem.at[stage], 1)

    picks = (pick_k, pick_v)
    rest = (rest_k, rest_v)
    query = (whole_q,)

    def arrival_of(which, source, target):
        low = chips // 2
        apart = (source < low) != (target < low)
        if which in picks:
            return 2 if apart else 0
        if not apart:
            return 1
        if target < low:
            return 3 if which == whole_q else 4 + source % low
        if source == 0 or which == pick_q:
            return 4
        return 5 if which == rest_q else 3

    def send(source, batches):
        for group, targets in batches:
            for target in targets:
                for other in range(2):
                    for which in group:
                        arrival = arrival_of(which, source, target)
                        inbound(which, target * 2 + other, me, arrival).start()

    def send_partner(group):
        for which in group:
            inbound(which, partner, me, 0 if which in picks else 1).start()

    place_rows(0)
    place_rows(1)
    pass_on(1, 0, near_count)
    send_partner(picks + rest)

    @pl.when(chip == 0)
    def _():
        send(0, ((picks, (1,)), (rest, (1,))))

        @pl.when(core == 0)
        def _():
            for which in range(2):
                sidebound(which, half, 1).start()


    @pl.when(chip == 1)
    def _():
        send(1, ((picks, (2, 0)), ((rest_k,), (2,)), (rest, (0,))))

    @pl.when(chip == 2)
    def _():
        send(2, ((picks, (0, 1)),))

    @pl.when(chip == 3)
    def _():
        send(3, ((picks, (0, 1, 2)),))

    place_rows(2)
    send_partner(query)

    @pl.when(chip == 0)
    def _():
        send(0, ((query, (1,)),))
        pass_on(0, 1, rest_count)
        send(0, ((picks, (3, 2)), ((pick_q,) + rest, (2, 3))))

    @pl.when(chip == 1)
    def _():
        send(1, (((pick_q,), (2,)), (query, (0,))))
        pass_on(0, 1, rest_count)
        send(1, ((picks + (pick_q,), (3,)), (rest, (3,)), ((rest_v,), (2,)), ((rest_q,), (3, 2))))

    @pl.when(chip == 2)
    def _():
        @pl.when(mine == 0)
        def _():
            send(2, ((query, (0, 1)),))

        @pl.when(mine > 0)
        def _():
            pass_on(0, 1, rest_count)

        send(2, ((picks, (3,)),))

        @pl.when(mine > 0)
        def _():
            send(2, ((query, (0, 1)),))

        send(2, ((rest, (0, 1)), (query, (3,)), (rest, (3,))))

        @pl.when(mine == 0)
        def _():
            pass_on(0, 1, rest_count)


    @pl.when(chip == 3)
    def _():
        send(3, ((query, (0, 1, 2)), (rest, (2,))))

        @pl.when(core == 0)
        def _():
            for which in range(2):
                sidebound(which, 0, inner - 1).start()

        pass_on(0, 1, rest_count)

    for place, base in ((0, half), (inner - 2, 0)):

        @pl.when(me == place)
        def _():
            side_k[...] = k_rows[:, apart_columns(base)]
            side_v[...] = v_rows[:, apart_columns(base)]

    for other in range(outer - 1):

        @pl.when(mine <= other)
        def _():
            far_k[other] = jnp.zeros((inner, tile, slab), jnp.bfloat16)
            far_v[other] = jnp.zeros((inner, tile, slab), jnp.bfloat16)

    def forward(part):
        for other in range(outer - 1, 0, -1):

            @pl.when(mine < other)
            def _():
                for which in range(2):
                    farbound(which, part, other, mine).start()

    same = at_row % tile // run == at_column % tile // run
    both = (at_row < tile) & (at_column < tile)
    below = jnp.where(same, jnp.where(both, 1.0, 0.0), FLOOR_SCORE)
    before = row_place(square, 1, band) <= row_place(square, 0, band)
    diagonal = jnp.where(
        before, jnp.where(same, jnp.where(both, math.log2(3.0), 1.0), 0.0), FLOOR_SCORE
    )
    never = jnp.full(square, FLOOR_SCORE, jnp.float32)

    def twice(table):
        return jnp.concatenate([table, table], axis=0)

    below_pair = twice(jnp.concatenate([below, below], axis=1))
    below_pair = jnp.concatenate([below_pair, below_pair], axis=0)
    edge_pair = jnp.concatenate(
        [jnp.concatenate([diagonal, never], axis=1), jnp.concatenate([below, diagonal], axis=1)], axis=0
    )
    edge_pair = twice(edge_pair)
    far_rows = inner * tile
    far_shape = (pairs * 4 * tile, (outer - 1) * far_rows)
    far_query = lax.broadcasted_iota(jnp.int32, far_shape, 0)
    far_key = lax.broadcasted_iota(jnp.int32, far_shape, 1)
    far_table = jnp.where(
        (far_query % tile // run == far_key % tile // run) & (far_key // far_rows < mine), 0.0, FLOOR_SCORE
    )
    factor = width ** (-0.5) * math.log2(math.e)
    contract = (((1,), (1,)), ((), ()))

    def by_head(rows):
        lane_head = lax.broadcasted_iota(jnp.int32, rows.shape, 1) // width
        return jnp.concatenate(
            [jnp.where(lane_head == head, rows, jnp.zeros_like(rows)) for head in range(2)], axis=0
        )

    def across(column):
        return jnp.broadcast_to(column, (column.shape[0], slab))

    def attend_part(rows, keys, values, table):
        scores = lax.dot_general(rows, keys, contract, preferred_element_type=jnp.float32)
        scores = scores * factor + table
        top = jnp.max(scores, axis=1, keepdims=True)
        weights = jnp.exp2(scores - top)
        total = jnp.sum(weights, axis=1, keepdims=True)
        summed = jnp.dot(weights.astype(jnp.bfloat16), values, preferred_element_type=jnp.float32)
        return across(top), across(total), summed

    def join(one, two):
        top = jnp.maximum(one[0], two[0])
        first = jnp.exp2(one[0] - top)
        second = jnp.exp2(two[0] - top)
        return top, one[1] * first + two[1] * second, one[2] * first + two[2] * second

    def join_tile(state, far):
        cut = [part.reshape(4, tokens, slab) for part in state]
        met = join([part[:, 0:tile] for part in cut], far)
        return [
            jnp.concatenate([new, old[:, tile:]], axis=1).reshape(4 * tokens, slab)
            for new, old in zip(met, cut)
        ]

    def load_state(index, pair):
        return [state_ref[which, index, pair] for which in range(3)]

    def keep_state(index, pair, state):
        for which in range(3):
            state_ref[which, index, pair] = state[which]

    def pair_queries(index, pair):
        rows = q_buf[index * half + 2 * pair : index * half + 2 * pair + 2]
        return by_head(rows.reshape(2 * tokens, slab))

    def span_of(buffer, start, stop):
        return buffer[start:stop].reshape((stop - start) * tokens, slab)

    def edge(index, pair):
        start = index * half
        stop = start + 2 * pair + 2
        table = jnp.concatenate([below_pair] * pair + [edge_pair], axis=1)
        return attend_part(
            pair_queries(index, pair), span_of(k_buf, start, stop), span_of(v_buf, start, stop), table
        )

    def below_block(pair):
        table = jnp.concatenate([below_pair] * pairs, axis=1)
        return attend_part(
            pair_queries(1, pair), span_of(k_buf, 0, half), span_of(v_buf, 0, half), table
        )

    def far_block(index, first, stop):
        span = stop - first
        rows = [
            by_head(
                q_buf[index * half + 2 * pair : index * half + 2 * pair + 2, 0:tile].reshape(2 * tile, slab)
            )
            for pair in range(first, stop)
        ]
        count = span * 4 * tile
        keys = far_k[...].reshape((outer - 1) * far_rows, slab)
        values = far_v[...].reshape((outer - 1) * far_rows, slab)
        state = attend_part(jnp.concatenate(rows, axis=0), keys, values, far_table[0:count])
        return [
            [part.reshape(span, 4, tile, slab)[place] for part in state] for place in range(span)
        ]

    pair_rows = (2 * tokens, 2 * tokens)
    natural = lax.broadcasted_iota(jnp.int32, pair_rows, 0)
    stored = lax.broadcasted_iota(jnp.int32, pair_rows, 1)
    stored_place = stored // tokens * tokens + row_place(pair_rows, 1, band) % tokens
    restore = (natural == stored_place).astype(jnp.float32).astype(jnp.bfloat16)
    lane_head = lax.broadcasted_iota(jnp.int32, (2 * tokens, slab), 1) // width

    def finish(state):
        total, summed = (part.reshape(2, 2 * tokens, slab) for part in state[1:])
        return jnp.where(lane_head == 0, summed[0], summed[1]) / jnp.where(
            lane_head == 0, total[0], total[1]
        )

    def restored(result, exact):
        coarse = result.astype(jnp.bfloat16)
        moved = jnp.dot(restore, coarse, preferred_element_type=jnp.float32)
        if exact:
            rest = (result - coarse.astype(jnp.float32)).astype(jnp.bfloat16)
            moved = moved + jnp.dot(restore, rest, preferred_element_type=jnp.float32)
        return moved.reshape(2, tokens, slab)

    def keep_exact(index, pair, state):
        moved = restored(finish(state), True)
        for step in range(2):
            ready[index * half + 2 * pair + step] = moved[step]

    def send_half(index, pair, state, arrival):
        moved = restored(finish(state), False).astype(jnp.bfloat16)
        for step in range(2):
            peer = index * half + 2 * pair + step
            ready_half[peer] = moved[step]
            crossbound(peer, me, arrival).start()

    head_lane = lax.broadcasted_iota(jnp.int32, (tokens, slab), 1) // width

    def local_part(base, place):
        first = (base + place) * 4 // inner
        at = slice((base + place) * slab, (base + place + 1) * slab)
        side_at = slice(place * slab, (place + 1) * slab)
        before = row_place(square, 1, first) <= row_place(square, 0, first)
        own = jnp.where(
            before, jnp.where(same, jnp.where(both, math.log2(3.0), 1.0), 0.0), FLOOR_SCORE
        )
        table = jnp.concatenate([jnp.where(core == 1, below, FLOOR_SCORE), own], axis=1)
        keys = jnp.concatenate([side_k[:, side_at], k_rows[:, at]], axis=0)
        values = jnp.concatenate([side_v[:, side_at], v_rows[:, at]], axis=0)
        state = attend_part(by_head(q_rows[:, at]), keys, values, twice(table))
        for which in range(3):
            local_ref[which, place] = jnp.where(
                head_lane == 0, state[which][0:tokens], state[which][tokens:]
            )

    tile_lane = lax.broadcasted_iota(jnp.int32, (tile, slab), 1)
    spread_row = lax.broadcasted_iota(jnp.int32, (slab, slab), 0)
    spread_column = lax.broadcasted_iota(jnp.int32, (slab, slab), 1)
    spread = jnp.where(
        (spread_row // width == spread_column // width)
        & (spread_row % (width // 4) == 0)
        & (spread_row % width < 3 * (width // 4)),
        1.0,
        0.0,
    ).astype(jnp.bfloat16)

    def keep_far(state):
        for which in range(3):
            state_ref[which, 0, 1, 0 : 4 * tile] = state[which].reshape(4 * tile, slab)

    def kept_far():
        return [
            state_ref[which, 0, 1, 0 : 4 * tile].reshape(4, tile, slab) for which in range(3)
        ]

    def far_part():
        first_far, second_far = far_block(0, 0, pairs)
        keep_far(second_far)
        top, total, summed = first_far
        lane = lax.broadcasted_iota(jnp.int32, (2, tile, slab), 2)
        top, total, summed = (
            jnp.where(lane < width, part[0:2], part[2:4]) for part in (top, total, summed)
        )
        lse = top + jnp.log2(total)
        place = lane % width // (width // 4)
        high = lse.astype(jnp.bfloat16).astype(jnp.float32)
        middle = (lse - high).astype(jnp.bfloat16).astype(jnp.float32)
        low = lse - high - middle
        packed = jnp.where(
            place == 0, high, jnp.where(place == 1, middle, jnp.where(place == 2, low, 0.0))
        )
        result = summed / total
        for peer in range(2):
            far_out[peer, 0] = result[peer].astype(jnp.bfloat16)
            far_out[peer, 1] = packed[peer].astype(jnp.bfloat16)
            partbound(peer).start()

    def local_join(place):
        at = slice(place * slab, (place + 1) * slab)
        result = far_landed[0, :, at].astype(jnp.float32)
        lse = jnp.dot(far_landed[1, :, at], spread, preferred_element_type=jnp.float32)
        top, total, summed = (local_ref[which, place, 0:tile] for which in range(3))
        top, total, summed = join((top, total, summed), (lse, jnp.ones_like(lse), result))
        local_ref[1, place, 0:tile] = total
        local_ref[2, place, 0:tile] = summed

    def thirds(value):
        high = value.astype(jnp.bfloat16).astype(jnp.float32)
        middle = (value - high).astype(jnp.bfloat16).astype(jnp.float32)
        return high, middle, value - high - middle

    lanes = width // 4

    def send_last(state):
        top, total, summed = (part.reshape(2, 2, tokens, slab) for part in state)
        lse = top + jnp.log2(total)
        lane = lax.broadcasted_iota(jnp.int32, (tokens, slab), 1)
        term = lane % lanes // (lanes // 4)
        for step in range(2):
            result = jnp.where(lane < width, summed[0, step], summed[1, step]) / jnp.where(
                lane < width, total[0, step], total[1, step]
            )
            kept = jnp.where(lane % (2 * lanes) < lanes, lse[0, step], lse[1, step])
            high, middle, low = thirds(kept)
            packed = jnp.where(
                term == 0, high, jnp.where(term == 1, middle, jnp.where(term == 2, low, 0.0))
            )
            group = lax.broadcasted_iota(jnp.int32, (tile, slab), 1) // (2 * lanes)
            folded = packed[0:tile]
            for part in range(1, 4):
                folded = jnp.where(group == part, packed[part * tile : (part + 1) * tile], folded)
            part_out[step, 0:tokens] = result.astype(jnp.bfloat16)
            part_out[step, tokens : tokens + tile] = folded.astype(jnp.bfloat16)
            lastbound(step).start()

    unfold_shape = (slab, 4 * slab)
    unfold_row = lax.broadcasted_iota(jnp.int32, unfold_shape, 0)
    unfold_column = lax.broadcasted_iota(jnp.int32, unfold_shape, 1)
    unfold = jnp.where(
        (unfold_row // (2 * lanes) == unfold_column // slab)
        & (unfold_row % (2 * lanes) // lanes == unfold_column % slab // width)
        & (unfold_row % (lanes // 4) == 0)
        & (unfold_row % lanes < 3 * (lanes // 4)),
        1.0,
        0.0,
    ).astype(jnp.bfloat16)

    def last_join(place):
        at = slice(place * slab, (place + 1) * slab)
        result = part_landed[0:tokens, at].astype(jnp.float32)
        wide_lse = jnp.dot(
            part_landed[tokens : tokens + tile, at], unfold, preferred_element_type=jnp.float32
        )
        lse = jnp.concatenate(
            [wide_lse[:, part * slab : (part + 1) * slab] for part in range(4)], axis=0
        )
        state = [local_ref[which, place] for which in range(3)]
        top, total, summed = join(state, (lse, jnp.ones_like(lse), result))
        local_ref[1, place] = total
        local_ref[2, place] = summed

    def local_finish(base, place):
        first = (base + place) * 4 // inner
        order = (at_row == row_place(square, 1, first)).astype(jnp.float32).astype(jnp.bfloat16)
        result = local_ref[2, place] / local_ref[1, place]
        coarse = result.astype(jnp.bfloat16)
        fine = (result - coarse.astype(jnp.float32)).astype(jnp.bfloat16)
        moved = jnp.dot(order, coarse, preferred_element_type=jnp.float32)
        moved = moved + jnp.dot(order, fine, preferred_element_type=jnp.float32)
        out_ref[:, (base + place) * slab : (base + place + 1) * slab] = moved

    drain(in_sem.at[0], (half - 1) * 2 * tile)

    forward(side)

    @pl.when(chip == 0)
    def _():
        @pl.when(core == 1)
        def _():
            drain(in_sem.at[6], 2 * tokens * half)

        for place in range(half):
            local_part(half, place)

    drain(in_sem.at[2], half * 2 * tile)
    forward(1 - side)

    @pl.when(chip == chips - 1)
    def _():
        @pl.when(core == 1)
        def _():
            drain(in_sem.at[6], 2 * tokens * half)

        for place in range(half):
            local_part(0, place)

    drain(in_sem.at[1], (half - 1) * (3 * tokens - 2 * tile))

    def wait_far():
        for other in range(outer - 1):

            @pl.when(mine > other)
            def _():
                drain(far_sem.at[other], 2 * far_rows)

    @pl.when(side == 0)
    def _():
        for pair in range(pairs):
            keep_state(0, pair, edge(0, pair))
        drain(in_sem.at[3], half * tokens)
        for pair in range(pairs):
            keep_state(1, pair, below_block(pair))
        wait_far()
        near_far = far_block(0, 0, pairs)
        apart_far = far_block(1, 0, pairs)
        for pair in range(pairs):
            keep_state(1, pair, join_tile(load_state(1, pair), apart_far[pair]))
        for pair in range(pairs):
            keep_exact(0, pair, join_tile(load_state(0, pair), near_far[pair]))
        for step in range(1, half):
            backbound(lax.rem(me + step, half), me).start()
        out_ref[:, columns(me)] = ready[me]
        drain(in_sem.at[4], 4 * (tokens - tile))
        send_last(
            join(
                load_state(1, 1),
                attend_part(
                    pair_queries(1, 1),
                    span_of(k_buf, half, half + 2),
                    span_of(v_buf, half, half + 2),
                    below_pair,
                ),
            )
        )
        send_half(1, 0, join(load_state(1, 0), edge(1, 0)), 1 + me // 2)

    @pl.when(side == 1)
    def _():
        for pair in range(pairs):
            keep_state(1, pair, edge(1, pair))

        drain(in_sem.at[4], 4 * tokens)
        drain(in_sem.at[3], 4 * (tokens - tile))
        for pair in range(pairs):
            keep_state(1, pair, join(load_state(1, pair), below_block(pair)))
        wait_far()

        @pl.when(mine > 0)
        def _():
            far_part()

        @pl.when(mine == 0)
        def _():
            nothing = jnp.zeros((4, tile, slab), jnp.float32)
            keep_far([nothing + FLOOR_SCORE, nothing, nothing])

        def near_block(own):
            away = 1 - own
            near_far = far_block(1, 0, pairs)
            send_half(1, away, join_tile(load_state(1, away), near_far[away]), 0)
            keep_exact(1, own, join_tile(load_state(1, own), near_far[own]))
            backbound(partner, me).start()
            out_ref[:, columns(me)] = ready[me]

        drain(in_sem.at[5], 2 * (tokens - tile))
        send_half(0, 1, join_tile(edge(0, 1), kept_far()), chip - 1)

        @pl.when(chip < chips - 1)
        def _():
            near_block(0)

        @pl.when(chip == chips - 1)
        def _():
            near_block(1)

    @pl.when(side == 0)
    def _():
        drain(back_sem.at[0], (half - 1) * 2 * tokens)

    @pl.when(side == 1)
    def _():
        drain(back_sem.at[0], 4 * tokens)
        for step in range(2):
            owner = (chips - 1 - chip + chips // 2) * 2 + step
            out_ref[:, columns(owner)] = landed[:, columns(owner)].astype(jnp.float32)

    @pl.when(chip == 0)
    def _():
        @pl.when(mine > 0)
        def _():
            drain(back_sem.at[1], half * 2 * tile)
            for place in range(half):
                local_join(place)

        for place in range(half):
            local_finish(half, place)

    @pl.when(chip == chips - 1)
    def _():
        drain(back_sem.at[1], half * (tokens + tile))
        for place in range(half):
            last_join(place)
        for place in range(half):
            local_finish(0, place)

    @pl.when((chip > 0) & (chip < chips - 1))
    def _():
        for pair in range(pairs):
            drain(back_sem.at[1 + pair], 2 * tokens)
            for step in (2 * pair, 2 * pair + 1):
                owner = (1 - side) * half + step
                out_ref[:, columns(owner)] = landed[:, columns(owner)].astype(jnp.float32)

        drain(send_sem.at[0], (inner - 1) * 3 * tokens)

    sent_near = (half - 1) * 3 * tokens + half * (2 * tokens + tile)

    @pl.when((chip == 0) & (core == 0))
    def _():
        drain(send_sem.at[0], sent_near + 2 * tokens * half)

    @pl.when((chip == 0) & (core == 1))
    def _():
        drain(send_sem.at[0], sent_near)

    sent_last = (half - 1) * 3 * tokens + half * (tokens + 2 * tile)

    @pl.when((chip == chips - 1) & (core == 0))
    def _():
        drain(send_sem.at[0], sent_last + 2 * tokens * half)

    @pl.when((chip == chips - 1) & (core == 1))
    def _():
        drain(send_sem.at[0], sent_last)

    @pl.when(side == 0)
    def _():
        drain(send_sem.at[2], (half - 1) * 2 * tokens + half * tokens + 2 * tile)

    @pl.when((side == 1) & (mine == 0))
    def _():
        drain(send_sem.at[2], 6 * tokens)

    @pl.when((side == 1) & (mine > 0))
    def _():
        drain(send_sem.at[2], 6 * tokens + 4 * tile)

    for count in range(1, outer):

        @pl.when(outer - 1 - mine == count)
        def _():
            drain(send_sem.at[1], count * 2 * far_rows)


def fused(queries, key_rows, value_rows):
    tokens, features = queries.shape
    inner = lax.axis_size("inner")
    outer = lax.axis_size("outer")
    slab = features // inner
    tile = tokens // 4
    pairs = inner // 4
    any_space = pl.BlockSpec(memory_space=pl.ANY)
    dims = (inner, outer, tokens, slab, features // HEADS)
    return pl.pallas_call(
        partial(fused_kernel, dims),
        out_shape=pltpu.VMEM((tokens, features), jnp.float32),
        in_specs=[any_space] * 3,
        out_specs=pl.BlockSpec(memory_space=pltpu.VMEM),
        scratch_shapes=[
            *[pltpu.VMEM((tokens, features), jnp.bfloat16)] * 6,
            *[pltpu.VMEM((inner, tokens, slab), jnp.bfloat16)] * 3,
            *[pltpu.VMEM((outer - 1, inner, tile, slab), jnp.bfloat16)] * 2,
            pltpu.VMEM((3, 2, pairs, 4 * tokens, slab), jnp.float32),
            pltpu.VMEM((inner, tokens, slab), jnp.float32),
            pltpu.VMEM((inner, tokens, slab), jnp.bfloat16),
            pltpu.VMEM((tokens, features), jnp.bfloat16),
            *[pltpu.VMEM((tokens, features // 2), jnp.bfloat16)] * 2,
            pltpu.VMEM((3, inner // 2, tokens, slab), jnp.float32),
            pltpu.VMEM((2, 2, tile, slab), jnp.bfloat16),
            pltpu.VMEM((2, tile, features // 2), jnp.bfloat16),
            pltpu.VMEM((2, tokens + tile, slab), jnp.bfloat16),
            pltpu.VMEM((tokens + tile, features // 2), jnp.bfloat16),
            pltpu.VMEM((inner * 2 * tokens, slab), jnp.float32),
            pltpu.SemaphoreType.DMA((3,)),
            pltpu.SemaphoreType.DMA((5 + pairs,)),
            pltpu.SemaphoreType.DMA((outer - 1,)),
            pltpu.SemaphoreType.DMA((1 + pairs,)),
            pltpu.SemaphoreType.DMA((3,)),
            pltpu.SemaphoreType.REGULAR((2,)),
        ],
        compiler_params=pltpu.CompilerParams(collective_id=0, has_side_effects=True),
    )(queries, key_rows, value_rows)


def device_program(queries, key_rows, value_rows):
    tokens, features = queries.shape
    inner = lax.axis_size("inner")
    outer = lax.axis_size("outer")
    width = features // HEADS
    fits = (
        inner * 2 == HEADS
        and outer > 1
        and inner % 4 == 0
        and width * 2 == 128
        and tokens % 64 == 0
        and inner * tokens <= 1024
        and (outer - 1) * inner * tokens // 4 <= 1024
    )
    if fits:
        return fused(queries, key_rows, value_rows)
    return on_device(queries, key_rows, value_rows)


def solution(mesh):
    placed = (P(("outer", "inner"), None), P(("outer", "inner"), None), P(("outer", "inner"), None))
    return jax.shard_map(
        device_program,
        mesh=mesh,
        in_specs=placed,
        out_specs=P(("outer", "inner"), None),
        check_vma=False,
    )
```
